32 devices in a mesh: dp: 2 (over x), row: 4 (over y, core), col: 4 (over z).
Axes of the slice: x: 2, y: 2, z: 4, core: 2. Of those that a mesh axis runs over, the one named last changes fastest.
Arguments:
- tokens: bfloat16 [4096, 2048], P(('dp', 'row'), 'col'), may hold values from -6 to 6
- w_query: bfloat16 [2048, 2048], P('col', 'row'), may hold values from -0.125 to 0.125
- w_key: bfloat16 [2048, 2048], P('col', 'row'), may hold values from -0.125 to 0.125
- w_value: bfloat16 [2048, 2048], P('col', 'row'), may hold values from -0.125 to 0.125
- w_output: bfloat16 [2048, 2048], P('row', 'col'), may hold values from -0.75 to 0.75
- w_gate: bfloat16 [2048, 8192], P('col', 'row'), may hold values from -0.125 to 0.125
- w_up: bfloat16 [2048, 8192], P('col', 'row'), may hold values from -0.125 to 0.125
- w_down: bfloat16 [8192, 2048], P('row', 'col'), may hold values from -0.0625 to 0.0625
- norm_attn: bfloat16 [2048], P('col'), may hold values from 0.5 to 1.5
- norm_ffn: bfloat16 [2048], P('col'), may hold values from 0.5 to 1.5
- prefix_len: int32 [8], P(('dp', 'col')), may hold values from 51 to 256
- cotangent: bfloat16 [4096, 2048], P(('dp', 'row'), 'col'), may hold values from -6 to 6
Outputs:
- output: bfloat16 [4096, 2048], P(('dp', 'row'), 'col')
- grad_tokens: bfloat16 [4096, 2048], P(('dp', 'row'), 'col')
- grad_query: float32 [2048, 2048], P('col', 'row')
- grad_key: float32 [2048, 2048], P('col', 'row')
- grad_value: float32 [2048, 2048], P('col', 'row')
- grad_output_proj: float32 [2048, 2048], P('row', 'col')
- grad_gate: float32 [2048, 8192], P('col', 'row')
- grad_up: float32 [2048, 8192], P('col', 'row')
- grad_down: float32 [8192, 2048], P('row', 'col')
- grad_norm_attn: float32 [2048], P('col')
- grad_norm_ffn: float32 [2048], P('col')
The draws below stay inside these ranges and needn't reach their ends.
Inputs may be any that keep to these rules, and one draw needn't show every extreme that they name: Each sequence's first prefix_len tokens see one another both ways, the rest see earlier tokens and the prefix.
All inputs are finite; a program needn't handle non-finite values.
Results may differ from the reference program's by a relative error of at most 0.035.
Values may be sent and summed in bfloat16 or wider, within the bound.
A program may use at most 192 MiB of HBM per device.

```python
import math
import jax
import jax.numpy as jnp
from jax import lax

D = 2048
HEADS = 32
HEAD_DIM = 64
FF = 8192
SEQ_LEN = 512
TOKENS = 4096
SEQS = 8


def set_ends(array, rng, smallest, high):
    longest = array.shape.index(max(array.shape))
    spots = []
    for shift in (0, 1):
        where = [jax.random.randint(jax.random.fold_in(rng, axis), (), 0, length) for axis, length in enumerate(array.shape)]
        where[longest] = (where[longest] + shift) % array.shape[longest]
        spots.append(tuple(where))
    return array.at[spots[0]].set(smallest).at[spots[1]].set(high)


def block_scale(key, shape, cuts, least, largest):
    def one(dim, blocks):
        draws = jax.random.uniform(jax.random.fold_in(jax.random.fold_in(key, 6), dim), (blocks,), jnp.float32, least / len(cuts), largest / len(cuts))
        return jnp.repeat(jnp.exp(draws), shape[dim] // blocks).reshape((-1,) + (1,) * (len(shape) - dim - 1))

    loudness = one(*cuts[0])
    for cut in cuts[1:]:
        loudness = loudness * one(*cut)
    return loudness


def normal_values(key, shape, deviation, limit, split=(), kind=jnp.bfloat16):
    factor_of = block_scale(key, shape, split, -0.22, 0.18) if split else 1.0
    values = jax.random.normal(key, shape, jnp.float32) * deviation * factor_of
    return jnp.minimum(jnp.maximum(values, -limit), limit).astype(kind)


def setup_inputs(seed: int = 0) -> dict:
    arg_keys = jax.random.split(jax.random.key(seed), 13)
    return {
        "tokens": normal_values(arg_keys[0], (TOKENS, D), 1.0, 6.0, ((0, 8), (1, 4))),
        "w_query": normal_values(arg_keys[1], (D, D), D ** -0.5, 0.125, ((0, 4), (1, 4))),
        "w_key": normal_values(arg_keys[2], (D, D), D ** -0.5, 0.125, ((0, 4), (1, 4))),
        "w_value": normal_values(arg_keys[3], (D, D), D ** -0.5, 0.125, ((0, 4), (1, 4))),
        "w_output": normal_values(arg_keys[4], (D, D), (D * 16 // SEQ_LEN) ** -0.5, 0.75, ((0, 4), (1, 4))),
        "w_gate": normal_values(arg_keys[5], (D, FF), D ** -0.5, 0.125, ((0, 4), (1, 4))),
        "w_up": normal_values(arg_keys[6], (D, FF), D ** -0.5, 0.125, ((0, 4), (1, 4))),
        "w_down": normal_values(arg_keys[7], (FF, D), FF ** -0.5, 0.0625, ((0, 4), (1, 4))),
        "norm_attn": jnp.clip(1.0 + 0.1 * jax.random.normal(arg_keys[8], (D,), jnp.float32), 0.5, 1.5).astype(jnp.bfloat16),
        "norm_ffn": jnp.clip(1.0 + 0.1 * jax.random.normal(arg_keys[9], (D,), jnp.float32), 0.5, 1.5).astype(jnp.bfloat16),
        "prefix_len": set_ends(jax.random.randint(arg_keys[10], (SEQS,), SEQ_LEN // 10, SEQ_LEN // 2 + 1), jax.random.fold_in(arg_keys[10], 1), SEQ_LEN // 10, (SEQ_LEN // 2 + 1) - 1).astype(jnp.int32),
        "cotangent": normal_values(arg_keys[11], (TOKENS, D), 1.0, 6.0, ((0, 8), (1, 4))),
    }


EPSILON = 1e-05
THETA = 130000.0
HIGHEST = lax.Precision.HIGHEST

@jax.custom_vjp
def low(v):
    return lax.optimization_barrier(v.astype(jnp.bfloat16)).astype(jnp.float32)

@jax.custom_vjp
def low_back(v):
    return v

def low_keep(v):
    return (low(v), None)

def low_pass(kept, grad):
    return (grad,)

def back_keep(v):
    return (v, None)

def back_low(kept, grad):
    return (low(grad),)
low.defvjp(low_keep, low_pass)
low_back.defvjp(back_keep, back_low)

def matmul(left, right):
    return jnp.dot(left, right, precision=HIGHEST, preferred_element_type=jnp.float32)

def rms_norm(values, gain):
    inverse = lax.rsqrt(lax.optimization_barrier(jnp.mean(values * values, axis=-1, keepdims=True)) + EPSILON)
    return values * inverse * gain

def rotate(values, cosine, sine):
    row_count = values.shape[0]
    shaped = values.reshape(row_count, HEADS, HEAD_DIM)
    half_dim = HEAD_DIM // 2
    first_half = shaped[:, :, :half_dim]
    second_half = shaped[:, :, half_dim:]
    cosine_rows = cosine[:, None, :]
    sine_rows = sine[:, None, :]
    turned = jnp.concatenate([first_half * cosine_rows - second_half * sine_rows, second_half * cosine_rows + first_half * sine_rows], axis=2)
    return turned.reshape(row_count, HEADS * HEAD_DIM)

def attend(queries, keys, values, prefix_here):
    block_rows = min(512, SEQ_LEN)
    count_blocks = SEQ_LEN // block_rows
    query_blocks = queries.reshape(count_blocks, block_rows, HEADS, HEAD_DIM)
    firsts = jnp.arange(count_blocks, dtype=jnp.int32) * block_rows
    factor = HEAD_DIM ** (-0.5)
    key_place = jnp.arange(SEQ_LEN, dtype=jnp.int32)

    def one_block(inputs):
        query_block, first_row = inputs
        raw_scores = jnp.einsum('qhd,khd->hqk', query_block, keys, precision=HIGHEST)
        scores = low_back(raw_scores) * factor
        query_place = first_row + jnp.arange(block_rows, dtype=jnp.int32)
        visible = (key_place[None, :] <= query_place[:, None]) | (key_place[None, :] < prefix_here)
        exponent = jnp.where(visible[None], jnp.exp(scores), 0.0)
        probabilities = exponent / lax.optimization_barrier(jnp.sum(exponent, axis=2, keepdims=True))
        return jnp.einsum('hqk,khd->qhd', low(probabilities), values, precision=HIGHEST)
    blocks_out = lax.map(jax.checkpoint(one_block), (query_blocks, firsts))
    return blocks_out.reshape(SEQ_LEN, HEADS * HEAD_DIM)

def layer(inputs, weights, prefix_group):
    w_query, w_key, w_value, w_output, w_gate, w_up, w_down, norm_attn, norm_ffn = weights
    row_count = inputs.shape[0]
    count_seqs = row_count // SEQ_LEN
    places = (jnp.arange(row_count, dtype=jnp.int32) % SEQ_LEN).astype(jnp.float32)
    rates = THETA ** (-2.0 * jnp.arange(HEAD_DIM // 2, dtype=jnp.float32) / HEAD_DIM)
    angles = places[:, None] * rates[None, :]
    cosine = jnp.cos(angles)
    sine = jnp.sin(angles)
    normed_one = low(rms_norm(inputs, norm_attn))
    queries = low(rotate(low_back(matmul(normed_one, w_query)), cosine, sine))
    keys = low(rotate(low_back(matmul(normed_one, w_key)), cosine, sine))
    values = low(low_back(matmul(normed_one, w_value)))
    shape_seq = (count_seqs, SEQ_LEN, HEADS, HEAD_DIM)
    attended = jax.vmap(attend)(queries.reshape(shape_seq), keys.reshape(shape_seq), values.reshape(shape_seq), prefix_group)
    attended = low(low_back(attended.reshape(row_count, HEADS * HEAD_DIM)))
    hidden = inputs + low_back(matmul(attended, w_output))
    normed_two = low(rms_norm(hidden, norm_ffn))
    gate = low_back(matmul(normed_two, w_gate))
    up_proj = low_back(matmul(normed_two, w_up))
    activ = low(jax.nn.silu(gate) * up_proj)
    return hidden + low_back(matmul(activ, w_down))

def reference(tokens, w_query, w_key, w_value, w_output, w_gate, w_up, w_down, norm_attn, norm_ffn, prefix_len, cotangent):
    group = math.gcd(SEQS, max(1, 4096 // SEQ_LEN))
    steps_total = SEQS // group
    rows_group = group * SEQ_LEN
    params = tuple((weight.astype(jnp.float32) for weight in (w_query, w_key, w_value, w_output, w_gate, w_up, w_down, norm_attn, norm_ffn)))
    token_groups = tokens.astype(jnp.float32).reshape(steps_total, rows_group, D)
    grad_groups = cotangent.astype(jnp.float32).reshape(steps_total, rows_group, D)
    prefix_groups = prefix_len.reshape(steps_total, group)

    def one_group(summed, inputs):
        token_group, grad_group, prefix_group = inputs

        def forward(token_in, weights):
            return layer(token_in, weights, prefix_group)
        result, pullback = jax.vjp(forward, token_group, params)
        grad_in, grad_params = pullback(grad_group)
        summed = tuple((before + addend for before, addend in zip(summed, grad_params)))
        return (summed, (result, grad_in))
    zeros_init = tuple((jnp.zeros(weight.shape, jnp.float32) for weight in params))
    summed, outputs = lax.scan(one_group, zeros_init, (token_groups, grad_groups, prefix_groups))
    results, grads_in = outputs
    return (results.reshape(TOKENS, D).astype(jnp.bfloat16), grads_in.reshape(TOKENS, D).astype(jnp.bfloat16), summed[0], summed[1], summed[2], summed[3], summed[4], summed[5], summed[6], summed[7], summed[8])
```

```python
import jax
import jax.numpy as jnp
from jax import lax
from jax.sharding import PartitionSpec as P

D = 2048
HEAD_DIM = 64


EPSILON = 1e-05
THETA = 130000.0


def feature_total(values):
    return lax.psum(jnp.sum(values, axis=1), "col")


def normalize(values):
    squares = feature_total(values * values)
    inverse_rms = lax.rsqrt(squares / D + EPSILON)
    return (values * inverse_rms[:, None], inverse_rms)


def norm_backward(grad_normed, unit_rows, inverse_rms, gain_row):
    scaled = grad_normed * gain_row[None, :]
    center = feature_total(scaled * unit_rows) / D
    grad_values = inverse_rms[:, None] * (scaled - unit_rows * center[:, None])
    return (grad_values, jnp.sum(grad_normed * unit_rows, axis=0))


def product(left, weight, transposed):
    if transposed:
        return lax.dot_general(
            left, weight, (((1,), (1,)), ((), ())), preferred_element_type=jnp.float32
        )
    return jnp.dot(left, weight, preferred_element_type=jnp.float32)


def outer_product(left, right):
    return lax.dot_general(
        left, right, (((0,), (0,)), ((), ())), preferred_element_type=jnp.float32
    )


def gather_rows(values):
    return lax.all_gather(values, "row", axis=0, tiled=True)


def gather_cols(values):
    return lax.all_gather(values, "col", axis=0, tiled=True)


def sum_to_cols(gathered, weight, transposed):
    row_count = gathered.shape[0] // lax.axis_size("col")

    def partial_term(offset_rows, length_rows):
        return product(gathered, weight, transposed)

    return lax.psum_scatter(
        partial_term(jnp.int32(0), row_count * lax.axis_size("col")).astype(jnp.bfloat16),
        "col",
        scatter_dimension=0,
        tiled=True,
    ).astype(jnp.float32)


def sum_to_rows(gathered, weight, transposed):
    row_count = gathered.shape[0] // lax.axis_size("row")

    def partial_term(offset_rows, length_rows):
        return product(gathered, weight, transposed)

    return lax.psum_scatter(
        partial_term(jnp.int32(0), row_count * lax.axis_size("row")).astype(jnp.bfloat16),
        "row",
        scatter_dimension=0,
        tiled=True,
    ).astype(jnp.float32)


def rope_tables(row_count, seq_len):
    half_dim = HEAD_DIM // 2
    places = (jnp.arange(row_count, dtype=jnp.int32) % seq_len).astype(jnp.float32)
    rates = THETA ** (-2.0 * jnp.arange(half_dim, dtype=jnp.float32) / HEAD_DIM)
    angles = places[:, None] * rates[None, :]
    return (jnp.cos(angles), jnp.sin(angles))


def rotate(values, cosine, sine):
    row_count = values.shape[0]
    shaped = values.reshape(row_count, -1, HEAD_DIM)
    half_dim = HEAD_DIM // 2
    first_half = shaped[:, :, :half_dim]
    second_half = shaped[:, :, half_dim:]
    cosine_rows = cosine[:, None, :]
    sine_rows = sine[:, None, :]
    turned = jnp.concatenate(
        [
            first_half * cosine_rows - second_half * sine_rows,
            second_half * cosine_rows + first_half * sine_rows,
        ],
        axis=2,
    )
    return turned.reshape(row_count, -1)


def visible_keys(first_row, block_rows, seq_len, prefix_here):
    query_place = first_row + jnp.arange(block_rows, dtype=jnp.int32)
    key_place = jnp.arange(seq_len, dtype=jnp.int32)
    return (key_place[None, :] <= query_place[:, None]) | (key_place[None, :] < prefix_here)


def attention_forward(queries, keys, values, prefix_len, seq_len):
    row_count = queries.shape[0]
    heads_here = queries.shape[1] // HEAD_DIM
    block_rows = min(512, seq_len)
    per_sequence = seq_len // block_rows
    query_blocks = queries.reshape(row_count // block_rows, block_rows, heads_here, HEAD_DIM)
    key_seqs = keys.reshape(row_count // seq_len, seq_len, heads_here, HEAD_DIM)
    value_seqs = values.reshape(row_count // seq_len, seq_len, heads_here, HEAD_DIM)
    factor = HEAD_DIM ** (-0.5)
    numbers = jnp.arange(row_count // block_rows, dtype=jnp.int32)

    def one_block(inputs):
        query_block, number = inputs
        sequence = number // per_sequence
        first_row = number % per_sequence * block_rows
        key_seq = lax.dynamic_index_in_dim(key_seqs, sequence, 0, keepdims=False)
        value_seq = lax.dynamic_index_in_dim(value_seqs, sequence, 0, keepdims=False)
        prefix_here = lax.dynamic_index_in_dim(prefix_len, sequence, 0, keepdims=False)
        scores = (
            jnp.einsum("qhd,khd->hqk", query_block, key_seq, preferred_element_type=jnp.float32)
            * factor
        )
        visible = visible_keys(first_row, block_rows, seq_len, prefix_here)
        exponent = jnp.where(visible[None], jnp.exp(scores), 0.0)
        totals = jnp.sum(exponent, axis=2)
        probabilities = (exponent / totals[:, :, None]).astype(jnp.bfloat16)
        attended = jnp.einsum(
            "hqk,khd->qhd", probabilities, value_seq, preferred_element_type=jnp.float32
        )
        return (attended.reshape(block_rows, heads_here * HEAD_DIM), jnp.log(totals))

    attended, log_totals = lax.map(one_block, (query_blocks, numbers))
    return (attended.reshape(row_count, -1), log_totals)


def attention_backward(queries, keys, values, grad_attended, log_totals, prefix_len, seq_len):
    row_count = queries.shape[0]
    heads_here = queries.shape[1] // HEAD_DIM
    block_rows = min(512, seq_len)
    per_sequence = seq_len // block_rows
    query_blocks = queries.reshape(row_count // block_rows, block_rows, heads_here, HEAD_DIM)
    grad_blocks = grad_attended.reshape(row_count // block_rows, block_rows, heads_here, HEAD_DIM)
    key_seqs = keys.reshape(row_count // seq_len, seq_len, heads_here, HEAD_DIM)
    value_seqs = values.reshape(row_count // seq_len, seq_len, heads_here, HEAD_DIM)
    factor = HEAD_DIM ** (-0.5)
    numbers = jnp.arange(row_count // block_rows, dtype=jnp.int32)
    zero_seqs = jnp.zeros(key_seqs.shape, jnp.float32)

    def one_block(carry, inputs):
        grad_key_seqs, grad_value_seqs = carry
        query_block, grad_block, log_block, number = inputs
        sequence = number // per_sequence
        first_row = number % per_sequence * block_rows
        key_seq = lax.dynamic_index_in_dim(key_seqs, sequence, 0, keepdims=False)
        value_seq = lax.dynamic_index_in_dim(value_seqs, sequence, 0, keepdims=False)
        prefix_here = lax.dynamic_index_in_dim(prefix_len, sequence, 0, keepdims=False)
        scores = (
            jnp.einsum("qhd,khd->hqk", query_block, key_seq, preferred_element_type=jnp.float32)
            * factor
        )
        visible = visible_keys(first_row, block_rows, seq_len, prefix_here)
        probabilities = jnp.where(visible[None], jnp.exp(scores - log_block[:, :, None]), 0.0)
        grad_probs = jnp.einsum(
            "qhd,khd->hqk", grad_block, value_seq, preferred_element_type=jnp.float32
        )
        center = jnp.sum(probabilities * grad_probs, axis=2)
        grad_scores = (probabilities * (grad_probs - center[:, :, None]) * factor).astype(
            jnp.bfloat16
        )
        grad_query = jnp.einsum(
            "hqk,khd->qhd", grad_scores, key_seq, preferred_element_type=jnp.float32
        )
        grad_key = jnp.einsum(
            "hqk,qhd->khd", grad_scores, query_block, preferred_element_type=jnp.float32
        )
        grad_value = jnp.einsum(
            "hqk,qhd->khd",
            probabilities.astype(jnp.bfloat16),
            grad_block,
            preferred_element_type=jnp.float32,
        )
        grad_key_seqs = lax.dynamic_update_index_in_dim(
            grad_key_seqs,
            lax.dynamic_index_in_dim(grad_key_seqs, sequence, 0, keepdims=False) + grad_key,
            sequence,
            0,
        )
        grad_value_seqs = lax.dynamic_update_index_in_dim(
            grad_value_seqs,
            lax.dynamic_index_in_dim(grad_value_seqs, sequence, 0, keepdims=False) + grad_value,
            sequence,
            0,
        )
        return (
            (grad_key_seqs, grad_value_seqs),
            grad_query.reshape(block_rows, heads_here * HEAD_DIM),
        )

    carried, grad_queries = lax.scan(
        one_block, (zero_seqs, zero_seqs), (query_blocks, grad_blocks, log_totals, numbers)
    )
    grad_key_seqs, grad_value_seqs = carried
    return (
        grad_queries.reshape(row_count, -1),
        grad_key_seqs.reshape(row_count, -1),
        grad_value_seqs.reshape(row_count, -1),
    )


def per_device_general(
    tokens,
    w_query,
    w_key,
    w_value,
    w_output,
    w_gate,
    w_up,
    w_down,
    norm_attn,
    norm_ffn,
    prefix_len,
    cotangent,
):
    width_attn = w_query.shape[1]
    width_ffn = w_gate.shape[1]
    inputs = tokens.astype(jnp.float32)
    gain_attn = norm_attn.astype(jnp.float32)
    gain_ffn = norm_ffn.astype(jnp.float32)
    unit_one, inverse_one = normalize(inputs)
    normed_one = (unit_one * gain_attn[None, :]).astype(jnp.bfloat16)
    rows_one = gather_rows(normed_one)
    w_attn = jnp.concatenate([w_query, w_key, w_value], axis=1)
    projected = sum_to_cols(rows_one, w_attn, False)
    row_count = projected.shape[0]
    seq_len = row_count // prefix_len.shape[0]
    cosine, sine = rope_tables(row_count, seq_len)
    queries = rotate(projected[:, :width_attn], cosine, sine).astype(jnp.bfloat16)
    keys = rotate(projected[:, width_attn : 2 * width_attn], cosine, sine).astype(jnp.bfloat16)
    values = projected[:, 2 * width_attn :].astype(jnp.bfloat16)
    attended, log_totals = attention_forward(queries, keys, values, prefix_len, seq_len)
    attended_low = attended.astype(jnp.bfloat16)
    attended_rows = gather_cols(attended_low)
    hidden = inputs + sum_to_rows(attended_rows, w_output, False)
    unit_two, inverse_two = normalize(hidden)
    normed_two = (unit_two * gain_ffn[None, :]).astype(jnp.bfloat16)
    rows_two = gather_rows(normed_two)
    w_pair = jnp.concatenate([w_gate, w_up], axis=1)
    gate_up = sum_to_cols(rows_two, w_pair, False)
    gate = gate_up[:, :width_ffn]
    up_proj = gate_up[:, width_ffn:]
    gate_sigmoid = jax.nn.sigmoid(gate)
    silu_gate = gate * gate_sigmoid
    activ = (silu_gate * up_proj).astype(jnp.bfloat16)
    act_rows = gather_cols(activ)
    result = hidden + sum_to_rows(act_rows, w_down, False)
    output = result.astype(jnp.bfloat16)
    grad_rows = gather_rows(cotangent)
    grad_act = sum_to_cols(grad_rows, w_down, True)
    grad_gate = grad_act * up_proj * gate_sigmoid * (1.0 + gate * (1.0 - gate_sigmoid))
    grad_up = grad_act * silu_gate
    grad_pair = jnp.concatenate([grad_gate, grad_up], axis=1).astype(jnp.bfloat16)
    grad_pair_rows = gather_cols(grad_pair)
    grad_normed_two = sum_to_rows(grad_pair_rows, w_pair, True)
    weight_pair = outer_product(rows_two, grad_pair_rows)
    weight_down = outer_product(act_rows, grad_rows)
    grad_from_two, gain_part_two = norm_backward(grad_normed_two, unit_two, inverse_two, gain_ffn)
    grad_hidden = cotangent.astype(jnp.float32) + grad_from_two
    grad_hidden_low = grad_hidden.astype(jnp.bfloat16)
    grad_hidden_rows = gather_rows(grad_hidden_low)
    grad_attended = sum_to_cols(grad_hidden_rows, w_output, True).astype(jnp.bfloat16)
    weight_out = outer_product(attended_rows, grad_hidden_rows)
    grad_queries, grad_keys, grad_values = attention_backward(
        queries, keys, values, grad_attended, log_totals, prefix_len, seq_len
    )
    grad_proj = jnp.concatenate(
        [rotate(grad_queries, cosine, -sine), rotate(grad_keys, cosine, -sine), grad_values], axis=1
    ).astype(jnp.bfloat16)
    grad_proj_rows = gather_cols(grad_proj)
    grad_normed_one = sum_to_rows(grad_proj_rows, w_attn, True)
    weight_attn = outer_product(rows_one, grad_proj_rows)
    weight_attn, weight_out, weight_pair, weight_down = (
        lax.psum(weight_attn.astype(jnp.bfloat16), "dp").astype(jnp.float32),
        lax.psum(weight_out.astype(jnp.bfloat16), "dp").astype(jnp.float32),
        lax.psum(weight_pair.astype(jnp.bfloat16), "dp").astype(jnp.float32),
        lax.psum(weight_down.astype(jnp.bfloat16), "dp").astype(jnp.float32),
    )
    grad_from_one, gain_part_one = norm_backward(grad_normed_one, unit_one, inverse_one, gain_attn)
    grad_tokens = (grad_hidden + grad_from_one).astype(jnp.bfloat16)
    gain_one, gain_two = lax.psum((gain_part_one, gain_part_two), ("dp", "row"))
    return (
        output,
        grad_tokens,
        weight_attn[:, :width_attn],
        weight_attn[:, width_attn : 2 * width_attn],
        weight_attn[:, 2 * width_attn :],
        weight_out,
        weight_pair[:, :width_ffn],
        weight_pair[:, width_ffn:],
        weight_down,
        gain_one,
        gain_two,
    )


def col_exchange(values, split_axis, concat_axis):
    return lax.all_to_all(values, "col", split_axis=split_axis, concat_axis=concat_axis, tiled=True)


def row_partner(values, bit):
    size = lax.axis_size("row")
    return lax.ppermute(values, "row", [(i, i ^ bit) for i in range(size)])


def dp_partner(values):
    return lax.ppermute(values, "dp", [(0, 1), (1, 0)])


def gather_tokens(values):
    cols = lax.axis_size("col")
    spread = jnp.broadcast_to(values[None], (cols,) + values.shape)
    return lax.all_to_all(spread, "col", 0, 0, tiled=True).reshape(-1, values.shape[1])


def gather_features(values):
    cols = lax.axis_size("col")
    spread = jnp.broadcast_to(values[None], (cols,) + values.shape)
    return jnp.concatenate(
        list(lax.all_to_all(spread, "col", 0, 0, tiled=True)), axis=1
    )


def scatter_tokens(partial):
    cols = lax.axis_size("col")
    parts = partial.astype(jnp.bfloat16).reshape(cols, -1, partial.shape[1])
    parts = lax.all_to_all(parts, "col", 0, 0, tiled=True)
    return jnp.sum(parts.astype(jnp.float32), axis=0)


def columns_of_group(weight):
    own = col_exchange(weight, 1, 0)
    far = row_partner(own, 2)
    near = row_partner(own, 1)
    both = row_partner(far, 1)
    return jnp.concatenate([own, near, far, both], axis=1)


def rows_of_group(weight):
    own = col_exchange(weight, 0, 1)
    far = row_partner(own, 2)
    near = row_partner(own, 1)
    both = row_partner(far, 1)
    return jnp.concatenate([own, near, far, both], axis=0)


def reduce_columns(left, right):
    width = right.shape[1] // 4
    depth = left.shape[1]
    cols = lax.axis_size("col")

    def piece(k):
        return outer_product(left, right[:, k * width : (k + 1) * width])

    near = row_partner(jnp.concatenate([piece(1), piece(3)], axis=1).astype(jnp.bfloat16), 1)
    far = row_partner((piece(2) + near[:, width:]).astype(jnp.bfloat16), 2)
    mine = piece(0) + near[:, :width] + far
    halves = mine.astype(jnp.bfloat16).reshape(cols, 2, depth // cols // 2, width)
    side = lax.axis_index("dp")
    keep = lax.dynamic_index_in_dim(halves, side, 1, keepdims=False)
    give = lax.dynamic_index_in_dim(halves, 1 - side, 1, keepdims=False)
    summed = (keep.astype(jnp.float32) + dp_partner(give)).astype(jnp.bfloat16)
    block = lax.all_to_all(summed, "col", 0, 0, tiled=True)
    block = jnp.concatenate(list(block), axis=1)
    other = dp_partner(block)
    first = jnp.where(side == 0, block, other)
    second = jnp.where(side == 0, other, block)
    return jnp.concatenate([first, second], axis=0).astype(jnp.float32)


def reduce_rows(left, right):
    width = left.shape[1] // 4
    depth = right.shape[1]
    cols = lax.axis_size("col")

    def piece(k):
        return outer_product(left[:, k * width : (k + 1) * width], right)

    near = row_partner(jnp.concatenate([piece(1), piece(3)], axis=0).astype(jnp.bfloat16), 1)
    far = row_partner((piece(2) + near[width:]).astype(jnp.bfloat16), 2)
    mine = piece(0) + near[:width] + far
    halves = mine.astype(jnp.bfloat16).reshape(2, width // 2, depth)
    side = lax.axis_index("dp")
    keep = lax.dynamic_index_in_dim(halves, side, 0, keepdims=False)
    give = lax.dynamic_index_in_dim(halves, 1 - side, 0, keepdims=False)
    summed = (keep.astype(jnp.float32) + dp_partner(give)).astype(jnp.bfloat16)
    parts = jnp.stack(jnp.split(summed, cols, axis=1))
    block = lax.all_to_all(parts, "col", 0, 0, tiled=True)
    other = dp_partner(block)
    first = jnp.where(side == 0, block, other)
    second = jnp.where(side == 0, other, block)
    return (
        jnp.stack([first, second], axis=1).reshape(cols * width, depth // cols).astype(jnp.float32)
    )


def per_device(
    tokens,
    w_query,
    w_key,
    w_value,
    w_output,
    w_gate,
    w_up,
    w_down,
    norm_attn,
    norm_ffn,
    prefix_len,
    cotangent,
):
    rows = lax.axis_size("row")
    cols = lax.axis_size("col")
    seq_len = tokens.shape[0]
    col_index = lax.axis_index("col")
    share = seq_len // cols
    depth = tokens.shape[1] * cols

    prefix_here = lax.ppermute(
        prefix_len,
        ("row", "col"),
        [(c * cols + r, r * cols + c) for r in range(rows) for c in range(cols)],
    )
    gains = lax.all_gather(
        jnp.stack([norm_attn, norm_ffn]), "col", axis=1, tiled=True
    ).astype(jnp.float32)
    gain_attn = gains[0]
    gain_ffn = gains[1]

    inputs = gather_features(tokens).astype(jnp.float32)
    wide_query = columns_of_group(w_query)
    wide_key = columns_of_group(w_key)
    wide_value = columns_of_group(w_value)
    wide_output = rows_of_group(w_output)
    wide_gate = columns_of_group(w_gate)
    wide_up = columns_of_group(w_up)
    wide_down = rows_of_group(w_down)
    grad_rows = gather_features(cotangent)

    def own_tokens(values):
        return lax.dynamic_slice_in_dim(values, col_index * share, share, 0)

    inverse_one = lax.rsqrt(jnp.mean(inputs * inputs, axis=1) + EPSILON)
    unit_one = inputs * inverse_one[:, None]
    normed_one = (unit_one * gain_attn[None, :]).astype(jnp.bfloat16)
    cosine, sine = rope_tables(seq_len, seq_len)
    queries = rotate(product(normed_one, wide_query, False), cosine, sine).astype(jnp.bfloat16)
    keys = rotate(product(normed_one, wide_key, False), cosine, sine).astype(jnp.bfloat16)
    values = product(normed_one, wide_value, False).astype(jnp.bfloat16)
    attended, log_totals = attention_forward(queries, keys, values, prefix_here, seq_len)
    attended_low = attended.astype(jnp.bfloat16)
    hidden = own_tokens(inputs) + scatter_tokens(product(attended_low, wide_output, False))
    inverse_two = lax.rsqrt(jnp.mean(hidden * hidden, axis=1) + EPSILON)
    unit_two = hidden * inverse_two[:, None]
    normed_two = gather_tokens((unit_two * gain_ffn[None, :]).astype(jnp.bfloat16))
    gate = product(normed_two, wide_gate, False)
    up_proj = product(normed_two, wide_up, False)
    gate_sigmoid = jax.nn.sigmoid(gate)
    silu_gate = gate * gate_sigmoid
    activ = (silu_gate * up_proj).astype(jnp.bfloat16)
    grad_act = product(grad_rows, wide_down, True)
    grad_gate = (grad_act * up_proj * gate_sigmoid * (1.0 + gate * (1.0 - gate_sigmoid))).astype(
        jnp.bfloat16
    )
    grad_up = (grad_act * silu_gate).astype(jnp.bfloat16)
    grad_normed_two = scatter_tokens(
        product(grad_gate, wide_gate, True) + product(grad_up, wide_up, True)
    )
    result = hidden + scatter_tokens(product(activ, wide_down, False))
    output = col_exchange(result.astype(jnp.bfloat16), 1, 0)
    scaled_two = grad_normed_two * gain_ffn[None, :]
    center_two = jnp.mean(scaled_two * unit_two, axis=1)
    grad_hidden = own_tokens(grad_rows).astype(jnp.float32) + inverse_two[:, None] * (
        scaled_two - unit_two * center_two[:, None]
    )
    gain_part_two = jnp.sum(grad_normed_two * unit_two, axis=0)
    grad_hidden_rows = gather_tokens(grad_hidden.astype(jnp.bfloat16))
    weight_down = reduce_rows(activ, grad_rows)
    weight_gate = reduce_columns(normed_two, grad_gate)
    weight_up = reduce_columns(normed_two, grad_up)

    grad_attended = product(grad_hidden_rows, wide_output, True).astype(jnp.bfloat16)
    weight_out = reduce_rows(attended_low, grad_hidden_rows)
    grad_queries, grad_keys, grad_values = attention_backward(
        queries, keys, values, grad_attended, log_totals, prefix_here, seq_len
    )
    grad_queries = rotate(grad_queries, cosine, -sine).astype(jnp.bfloat16)
    grad_keys = rotate(grad_keys, cosine, -sine).astype(jnp.bfloat16)
    grad_values = grad_values.astype(jnp.bfloat16)
    partial_one = (
        product(grad_queries, wide_query, True)
        + product(grad_keys, wide_key, True)
        + product(grad_values, wide_value, True)
    )
    center_part = jnp.sum(partial_one * gain_attn[None, :] * unit_one, axis=1)
    gain_part_one = jnp.sum(partial_one * unit_one, axis=0)
    parts = jnp.stack(jnp.split(partial_one.astype(jnp.bfloat16), cols, axis=1))
    grad_normed_one = jnp.sum(
        lax.all_to_all(parts, "col", 0, 0, tiled=True).astype(jnp.float32), axis=0
    )
    weight_query = reduce_columns(normed_one, grad_queries)
    weight_key = reduce_columns(normed_one, grad_keys)
    weight_value = reduce_columns(normed_one, grad_values)
    center_one = lax.psum(center_part, "col") / depth
    gain_one, gain_two = lax.psum((gain_part_one, gain_part_two), ("dp", "row", "col"))

    def own_features(array, axis):
        width = array.shape[axis] // cols
        return lax.dynamic_slice_in_dim(array, col_index * width, width, axis)

    grad_tokens = own_features(grad_hidden_rows, 1).astype(jnp.float32) + inverse_one[:, None] * (
        grad_normed_one * own_features(gain_attn, 0)[None, :]
        - own_features(unit_one, 1) * center_one[:, None]
    )
    return (
        output,
        grad_tokens.astype(jnp.bfloat16),
        weight_query,
        weight_key,
        weight_value,
        weight_out,
        weight_gate,
        weight_up,
        weight_down,
        own_features(gain_one, 0),
        own_features(gain_two, 0),
    )


def solution(mesh):
    in_specs = (
        P(("dp", "row"), "col"),
        P("col", "row"),
        P("col", "row"),
        P("col", "row"),
        P("row", "col"),
        P("col", "row"),
        P("col", "row"),
        P("row", "col"),
        P("col"),
        P("col"),
        P(("dp", "col")),
        P(("dp", "row"), "col"),
    )
    out_specs = (
        P(("dp", "row"), "col"),
        P(("dp", "row"), "col"),
        P("col", "row"),
        P("col", "row"),
        P("col", "row"),
        P("row", "col"),
        P("col", "row"),
        P("col", "row"),
        P("row", "col"),
        P("col"),
        P("col"),
    )

    def step(*arrays):
        tokens, prefix_len = arrays[0], arrays[10]
        sequence_each = prefix_len.shape[0] == mesh.shape["dp"] * mesh.shape["row"]
        square = mesh.shape["dp"] == 2 and mesh.shape["row"] == 4 and mesh.shape["col"] == 4
        body = per_device if sequence_each and square else per_device_general
        return jax.shard_map(
            body, mesh=mesh, in_specs=in_specs, out_specs=out_specs, check_vma=False
        )(*arrays)

    return step
```

```python
import jax
import jax.numpy as jnp
from jax import lax
from jax.experimental import pallas as pl
from jax.experimental.pallas import tpu as pltpu
from jax.sharding import PartitionSpec as P

D = 2048
HEAD_DIM = 64


EPSILON = 1e-05
THETA = 130000.0


def feature_total(values):
    return lax.psum(jnp.sum(values, axis=1), "col")


def normalize(values):
    squares = feature_total(values * values)
    inverse_rms = lax.rsqrt(squares / D + EPSILON)
    return (values * inverse_rms[:, None], inverse_rms)


def norm_backward(grad_normed, unit_rows, inverse_rms, gain_row):
    scaled = grad_normed * gain_row[None, :]
    center = feature_total(scaled * unit_rows) / D
    grad_values = inverse_rms[:, None] * (scaled - unit_rows * center[:, None])
    return (grad_values, jnp.sum(grad_normed * unit_rows, axis=0))


def product(left, weight, transposed):
    if transposed:
        return lax.dot_general(
            left, weight, (((1,), (1,)), ((), ())), preferred_element_type=jnp.float32
        )
    return jnp.dot(left, weight, preferred_element_type=jnp.float32)


def outer_product(left, right):
    return lax.dot_general(
        left, right, (((0,), (0,)), ((), ())), preferred_element_type=jnp.float32
    )


def gather_rows(values):
    return lax.all_gather(values, "row", axis=0, tiled=True)


def gather_cols(values):
    return lax.all_gather(values, "col", axis=0, tiled=True)


def sum_to_cols(gathered, weight, transposed):
    row_count = gathered.shape[0] // lax.axis_size("col")

    def partial_term(offset_rows, length_rows):
        return product(gathered, weight, transposed)

    return lax.psum_scatter(
        partial_term(jnp.int32(0), row_count * lax.axis_size("col")).astype(jnp.bfloat16),
        "col",
        scatter_dimension=0,
        tiled=True,
    ).astype(jnp.float32)


def sum_to_rows(gathered, weight, transposed):
    row_count = gathered.shape[0] // lax.axis_size("row")

    def partial_term(offset_rows, length_rows):
        return product(gathered, weight, transposed)

    return lax.psum_scatter(
        partial_term(jnp.int32(0), row_count * lax.axis_size("row")).astype(jnp.bfloat16),
        "row",
        scatter_dimension=0,
        tiled=True,
    ).astype(jnp.float32)


def rope_tables(row_count, seq_len):
    half_dim = HEAD_DIM // 2
    places = (jnp.arange(row_count, dtype=jnp.int32) % seq_len).astype(jnp.float32)
    rates = THETA ** (-2.0 * jnp.arange(half_dim, dtype=jnp.float32) / HEAD_DIM)
    angles = places[:, None] * rates[None, :]
    return (jnp.cos(angles), jnp.sin(angles))


def rotate(values, cosine, sine):
    row_count = values.shape[0]
    shaped = values.reshape(row_count, -1, HEAD_DIM)
    half_dim = HEAD_DIM // 2
    first_half = shaped[:, :, :half_dim]
    second_half = shaped[:, :, half_dim:]
    cosine_rows = cosine[:, None, :]
    sine_rows = sine[:, None, :]
    turned = jnp.concatenate(
        [
            first_half * cosine_rows - second_half * sine_rows,
            second_half * cosine_rows + first_half * sine_rows,
        ],
        axis=2,
    )
    return turned.reshape(row_count, -1)


def visible_keys(first_row, block_rows, seq_len, prefix_here):
    query_place = first_row + jnp.arange(block_rows, dtype=jnp.int32)
    key_place = jnp.arange(seq_len, dtype=jnp.int32)
    return (key_place[None, :] <= query_place[:, None]) | (key_place[None, :] < prefix_here)


def attention_forward(queries, keys, values, prefix_len, seq_len):
    row_count = queries.shape[0]
    heads_here = queries.shape[1] // HEAD_DIM
    block_rows = min(512, seq_len)
    per_sequence = seq_len // block_rows
    query_blocks = queries.reshape(row_count // block_rows, block_rows, heads_here, HEAD_DIM)
    key_seqs = keys.reshape(row_count // seq_len, seq_len, heads_here, HEAD_DIM)
    value_seqs = values.reshape(row_count // seq_len, seq_len, heads_here, HEAD_DIM)
    factor = HEAD_DIM ** (-0.5)
    numbers = jnp.arange(row_count // block_rows, dtype=jnp.int32)

    def one_block(inputs):
        query_block, number = inputs
        sequence = number // per_sequence
        first_row = number % per_sequence * block_rows
        key_seq = lax.dynamic_index_in_dim(key_seqs, sequence, 0, keepdims=False)
        value_seq = lax.dynamic_index_in_dim(value_seqs, sequence, 0, keepdims=False)
        prefix_here = lax.dynamic_index_in_dim(prefix_len, sequence, 0, keepdims=False)
        scores = (
            jnp.einsum("qhd,khd->hqk", query_block, key_seq, preferred_element_type=jnp.float32)
            * factor
        )
        visible = visible_keys(first_row, block_rows, seq_len, prefix_here)
        exponent = jnp.where(visible[None], jnp.exp(scores), 0.0)
        totals = jnp.sum(exponent, axis=2)
        probabilities = (exponent / totals[:, :, None]).astype(jnp.bfloat16)
        attended = jnp.einsum(
            "hqk,khd->qhd", probabilities, value_seq, preferred_element_type=jnp.float32
        )
        return (attended.reshape(block_rows, heads_here * HEAD_DIM), jnp.log(totals))

    attended, log_totals = lax.map(one_block, (query_blocks, numbers))
    return (attended.reshape(row_count, -1), log_totals)


def attention_backward(queries, keys, values, grad_attended, log_totals, prefix_len, seq_len):
    row_count = queries.shape[0]
    heads_here = queries.shape[1] // HEAD_DIM
    block_rows = min(512, seq_len)
    per_sequence = seq_len // block_rows
    query_blocks = queries.reshape(row_count // block_rows, block_rows, heads_here, HEAD_DIM)
    grad_blocks = grad_attended.reshape(row_count // block_rows, block_rows, heads_here, HEAD_DIM)
    key_seqs = keys.reshape(row_count // seq_len, seq_len, heads_here, HEAD_DIM)
    value_seqs = values.reshape(row_count // seq_len, seq_len, heads_here, HEAD_DIM)
    factor = HEAD_DIM ** (-0.5)
    numbers = jnp.arange(row_count // block_rows, dtype=jnp.int32)
    zero_seqs = jnp.zeros(key_seqs.shape, jnp.float32)

    def one_block(carry, inputs):
        grad_key_seqs, grad_value_seqs = carry
        query_block, grad_block, log_block, number = inputs
        sequence = number // per_sequence
        first_row = number % per_sequence * block_rows
        key_seq = lax.dynamic_index_in_dim(key_seqs, sequence, 0, keepdims=False)
        value_seq = lax.dynamic_index_in_dim(value_seqs, sequence, 0, keepdims=False)
        prefix_here = lax.dynamic_index_in_dim(prefix_len, sequence, 0, keepdims=False)
        scores = (
            jnp.einsum("qhd,khd->hqk", query_block, key_seq, preferred_element_type=jnp.float32)
            * factor
        )
        visible = visible_keys(first_row, block_rows, seq_len, prefix_here)
        probabilities = jnp.where(visible[None], jnp.exp(scores - log_block[:, :, None]), 0.0)
        grad_probs = jnp.einsum(
            "qhd,khd->hqk", grad_block, value_seq, preferred_element_type=jnp.float32
        )
        center = jnp.sum(probabilities * grad_probs, axis=2)
        grad_scores = (probabilities * (grad_probs - center[:, :, None]) * factor).astype(
            jnp.bfloat16
        )
        grad_query = jnp.einsum(
            "hqk,khd->qhd", grad_scores, key_seq, preferred_element_type=jnp.float32
        )
        grad_key = jnp.einsum(
            "hqk,qhd->khd", grad_scores, query_block, preferred_element_type=jnp.float32
        )
        grad_value = jnp.einsum(
            "hqk,qhd->khd",
            probabilities.astype(jnp.bfloat16),
            grad_block,
            preferred_element_type=jnp.float32,
        )
        grad_key_seqs = lax.dynamic_update_index_in_dim(
            grad_key_seqs,
            lax.dynamic_index_in_dim(grad_key_seqs, sequence, 0, keepdims=False) + grad_key,
            sequence,
            0,
        )
        grad_value_seqs = lax.dynamic_update_index_in_dim(
            grad_value_seqs,
            lax.dynamic_index_in_dim(grad_value_seqs, sequence, 0, keepdims=False) + grad_value,
            sequence,
            0,
        )
        return (
            (grad_key_seqs, grad_value_seqs),
            grad_query.reshape(block_rows, heads_here * HEAD_DIM),
        )

    carried, grad_queries = lax.scan(
        one_block, (zero_seqs, zero_seqs), (query_blocks, grad_blocks, log_totals, numbers)
    )
    grad_key_seqs, grad_value_seqs = carried
    return (
        grad_queries.reshape(row_count, -1),
        grad_key_seqs.reshape(row_count, -1),
        grad_value_seqs.reshape(row_count, -1),
    )


def per_device_general(
    tokens,
    w_query,
    w_key,
    w_value,
    w_output,
    w_gate,
    w_up,
    w_down,
    norm_attn,
    norm_ffn,
    prefix_len,
    cotangent,
):
    width_attn = w_query.shape[1]
    width_ffn = w_gate.shape[1]
    inputs = tokens.astype(jnp.float32)
    gain_attn = norm_attn.astype(jnp.float32)
    gain_ffn = norm_ffn.astype(jnp.float32)
    unit_one, inverse_one = normalize(inputs)
    normed_one = (unit_one * gain_attn[None, :]).astype(jnp.bfloat16)
    rows_one = gather_rows(normed_one)
    w_attn = jnp.concatenate([w_query, w_key, w_value], axis=1)
    projected = sum_to_cols(rows_one, w_attn, False)
    row_count = projected.shape[0]
    seq_len = row_count // prefix_len.shape[0]
    cosine, sine = rope_tables(row_count, seq_len)
    queries = rotate(projected[:, :width_attn], cosine, sine).astype(jnp.bfloat16)
    keys = rotate(projected[:, width_attn : 2 * width_attn], cosine, sine).astype(jnp.bfloat16)
    values = projected[:, 2 * width_attn :].astype(jnp.bfloat16)
    attended, log_totals = attention_forward(queries, keys, values, prefix_len, seq_len)
    attended_low = attended.astype(jnp.bfloat16)
    attended_rows = gather_cols(attended_low)
    hidden = inputs + sum_to_rows(attended_rows, w_output, False)
    unit_two, inverse_two = normalize(hidden)
    normed_two = (unit_two * gain_ffn[None, :]).astype(jnp.bfloat16)
    rows_two = gather_rows(normed_two)
    w_pair = jnp.concatenate([w_gate, w_up], axis=1)
    gate_up = sum_to_cols(rows_two, w_pair, False)
    gate = gate_up[:, :width_ffn]
    up_proj = gate_up[:, width_ffn:]
    gate_sigmoid = jax.nn.sigmoid(gate)
    silu_gate = gate * gate_sigmoid
    activ = (silu_gate * up_proj).astype(jnp.bfloat16)
    act_rows = gather_cols(activ)
    result = hidden + sum_to_rows(act_rows, w_down, False)
    output = result.astype(jnp.bfloat16)
    grad_rows = gather_rows(cotangent)
    grad_act = sum_to_cols(grad_rows, w_down, True)
    grad_gate = grad_act * up_proj * gate_sigmoid * (1.0 + gate * (1.0 - gate_sigmoid))
    grad_up = grad_act * silu_gate
    grad_pair = jnp.concatenate([grad_gate, grad_up], axis=1).astype(jnp.bfloat16)
    grad_pair_rows = gather_cols(grad_pair)
    grad_normed_two = sum_to_rows(grad_pair_rows, w_pair, True)
    weight_pair = outer_product(rows_two, grad_pair_rows)
    weight_down = outer_product(act_rows, grad_rows)
    grad_from_two, gain_part_two = norm_backward(grad_normed_two, unit_two, inverse_two, gain_ffn)
    grad_hidden = cotangent.astype(jnp.float32) + grad_from_two
    grad_hidden_low = grad_hidden.astype(jnp.bfloat16)
    grad_hidden_rows = gather_rows(grad_hidden_low)
    grad_attended = sum_to_cols(grad_hidden_rows, w_output, True).astype(jnp.bfloat16)
    weight_out = outer_product(attended_rows, grad_hidden_rows)
    grad_queries, grad_keys, grad_values = attention_backward(
        queries, keys, values, grad_attended, log_totals, prefix_len, seq_len
    )
    grad_proj = jnp.concatenate(
        [rotate(grad_queries, cosine, -sine), rotate(grad_keys, cosine, -sine), grad_values], axis=1
    ).astype(jnp.bfloat16)
    grad_proj_rows = gather_cols(grad_proj)
    grad_normed_one = sum_to_rows(grad_proj_rows, w_attn, True)
    weight_attn = outer_product(rows_one, grad_proj_rows)
    weight_attn, weight_out, weight_pair, weight_down = (
        lax.psum(weight_attn.astype(jnp.bfloat16), "dp").astype(jnp.float32),
        lax.psum(weight_out.astype(jnp.bfloat16), "dp").astype(jnp.float32),
        lax.psum(weight_pair.astype(jnp.bfloat16), "dp").astype(jnp.float32),
        lax.psum(weight_down.astype(jnp.bfloat16), "dp").astype(jnp.float32),
    )
    grad_from_one, gain_part_one = norm_backward(grad_normed_one, unit_one, inverse_one, gain_attn)
    grad_tokens = (grad_hidden + grad_from_one).astype(jnp.bfloat16)
    gain_one, gain_two = lax.psum((gain_part_one, gain_part_two), ("dp", "row"))
    return (
        output,
        grad_tokens,
        weight_attn[:, :width_attn],
        weight_attn[:, width_attn : 2 * width_attn],
        weight_attn[:, 2 * width_attn :],
        weight_out,
        weight_pair[:, :width_ffn],
        weight_pair[:, width_ffn:],
        weight_down,
        gain_one,
        gain_two,
    )


MESH = pl.DeviceIdType.MESH
F32 = jnp.float32
BF16 = jnp.bfloat16
COLS = 4
ROW_Y = 2
ROW_CORE = 1
VMEM_LIMIT = 64 * 1024 * 1024 - 64 * 1024


def dot_nn(left, right):
    return lax.dot_general(left, right, (((1,), (0,)), ((), ())), preferred_element_type=F32)


def dot_nt(left, right):
    return lax.dot_general(left, right, (((1,), (1,)), ((), ())), preferred_element_type=F32)


def dot_tn(left, right):
    return lax.dot_general(left, right, (((0,), (0,)), ((), ())), preferred_element_type=F32)


class Place:
    def __init__(self):
        self.x = lax.axis_index("dp")
        self.r = lax.axis_index("row")
        self.z = lax.axis_index("col")

    def peer_z(self, z):
        return {"col": z}

    def partner(self, name):
        if name == "x":
            return {"dp": 1 - self.x}
        bit = ROW_Y if name == "y" else ROW_CORE
        low = lax.rem(lax.div(self.r, bit), 2)
        return {"row": self.r + bit * (1 - 2 * low)}

    def barrier(self):
        sem = pltpu.get_barrier_semaphore()
        for s in (1, 2, 3):
            pl.semaphore_signal(
                sem, 1, device_id=self.peer_z(lax.rem(self.z + s, COLS)), device_id_type=MESH
            )
        for name in ("x", "y", "core"):
            pl.semaphore_signal(sem, 1, device_id=self.partner(name), device_id_type=MESH)
        pl.semaphore_wait(sem, 6)


def remote(src, dst, send, recv, device):
    return pltpu.make_async_remote_copy(
        src_ref=src,
        dst_ref=dst,
        send_sem=send,
        recv_sem=recv,
        device_id=device,
        device_id_type=MESH,
    )


class LineGather:
    def __init__(self, place, buf, send, recv):
        self.place, self.buf, self.send, self.recv = place, buf, send, recv

    def copy(self, step, side):
        z = self.place.z
        block = z - step if side == 0 else z + step
        to = z + 1 if side == 0 else z - 1
        block = jnp.clip(block, 0, COLS - 1)
        to = jnp.clip(to, 0, COLS - 1)
        return remote(
            self.buf.at[block],
            self.buf.at[block],
            self.send.at[side, step],
            self.recv.at[side, step],
            self.place.peer_z(to),
        )

    def sends(self, step, side):
        z = self.place.z
        if side == 0:
            return jnp.logical_and(z - step >= 0, z + 1 < COLS)
        return jnp.logical_and(z + step < COLS, z >= 1)

    def gets(self, step, side):
        z = self.place.z
        if side == 0:
            return z - 1 - step >= 0
        return z + 1 + step < COLS

    def start(self, step):
        for side in (0, 1):

            @pl.when(self.sends(step, side))
            def _():
                self.copy(step, side).start()

    def wait_recv(self, step):
        for side in (0, 1):

            @pl.when(self.gets(step, side))
            def _():
                self.copy(step, side).wait_recv()

    def finish(self):
        for step in range(COLS - 1):
            for side in (0, 1):

                @pl.when(self.sends(step, side))
                def _():
                    self.copy(step, side).wait_send()


class LineSum:
    def __init__(self, place, parts, right, left, send, recv):
        self.place, self.parts = place, parts
        self.inbox = (right, left)
        self.send, self.recv = send, recv

    def copy(self, step, side):
        z = self.place.z
        d = COLS - 1 - step if side == 0 else step
        to = jnp.clip(z + 1 if side == 0 else z - 1, 0, COLS - 1)
        return remote(
            self.parts.at[d],
            self.inbox[side].at[step],
            self.send.at[side, step],
            self.recv.at[side, step],
            self.place.peer_z(to),
        )

    def hops(self, side):
        z = self.place.z
        return z if side == 0 else COLS - 1 - z

    def sends(self, step, side):
        return self.hops(side) < COLS - 1 - step

    def gets(self, step, side):
        hops = self.hops(side)
        return jnp.logical_and(hops > 0, hops <= COLS - 1 - step)

    def run_slot(self, t):
        for side in (0, 1):
            step = t - self.hops(side)
            valid = jnp.logical_and(step >= 0, step < COLS - 1)
            step = jnp.clip(step, 0, COLS - 2)
            d = COLS - 1 - step if side == 0 else step

            @pl.when(jnp.logical_and(valid, self.gets(step, side)))
            def _():
                self.copy(step, side).wait_recv()
                rows = self.parts.shape[1]

                @pl.loop(0, rows // 32)
                def _(i):
                    part = pl.ds(pl.multiple_of(i * 32, 32), 32)
                    total = self.parts[d, part, :].astype(F32) + self.inbox[side][
                        step, part, :
                    ].astype(F32)
                    self.parts[d, part, :] = total.astype(BF16)

            @pl.when(jnp.logical_and(valid, self.sends(step, side)))
            def _():
                self.copy(step, side).start()

    def finish(self):
        for step in range(COLS - 1):
            for side in (0, 1):

                @pl.when(self.sends(step, side))
                def _():
                    self.copy(step, side).wait_send()


class Widen:
    def __init__(self, place, index, source, slot, sems):
        self.place, self.index, self.source, self.slot = place, index, source, slot
        self.sems = sems

    def pair(self, stage, j):
        return self.sems.at[0, stage, self.index, j], self.sems.at[1, stage, self.index, j]

    def local(self):
        z = self.place.z
        return pltpu.make_async_copy(
            self.source(z, None), self.slot(0, z, None), self.sems.at[0, 5, self.index, 0]
        )

    def to_col(self, s):
        place = self.place
        peer = lax.rem(place.z + s, COLS)
        send, recv = self.pair(0, s)
        return remote(
            self.source(peer, place.x), self.slot(0, place.z, place.x), send, recv, place.peer_z(peer)
        )

    def origin(self, s):
        return lax.rem(self.place.z + COLS - s, COLS)

    def to_dp(self, s):
        ref = self.slot(0, self.origin(s), self.place.x)
        send, recv = self.pair(1, s)
        return remote(ref, ref, send, recv, self.place.partner("x"))

    def near(self, stage, s):
        origin = self.origin(s)
        send, recv = self.pair(stage, s)
        if stage == 4:
            src, dst = self.slot(2, origin, None), self.slot(3, origin, None)
        else:
            src = self.source(self.place.z, None) if s == 0 else self.slot(0, origin, None)
            dst = self.slot(2 if stage == 2 else 1, origin, None)
        return remote(src, dst, send, recv, self.place.partner("y" if stage == 2 else "core"))

    def start(self):
        self.local().start()
        for s in (2, 1, 3):
            self.to_col(s).start()
        self.near(2, 0).start()
        self.near(3, 0).start()

    def pass_dp(self, s):
        self.to_col(s).wait_recv()
        self.to_dp(s).start()

    def pass_near(self, s):
        self.to_dp(s).wait_recv()
        self.near(2, s).start()
        self.near(3, s).start()

    def pass_far(self, s):
        self.near(2, s).wait_recv()
        self.near(4, s).start()

    def arrived(self):
        self.local().wait()
        for s in range(COLS):
            self.near(3, s).wait_recv()
            self.near(4, s).wait_recv()

    def finish(self):
        for s in range(COLS):
            if s:
                self.to_col(s).wait_send()
                self.to_dp(s).wait_send()
            for stage in (2, 3, 4):
                self.near(stage, s).wait_send()


def swap_halves(values):
    lane = lax.broadcasted_iota(jnp.int32, values.shape, 1)
    up = pltpu.roll(values, 96, 1)
    down = pltpu.roll(values, 32, 1)
    return jnp.where(lax.rem(lane, 64) < 32, up, down)


def half_lanes(values, h):
    lane = lax.broadcasted_iota(jnp.int32, values.shape, 1)
    return jnp.where((lane >= 64) == bool(h), values, jnp.zeros_like(values))


def visible_block(first, rows, keys, prefix):
    query = first + lax.broadcasted_iota(jnp.int32, (rows, keys), 0)
    key = lax.broadcasted_iota(jnp.int32, (rows, keys), 1)
    return jnp.logical_or(key <= query, key < prefix)


def weight_paths(place, sems, w_refs, wide_refs):
    wqkv, wo, wg, wu, wd = w_refs
    vqkv, vo, vg, vu, vd = wide_refs

    def rows_of(first, size, half):
        if half is None:
            return pl.ds(pl.multiple_of(first, 64), size)
        return pl.ds(pl.multiple_of(first + half * (size // 2), 64), size // 2)

    def columns(p, width):
        return pl.ds(pl.multiple_of(p * width, 128), width)

    paths = [
        Widen(
            place,
            0,
            lambda p, h: wqkv.at[:, rows_of(0, 512, h), columns(p, 128)],
            lambda k, j, h: vqkv.at[k, j, :, rows_of(0, 512, h), :],
            sems,
        ),
        Widen(
            place,
            1,
            lambda p, h: wo.at[rows_of(p * 128, 128, h), :],
            lambda k, j, h: vo.at[k, j, rows_of(0, 128, h), :],
            sems,
        ),
    ]
    for i, (w, v) in enumerate(((wg, vg), (wu, vu))):
        paths.append(
            Widen(
                place,
                2 + i,
                lambda p, h, w=w: w.at[rows_of(0, 512, h), columns(p, 512)],
                lambda k, j, h, v=v: v.at[k, j, rows_of(0, 512, h), :],
                sems,
            )
        )
    paths.append(
        Widen(
            place,
            4,
            lambda p, h: wd.at[rows_of(p * 512, 512, h), :],
            lambda k, j, h: vd.at[k, j, rows_of(0, 512, h), :],
            sems,
        )
    )
    return paths


def forward_kernel(
    xin,
    wqkv,
    wo,
    wg,
    wu,
    wd,
    cosine,
    sine,
    prefix,
    xg,
    normed_one,
    q_out,
    k_out,
    v_out,
    att,
    hidden,
    normed_two,
    gains,
    inverse_one,
    vqkv,
    vo,
    vg,
    vu,
    vd,
    parts,
    inbox_r,
    inbox_l,
    acc,
    sems,
    line_sems,
    local_sem,
):
    place = Place()
    z = place.z
    place.barrier()
    own = pltpu.make_async_copy(xin, xg.at[z], local_sem.at[0])
    own.start()
    own.wait()
    gather_x = LineGather(place, xg, line_sems.at[0, 0], line_sems.at[0, 1])
    gather_x.start(0)
    qkv, out, gate, up, down = weight_paths(
        place, sems, (wqkv, wo, wg, wu, wd), (vqkv, vo, vg, vu, vd)
    )
    qkv.start()
    out.start()
    gather_x.wait_recv(0)
    gather_x.start(1)
    for s in (1, 3, 2):
        qkv.pass_dp(s)
    gather_x.wait_recv(1)
    gather_x.start(2)
    qkv.pass_far(0)
    out.pass_far(0)
    for s in (1, 3, 2):
        out.pass_dp(s)
        qkv.pass_near(s)
    gate.start()
    up.start()
    for s in (1, 3, 2):
        out.pass_near(s)
    gather_x.wait_recv(2)

    @pl.loop(0, 16)
    def _(i):
        part = pl.ds(pl.multiple_of(i * 32, 32), 32)
        blocks = [xg[j, part, :].astype(F32) for j in range(COLS)]
        squares = sum(jnp.sum(b * b, axis=1, keepdims=True) for b in blocks)
        inverse = lax.rsqrt(squares / D + EPSILON)
        inverse_one[part, :] = jnp.broadcast_to(inverse, (32, 128))
        for j in range(COLS):
            gain = xg[j, 512:513, :].astype(F32)
            normed_one[part, j * 512 : (j + 1) * 512] = (blocks[j] * inverse * gain).astype(BF16)

    for j in range(COLS):
        gains[j] = xg[j, 512:528, :]
    for s in (1, 3, 2):
        qkv.pass_far(s)
    qkv.arrived()
    down.start()

    for w in range(3):
        for pair in range(2):
            wide = jnp.concatenate(
                [vqkv[2 * pair + i, :, w].reshape(D, 128) for i in range(2)], axis=1
            )
            acc[:, 0:256] = dot_nn(normed_one[...], wide)
            for i in range(2):
                k = 2 * pair + i
                block = acc[:, i * 128 : (i + 1) * 128]
                if w < 2:
                    block = block * cosine[...] + swap_halves(block) * sine[...]
                (q_out, k_out, v_out)[w][k] = block.astype(BF16)
    for s in (1, 3, 2):
        out.pass_far(s)
    gate.pass_far(0)
    up.pass_far(0)
    down.pass_far(0)

    reach = prefix[0]
    for k in range(COLS):
        for first, keys in ((0, 256), (256, 512)):
            queries = q_out[k, first : first + 256, :]
            visible = visible_block(first, 256, keys, reach)
            kept = None
            for h in range(2):
                scores = dot_nt(half_lanes(queries, h), k_out[k, 0:keys, :]) * (HEAD_DIM**-0.5)
                weights = jnp.where(visible, jnp.exp(scores), 0.0)
                probs = (weights / jnp.sum(weights, axis=1, keepdims=True)).astype(BF16)
                got = half_lanes(dot_nn(probs, v_out[k, 0:keys, :]), h)
                kept = got if kept is None else kept + got
            att[k, first : first + 256, :] = kept.astype(BF16)
        path = (gate, up, down, None)[k]
        if path is not None:
            for s in (1, 3, 2):
                path.pass_dp(s)

    out.arrived()
    attended = jnp.concatenate([att[k] for k in range(COLS)], axis=1)
    for j in range(COLS):
        piece = dot_nn(attended, vo[:, j].reshape(512, 512))
        parts[:, :, j * 512 : (j + 1) * 512] = piece.astype(BF16).reshape(COLS, 128, 512)
    total = LineSum(place, parts, inbox_r, inbox_l, line_sems.at[1, 0], line_sems.at[1, 1])
    total.run_slot(0)
    total.run_slot(1)
    for s in (1, 3, 2):
        gate.pass_near(s)
    total.run_slot(2)
    for s in (1, 3, 2):
        up.pass_near(s)
    total.run_slot(3)

    @pl.loop(0, 4)
    def _(i):
        part = pl.ds(pl.multiple_of(i * 32, 32), 32)
        rows = pl.ds(pl.multiple_of(z * 128 + i * 32, 32), 32)
        squares = jnp.zeros((32, 1), F32)
        for j in range(COLS):
            lanes = slice(j * 512, (j + 1) * 512)
            value = parts[z, part, lanes].astype(F32) + xg[j, rows, :].astype(F32)
            hidden[part, lanes] = value
            squares += jnp.sum(value * value, axis=1, keepdims=True)
        inverse = lax.rsqrt(squares / D + EPSILON)
        for j in range(COLS):
            lanes = slice(j * 512, (j + 1) * 512)
            gain = xg[j, 513:514, :].astype(F32)
            normed_two[z, part, lanes] = (hidden[part, lanes] * inverse * gain).astype(BF16)

    gather_n = LineGather(place, normed_two, line_sems.at[2, 0], line_sems.at[2, 1])
    gather_n.start(0)
    for s in (1, 3, 2):
        gate.pass_far(s)
        down.pass_near(s)
    gather_n.wait_recv(0)
    gather_n.start(1)
    for s in (1, 3, 2):
        up.pass_far(s)
    gather_n.wait_recv(1)
    gather_n.start(2)
    for s in (1, 3, 2):
        down.pass_far(s)
    gather_n.wait_recv(2)
    for path in (gate, up, down):
        path.arrived()
    for path in (qkv, out, gate, up, down):
        path.finish()
    gather_x.finish()
    total.finish()
    gather_n.finish()


def forward_half(xin, wqkv, wo, wg, wu, wd, cosine, sine, prefix):
    vmem = pl.BlockSpec(memory_space=pltpu.VMEM)
    hbm = pl.BlockSpec(memory_space=pl.ANY)
    shape = jax.ShapeDtypeStruct
    return pl.pallas_call(
        forward_kernel,
        name="forward_half",
        out_shape=[
            shape((4, 528, 512), BF16),
            shape((512, D), BF16),
            shape((4, 512, 128), BF16),
            shape((4, 512, 128), BF16),
            shape((4, 512, 128), BF16),
            shape((4, 512, 128), BF16),
            shape((128, D), F32),
            shape((4, 128, D), BF16),
            shape((4, 16, 512), BF16),
            shape((512, 128), F32),
            shape((4, 4, 3, 512, 128), BF16),
            shape((4, 4, 128, 512), BF16),
            shape((4, 4, 512, 512), BF16),
            shape((4, 4, 512, 512), BF16),
            shape((4, 4, 512, 512), BF16),
        ],
        in_specs=[vmem, hbm, hbm, hbm, hbm, hbm, vmem, vmem, pl.BlockSpec(memory_space=pltpu.SMEM)],
        out_specs=[vmem] * 12 + [hbm] * 3,
        scratch_shapes=[
            pltpu.VMEM((4, 128, D), BF16),
            pltpu.VMEM((3, 128, D), BF16),
            pltpu.VMEM((3, 128, D), BF16),
            pltpu.VMEM((512, 256), F32),
            pltpu.SemaphoreType.DMA((2, 6, 5, 4)),
            pltpu.SemaphoreType.DMA((3, 2, 2, 3)),
            pltpu.SemaphoreType.DMA((1,)),
        ],
        compiler_params=pltpu.CompilerParams(
            collective_id=1, has_side_effects=True, vmem_limit_bytes=VMEM_LIMIT
        ),
    )(xin, wqkv, wo, wg, wu, wd, cosine, sine, prefix)


def feed_forward_kernel(
    cot,
    n2,
    hidden,
    gains,
    vg_hbm,
    vu_hbm,
    vd_hbm,
    dh,
    orow,
    gain_part,
    mine,
    give,
    far,
    near,
    cg,
    vg,
    vu,
    vd,
    gate_s,
    up_s,
    act,
    dgate,
    dup,
    pout,
    box_or,
    box_ol,
    parts,
    box_r,
    box_l,
    tiles,
    adds,
    load_sems,
    line_sems,
    near_sems,
    tile_sems,
    add_sems,
    y_sems,
    local_sem,
):
    place = Place()
    z = place.z
    loads = []
    for i, (src, dst) in enumerate(((vg_hbm, vg), (vu_hbm, vu), (vd_hbm, vd))):
        for k in range(COLS):
            loads.append(pltpu.make_async_copy(src.at[k], dst.at[k], load_sems.at[i, k]))
    for k in range(COLS):
        loads[k].start()
        loads[COLS + k].start()
    for k in range(COLS):
        loads[2 * COLS + k].start()
    place.barrier()
    own = pltpu.make_async_copy(cot, cg.at[z], local_sem.at[0])
    own.start()
    own.wait()
    gather_c = LineGather(place, cg, line_sems.at[0, 0], line_sems.at[0, 1])
    gather_c.start(0)

    for k in range(COLS):
        loads[k].wait()
        loads[COLS + k].wait()
        rows = n2[...].reshape(512, D)
        gate_s[k] = dot_nn(rows, vg[k].reshape(D, 512))
        up_s[k] = dot_nn(rows, vu[k].reshape(D, 512))

        @pl.loop(0, 16)
        def _(i):
            part = pl.ds(pl.multiple_of(i * 32, 32), 32)
            gate = gate_s[k, part, :]
            act[k, part, :] = (gate * jax.nn.sigmoid(gate) * up_s[k, part, :]).astype(BF16)

        if k == 2:
            gather_c.wait_recv(0)
            gather_c.start(1)
    for k in range(COLS):
        loads[2 * COLS + k].wait()

    for j in range(COLS):
        wide = jnp.concatenate([act[k] for k in range(COLS)], axis=1)
        piece = dot_nn(wide, vd[:, j].reshape(D, 512))
        pout[:, :, j * 512 : (j + 1) * 512] = piece.astype(BF16).reshape(COLS, 128, 512)
    gather_c.wait_recv(1)
    gather_c.start(2)
    out_sum = LineSum(place, pout, box_or, box_ol, line_sems.at[1, 0], line_sems.at[1, 1])
    out_sum.run_slot(0)
    gather_c.wait_recv(2)

    def left_of(w, k, j):
        return act[k] if w == 0 else n2[:, :, pl.ds(pl.multiple_of(j * 512, 512), 512)].reshape(512, 512)

    def right_of(w, k, j):
        return cg[j] if w == 0 else (dgate, dup)[w - 1][k]

    def near_copy(w, t):
        slot = lax.rem(t, 2)
        return remote(
            tiles.at[slot],
            near.at[w, t],
            tile_sems.at[slot],
            near_sems.at[w, t],
            place.partner("core"),
        )

    def send_near(w, first):
        @pl.loop(0, 8)
        def _(t):
            k = 1 + 2 * lax.div(t, 4)
            j = lax.rem(t, 4)
            slot = lax.rem(t, 2)
            if first:

                @pl.when(t >= 2)
                def _():
                    near_copy(w, t).wait_send()
            else:
                near_copy(w, t).wait_send()
            tiles[slot] = dot_tn(left_of(w, k, j), right_of(w, k, j)).astype(BF16)
            near_copy(w, t).start()

    def fetch(w, t):
        slot = lax.rem(t, 2)
        return pltpu.make_async_copy(near.at[w, t], adds.at[slot], add_sems.at[0, slot])

    def settle(w, t):
        slot = lax.rem(t, 2)
        j = lax.rem(t, 4)
        to = mine if t < 4 else give
        return pltpu.make_async_copy(adds.at[2 + slot], to.at[w, j], add_sems.at[1, slot])

    def add_near(w, half):
        for j in range(COLS):
            t = 4 * half + j
            near_copy(w, t).wait_recv()
            fetch(w, t).start()
            if j >= 2:
                settle(w, t - 2).wait()
            fetch(w, t).wait()
            slot = t % 2
            k = 2 * half
            value = dot_tn(left_of(w, k, j), right_of(w, k, j)) + adds[slot].astype(F32)
            adds[2 + slot] = value.astype(BF16)
            settle(w, t).start()
        settle(w, 4 * half + 2).wait()
        settle(w, 4 * half + 3).wait()

    def y_copy(w, j):
        return remote(
            give.at[w, j], far.at[w, j], y_sems.at[0, w, j], y_sems.at[1, w, j], place.partner("y")
        )

    def send_far(w):
        for j in range(COLS):
            y_copy(w, j).start()

    send_near(0, True)
    out_sum.run_slot(1)

    for k in range(COLS):
        wide = jnp.concatenate([cg[j] for j in range(COLS)], axis=1)
        weight = jnp.concatenate([vd[k, j] for j in range(COLS)], axis=1)
        grad_act = dot_nt(wide, weight)
        for i in range(8):
            part = slice(i * 64, (i + 1) * 64)
            d_act = grad_act[part]
            gate = gate_s[k, part, :]
            sig = jax.nn.sigmoid(gate)
            dgate[k, part, :] = (
                d_act * up_s[k, part, :] * sig * (1.0 + gate * (1.0 - sig))
            ).astype(BF16)
            dup[k, part, :] = (d_act * gate * sig).astype(BF16)
        if k == 1:
            out_sum.run_slot(2)
    add_near(0, 1)
    send_far(0)

    for j in range(COLS):
        piece = dot_nt(
            jnp.concatenate([dgate[k] for k in range(COLS)], axis=1),
            jnp.concatenate([vg[k, j] for k in range(COLS)], axis=1),
        ) + dot_nt(
            jnp.concatenate([dup[k] for k in range(COLS)], axis=1),
            jnp.concatenate([vu[k, j] for k in range(COLS)], axis=1),
        )
        parts[:, :, j * 512 : (j + 1) * 512] = piece.astype(BF16).reshape(COLS, 128, 512)
    total = LineSum(place, parts, box_r, box_l, line_sems.at[2, 0], line_sems.at[2, 1])
    out_sum.run_slot(3)
    total.run_slot(0)
    send_near(1, False)
    total.run_slot(1)
    add_near(1, 1)
    send_far(1)
    send_near(2, False)
    total.run_slot(2)
    add_near(0, 0)
    total.run_slot(3)

    gain_part[...] = jnp.zeros((8, D), F32)

    @pl.loop(0, 4)
    def _(i):
        part = pl.ds(pl.multiple_of(i * 32, 32), 32)
        rows = pl.ds(pl.multiple_of(z * 128 + i * 32, 32), 32)
        squares = jnp.zeros((32, 1), F32)
        center = jnp.zeros((32, 1), F32)
        for j in range(COLS):
            lanes = slice(j * 512, (j + 1) * 512)
            value = hidden[part, lanes]
            squares += jnp.sum(value * value, axis=1, keepdims=True)
        inverse = lax.rsqrt(squares / D + EPSILON)
        for j in range(COLS):
            lanes = slice(j * 512, (j + 1) * 512)
            grad = parts[z, part, lanes].astype(F32)
            unit = hidden[part, lanes] * inverse
            center += jnp.sum(grad * gains[j, 1:2, :].astype(F32) * unit, axis=1, keepdims=True)
            gain_part[0:1, lanes] += jnp.sum(grad * unit, axis=0, keepdims=True)
        center = center / D
        for j in range(COLS):
            lanes = slice(j * 512, (j + 1) * 512)
            grad = parts[z, part, lanes].astype(F32)
            unit = hidden[part, lanes] * inverse
            scaled = grad * gains[j, 1:2, :].astype(F32)
            value = cg[j, rows, :].astype(F32) + inverse * (scaled - unit * center)
            dh[z, part, lanes] = value.astype(BF16)
            orow[j, part, :] = (hidden[part, lanes] + pout[z, part, lanes].astype(F32)).astype(BF16)

    gather_h = LineGather(place, dh, line_sems.at[3, 0], line_sems.at[3, 1])
    gather_h.start(0)
    add_near(1, 0)
    gather_h.wait_recv(0)
    gather_h.start(1)
    add_near(2, 1)
    gather_h.wait_recv(1)
    gather_h.start(2)
    add_near(2, 0)
    gather_h.wait_recv(2)
    for w in range(2):
        for j in range(COLS):
            y_copy(w, j).wait_recv()
    for w in range(2):
        for j in range(COLS):
            y_copy(w, j).wait_send()
    for t in range(6, 8):
        near_copy(2, t).wait_send()
    for line in (gather_c, out_sum, total, gather_h):
        line.finish()


def feed_forward(cot, n2, hidden, gains, vg, vu, vd):
    vmem = pl.BlockSpec(memory_space=pltpu.VMEM)
    hbm = pl.BlockSpec(memory_space=pl.ANY)
    shape = jax.ShapeDtypeStruct
    dma = pltpu.SemaphoreType.DMA
    return pl.pallas_call(
        feed_forward_kernel,
        name="feed_forward",
        out_shape=[
            shape((4, 128, D), BF16),
            shape((4, 128, 512), BF16),
            shape((8, D), F32),
            shape((3, 4, 512, 512), BF16),
            shape((3, 4, 512, 512), BF16),
            shape((2, 4, 512, 512), BF16),
            shape((3, 8, 512, 512), BF16),
        ],
        in_specs=[hbm, vmem, vmem, vmem, hbm, hbm, hbm],
        out_specs=[vmem, vmem, vmem, hbm, hbm, hbm, hbm],
        scratch_shapes=[
            pltpu.VMEM((4, 512, 512), BF16),
            pltpu.VMEM((4, 4, 512, 512), BF16),
            pltpu.VMEM((4, 4, 512, 512), BF16),
            pltpu.VMEM((4, 4, 512, 512), BF16),
            pltpu.VMEM((4, 512, 512), F32),
            pltpu.VMEM((4, 512, 512), F32),
            pltpu.VMEM((4, 512, 512), BF16),
            pltpu.VMEM((4, 512, 512), BF16),
            pltpu.VMEM((4, 512, 512), BF16),
            pltpu.VMEM((4, 128, D), BF16),
            pltpu.VMEM((3, 128, D), BF16),
            pltpu.VMEM((3, 128, D), BF16),
            pltpu.VMEM((4, 128, D), BF16),
            pltpu.VMEM((3, 128, D), BF16),
            pltpu.VMEM((3, 128, D), BF16),
            pltpu.VMEM((2, 512, 512), BF16),
            pltpu.VMEM((4, 512, 512), BF16),
            dma((3, 4)),
            dma((4, 2, 2, 3)),
            dma((3, 8)),
            dma((2,)),
            dma((2, 2)),
            dma((2, 2, 4)),
            dma((1,)),
        ],
        compiler_params=pltpu.CompilerParams(
            collective_id=2, has_side_effects=True, vmem_limit_bytes=VMEM_LIMIT
        ),
    )(cot, n2, hidden, gains, vg, vu, vd)


class Chain:
    def __init__(self, place, index, give, mine, far, side, final, sems, y_sems):
        self.place, self.index = place, index
        self.give, self.mine, self.far, self.side, self.final = give, mine, far, side, final
        self.sems, self.y_sems = sems, y_sems

    def remote(self, stage, j, src, dst, device):
        return remote(
            src, dst, self.sems.at[0, stage, self.index, j], self.sems.at[1, stage, self.index, j], device
        )

    def to_y(self, j):
        return remote(
            self.give.at[j],
            self.far.at[j],
            self.y_sems.at[0, self.index, j],
            self.y_sems.at[1, self.index, j],
            self.place.partner("y"),
        )

    def to_dp(self, j):
        return self.remote(
            0, j, self.mine.at[j, 1 - self.place.x], self.side.at[j], self.place.partner("x")
        )

    def to_col(self, s):
        place = self.place
        j = lax.rem(place.z + s, COLS)
        return self.remote(
            1, s, self.mine.at[j, place.x], self.final.at[place.z, place.x], place.peer_z(j)
        )

    def own(self):
        z, x = self.place.z, self.place.x
        return pltpu.make_async_copy(
            self.mine.at[z, x], self.final.at[z, x], self.sems.at[0, 1, self.index, 0]
        )

    def back(self, s):
        place = self.place
        origin = lax.rem(place.z + COLS - s, COLS)
        ref = self.final.at[origin, place.x]
        return self.remote(2, s, ref, ref, place.partner("x"))

    def start(self):
        for j in range(COLS):
            self.to_y(j).start()

    def level_dp(self, waits=True):
        x = self.place.x
        for j in range(COLS):
            if waits:
                self.to_y(j).wait_recv()
            for half in (1 - x, x):
                total = self.mine[j, half].astype(F32) + self.far[j, half].astype(F32)
                self.mine[j, half] = total.astype(BF16)
                if half is not x:
                    self.to_dp(j).start()

    def level_col(self):
        x = self.place.x
        for s in (2, 1, 3, 0):
            j = lax.rem(self.place.z + s, COLS)
            self.to_dp(j).wait_recv()
            total = self.mine[j, x].astype(F32) + self.side[j].astype(F32)
            self.mine[j, x] = total.astype(BF16)
            if s:
                self.to_col(s).start()
            else:
                self.own().start()

    def level_back(self):
        self.own().wait()
        self.back(0).start()
        for s in (1, 3, 2):
            self.to_col(s).wait_recv()
            self.back(s).start()

    def finish(self, waits=True):
        for s in range(COLS):
            self.back(s).wait_recv()
        for s in range(COLS):
            if waits:
                self.to_y(s).wait_send()
            self.to_dp(s).wait_send()
            if s:
                self.to_col(s).wait_send()
            self.back(s).wait_send()


def attention_grad_kernel(
    dh,
    att,
    q_in,
    k_in,
    v_in,
    vqkv,
    vo,
    normed_one,
    xg,
    inverse_one,
    gains,
    cosine,
    sine,
    prefix,
    orow,
    gain_two,
    mine_hbm,
    give_hbm,
    far_hbm,
    outg,
    gsum,
    small,
    final_f,
    final_a,
    final_o,
    datt,
    dqkv,
    acc,
    dk_acc,
    dv_acc,
    center,
    xb,
    parts,
    box_r,
    box_l,
    mine_f,
    far_f,
    side_f,
    away_a,
    near_a,
    give_a,
    mine_a,
    far_a,
    side_a,
    away_o,
    near_o,
    give_o,
    mine_o,
    far_o,
    side_o,
    msg,
    msg_in,
    swaps,
    load_sems,
    line_sems,
    chain_sems,
    y_sems,
    near_sems,
    msg_sems,
):
    place = Place()
    z = place.z
    loads = [pltpu.make_async_copy(mine_hbm.at[w], mine_f.at[w], load_sems.at[0, w]) for w in range(3)]
    loads += [pltpu.make_async_copy(far_hbm.at[w], far_f.at[w], load_sems.at[1, w]) for w in range(2)]
    for copy in loads:
        copy.start()
    place.barrier()
    chains = [
        Chain(
            place,
            w,
            give_hbm.at[w],
            mine_f.at[w],
            far_f.at[w],
            side_f.at[w],
            final_f.at[w],
            chain_sems,
            y_sems,
        )
        for w in range(3)
    ]
    down, gate, up = chains
    heads = Chain(place, 3, give_a, mine_a, far_a, side_a, final_a, chain_sems, y_sems)
    outs = Chain(place, 4, give_o, mine_o, far_o, side_o, final_o, chain_sems, y_sems)
    up.start()

    def out_copy(s):
        j = lax.rem(z + s, COLS)
        return remote(
            orow.at[j], outg.at[z], line_sems.at[1, 0, 0, s - 1], line_sems.at[1, 1, 0, s - 1], place.peer_z(j)
        )

    out_own = pltpu.make_async_copy(orow.at[z], outg.at[z], load_sems.at[2, 0])
    out_own.start()
    for s in (1, 2, 3):
        out_copy(s).start()

    rows = dh[...].reshape(512, D)
    wide = jnp.concatenate([vo[:, j].reshape(512, 512) for j in range(COLS)], axis=1)
    acc[...] = dot_nt(rows, wide)
    for k in range(COLS):
        datt[k] = acc[:, k * 128 : (k + 1) * 128].astype(BF16)

    loads[0].wait()
    loads[3].wait()
    down.level_dp(False)

    def near_piece(w, t):
        k = 1 + 2 * (t // 4)
        j = t % 4
        src, dst = ((away_a, near_a), (away_o, near_o))[w]
        return remote(
            src.at[t],
            dst.at[t],
            near_sems.at[0, w, t],
            near_sems.at[1, w, t],
            place.partner("core"),
        )

    def grad_piece(w, k, j):
        if w == 0:
            return dot_tn(normed_one[:, j * 512 : (j + 1) * 512], dqkv[k])
        return dot_tn(att[k], dh[:, :, j * 512 : (j + 1) * 512].reshape(512, 512))

    def send_near(w):
        for t in range(8):
            (away_a, away_o)[w][t] = grad_piece(w, 1 + 2 * (t // 4), t % 4).astype(BF16)
            near_piece(w, t).start()

    def add_near(w, half):
        for j in range(COLS):
            t = 4 * half + j
            value = grad_piece(w, 2 * half, j)
            near_piece(w, t).wait_recv()
            value = (value + (near_a, near_o)[w][t].astype(F32)).astype(BF16)
            to = ((mine_a, give_a), (mine_o, give_o))[w][half]
            to[j] = value.reshape(to.shape[1:])
        if half:
            (heads, outs)[w].start()

    send_near(1)

    reach = prefix[0]
    scale = HEAD_DIM**-0.5
    for k in range(COLS):
        dk_acc[...] = jnp.zeros((512, 128), F32)
        dv_acc[...] = jnp.zeros((512, 128), F32)
        for first, keys in ((0, 256), (256, 512)):
            part = slice(first, first + 256)
            visible = visible_block(first, 256, keys, reach)
            key_rows = k_in[k, 0:keys, :]
            value_rows = v_in[k, 0:keys, :]
            grad_q = None
            for h in range(2):
                query = half_lanes(q_in[k, part, :], h)
                grad = half_lanes(datt[k, part, :], h)
                scores = dot_nt(query, key_rows) * scale
                weights = jnp.where(visible, jnp.exp(scores), 0.0)
                probs = weights / jnp.sum(weights, axis=1, keepdims=True)
                grad_probs = dot_nt(grad, value_rows)
                middle = jnp.sum(probs * grad_probs, axis=1, keepdims=True)
                grad_scores = (probs * (grad_probs - middle) * scale).astype(BF16)
                got = half_lanes(dot_nn(grad_scores, key_rows), h)
                grad_q = got if grad_q is None else grad_q + got
                dk_acc[0:keys, :] += dot_tn(grad_scores, query)
                dv_acc[0:keys, :] += dot_tn(probs.astype(BF16), grad)
            turned = grad_q * cosine[part, :] - swap_halves(grad_q) * sine[part, :]
            dqkv[k, part, 0:128] = turned.astype(BF16)
        grad_k = dk_acc[...]
        dqkv[k, :, 128:256] = (grad_k * cosine[...] - swap_halves(grad_k) * sine[...]).astype(BF16)
        dqkv[k, :, 256:384] = dv_acc[...].astype(BF16)
        if k == 0:
            add_near(1, 1)
            loads[1].wait()
            loads[4].wait()
            gate.level_dp(False)
        if k == 1:
            down.level_col()
        if k == 2:
            add_near(1, 0)
            gate.level_col()
    send_near(0)

    center[...] = jnp.zeros((512, 128), F32)

    def block_copy(j):
        return pltpu.make_async_copy(xg.at[j], xb.at[j % 2], load_sems.at[3, j % 2])

    block_copy(0).start()
    wide_grad = jnp.concatenate([dqkv[k] for k in range(COLS)], axis=1)
    for j in range(COLS):
        if j < COLS - 1:
            block_copy(j + 1).start()
        weight = jnp.concatenate([vqkv[k, j, w] for k in range(COLS) for w in range(3)], axis=1)
        acc[...] = dot_nt(wide_grad, weight)
        block_copy(j).wait()
        msg[j] = jnp.zeros((8, 512), F32)
        gain = gains[j, 0:1, :].astype(F32)

        @pl.loop(0, 16)
        def _(i):
            part = pl.ds(pl.multiple_of(i * 32, 32), 32)
            grad = acc[part, :]
            unit = xb[j % 2, part, :].astype(F32) * inverse_one[part, 0:1]
            center[part, :] += jnp.broadcast_to(
                jnp.sum(grad * gain * unit, axis=1, keepdims=True), (32, 128)
            )
            msg[j, 1:2, :] += jnp.sum(grad * unit, axis=0, keepdims=True)
            parts[j, part, :] = grad.astype(BF16)

        msg[j, 2:3, :] = gain_two[0:1, j * 512 : (j + 1) * 512]
    total = LineSum(place, parts, box_r, box_l, line_sems.at[0, 0], line_sems.at[0, 1])
    total.run_slot(0)
    turned_center = jnp.transpose(center[...])
    for j in range(COLS):
        msg[j, 0:1, :] = turned_center[0:1, :]

    def msg_copy(s):
        j = lax.rem(z + s, COLS)
        return remote(
            msg.at[j], msg_in.at[s], msg_sems.at[0, s], msg_sems.at[1, s], place.peer_z(j)
        )

    for s in (1, 2, 3):
        msg_copy(s).start()
    add_near(0, 1)
    add_near(0, 0)
    total.run_slot(1)
    loads[2].wait()
    up.level_dp()
    total.run_slot(2)
    outs.level_dp()
    down.level_back()
    gate.level_back()
    total.run_slot(3)
    gsum[...] = parts[z].astype(F32)
    for s in (1, 2, 3):
        msg_copy(s).wait_recv()
    small[0] = msg[z] + msg_in[1] + msg_in[2] + msg_in[3]
    swaps[0] = small[0]

    def swap_copy(i):
        name = ("core", "y", "x")[i]
        return remote(
            swaps.at[2 * i], swaps.at[2 * i + 1], msg_sems.at[0, 4 + i], msg_sems.at[1, 4 + i], place.partner(name)
        )

    swap_copy(0).start()
    up.level_col()
    outs.level_col()
    heads.level_dp()
    swap_copy(0).wait_recv()
    swaps[2] = swaps[0] + swaps[1]
    swap_copy(1).start()
    up.level_back()
    outs.level_back()
    swap_copy(1).wait_recv()
    swaps[4] = swaps[2] + swaps[3]
    swap_copy(2).start()
    heads.level_col()
    heads.level_back()
    swap_copy(2).wait_recv()
    small[1] = swaps[4] + swaps[5]
    for i in range(3):
        swap_copy(i).wait_send()
    for s in (1, 2, 3):
        msg_copy(s).wait_send()
        out_copy(s).wait_recv()
        out_copy(s).wait_send()
    out_own.wait()
    for w in range(2):
        for t in range(8):
            near_piece(w, t).wait_send()
    down.finish(False)
    gate.finish(False)
    for chain in (up, outs, heads):
        chain.finish()
    total.finish()


def attention_grad(
    dh, att, q, k, v, vqkv, vo, normed_one, xg, inverse_one, gains, cosine, sine, prefix, orow, gain_two, mine, give, far
):
    vmem = pl.BlockSpec(memory_space=pltpu.VMEM)
    hbm = pl.BlockSpec(memory_space=pl.ANY)
    smem = pl.BlockSpec(memory_space=pltpu.SMEM)
    shape = jax.ShapeDtypeStruct
    dma = pltpu.SemaphoreType.DMA

    def buffers(rows, width):
        flat = (2 * rows, width)
        halves = (4, 2, rows, width)
        return [
            pltpu.VMEM((8,) + flat, BF16),
            pltpu.VMEM((8,) + flat, BF16),
            pltpu.VMEM(halves, BF16),
            pltpu.VMEM(halves, BF16),
            pltpu.VMEM(halves, BF16),
            pltpu.VMEM((4, rows, width), BF16),
        ]

    return pl.pallas_call(
        attention_grad_kernel,
        name="attention_grad",
        out_shape=[
            shape((4, 128, 512), BF16),
            shape((512, 512), F32),
            shape((2, 8, 512), F32),
            shape((3, 4, 2, 256, 512), BF16),
            shape((4, 2, 256, 384), BF16),
            shape((4, 2, 64, 512), BF16),
        ],
        in_specs=[vmem] * 8 + [hbm] + [vmem] * 4 + [smem] + [vmem] * 2 + [hbm] * 3,
        out_specs=[vmem, vmem, vmem, hbm, hbm, hbm],
        scratch_shapes=[
            pltpu.VMEM((4, 512, 128), BF16),
            pltpu.VMEM((4, 512, 384), BF16),
            pltpu.VMEM((512, 512), F32),
            pltpu.VMEM((512, 128), F32),
            pltpu.VMEM((512, 128), F32),
            pltpu.VMEM((512, 128), F32),
            pltpu.VMEM((2, 528, 512), BF16),
            pltpu.VMEM((4, 512, 512), BF16),
            pltpu.VMEM((3, 512, 512), BF16),
            pltpu.VMEM((3, 512, 512), BF16),
            pltpu.VMEM((3, 4, 2, 256, 512), BF16),
            pltpu.VMEM((3, 4, 2, 256, 512), BF16),
            pltpu.VMEM((3, 4, 256, 512), BF16),
        ]
        + buffers(256, 384)
        + buffers(64, 512)
        + [
            pltpu.VMEM((4, 8, 512), F32),
            pltpu.VMEM((4, 8, 512), F32),
            pltpu.VMEM((6, 8, 512), F32),
            dma((4, 4)),
            dma((2, 2, 2, 3)),
            dma((2, 3, 5, 4)),
            dma((2, 5, 4)),
            dma((2, 2, 8)),
            dma((2, 7)),
        ],
        compiler_params=pltpu.CompilerParams(
            collective_id=3, has_side_effects=True, vmem_limit_bytes=VMEM_LIMIT
        ),
    )(
        dh, att, q, k, v, vqkv, vo, normed_one, xg, inverse_one, gains, cosine, sine, prefix, orow, gain_two,
        mine.reshape(3, 4, 2, 256, 512), give.reshape(3, 4, 2, 256, 512), far.reshape(2, 4, 2, 256, 512),
    )


def per_device(
    tokens,
    w_query,
    w_key,
    w_value,
    w_output,
    w_gate,
    w_up,
    w_down,
    norm_attn,
    norm_ffn,
    prefix_len,
    cotangent,
):
    rows = lax.axis_size("row")
    cols = lax.axis_size("col")
    seq_len = tokens.shape[0]
    width = tokens.shape[1]
    col_index = lax.axis_index("col")

    prefix_here = lax.ppermute(
        prefix_len,
        ("row", "col"),
        [(c * cols + r, r * cols + c) for r in range(rows) for c in range(cols)],
    )
    xin = jnp.concatenate(
        [tokens, norm_attn[None], norm_ffn[None], jnp.zeros((14, width), BF16)], axis=0
    )
    cosine, sine = rope_tables(seq_len, seq_len)
    cos_wide = jnp.concatenate([cosine] * 4, axis=1)
    sin_wide = jnp.concatenate([-sine, sine] * 2, axis=1)
    (xg, normed_one, q4, k4, v4, att4, hidden, n2, gains, inverse_one, vqkv, vo, vg, vu, vd) = forward_half(
        xin,
        jnp.stack([w_query, w_key, w_value]),
        w_output,
        w_gate,
        w_up,
        w_down,
        cos_wide,
        sin_wide,
        prefix_here,
    )
    dh, orow, gain_two, mine, give, far, _ = feed_forward(cotangent, n2, hidden, gains, vg, vu, vd)
    outg, gsum, small, final_f, final_a, final_o = attention_grad(
        dh, att4, q4, k4, v4, vqkv, vo, normed_one, xg, inverse_one, gains, cos_wide, sin_wide, prefix_here,
        orow, gain_two, mine, give, far,
    )
    inverse = inverse_one[:, :1]
    unit = tokens.astype(F32) * inverse
    low = lax.dynamic_slice_in_dim(dh.reshape(seq_len, cols * width), col_index * width, width, 1)
    scaled = gsum * norm_attn.astype(F32)[None, :]
    grad_tokens = low.astype(F32) + inverse * (scaled - unit * (small[0, 0] / (cols * width))[:, None])

    def wide_columns(blocks):
        count, _, half, size = blocks.shape
        return blocks.reshape(count, 2 * half, size).transpose(1, 0, 2).reshape(2 * half, count * size).astype(F32)

    return (
        outg.reshape(seq_len, width),
        grad_tokens.astype(BF16),
        wide_columns(final_a[..., :128]),
        wide_columns(final_a[..., 128:256]),
        wide_columns(final_a[..., 256:]),
        final_o.reshape(-1, width).astype(F32),
        wide_columns(final_f[1]),
        wide_columns(final_f[2]),
        final_f[0].reshape(-1, width).astype(F32),
        small[1, 1],
        small[1, 2],
    )


def solution(mesh):
    in_specs = (
        P(("dp", "row"), "col"),
        P("col", "row"),
        P("col", "row"),
        P("col", "row"),
        P("row", "col"),
        P("col", "row"),
        P("col", "row"),
        P("row", "col"),
        P("col"),
        P("col"),
        P(("dp", "col")),
        P(("dp", "row"), "col"),
    )
    out_specs = (
        P(("dp", "row"), "col"),
        P(("dp", "row"), "col"),
        P("col", "row"),
        P("col", "row"),
        P("col", "row"),
        P("row", "col"),
        P("col", "row"),
        P("col", "row"),
        P("row", "col"),
        P("col"),
        P("col"),
    )

    def step(*arrays):
        tokens, prefix_len = arrays[0], arrays[10]
        sequence_each = prefix_len.shape[0] == mesh.shape["dp"] * mesh.shape["row"]
        square = mesh.shape["dp"] == 2 and mesh.shape["row"] == 4 and mesh.shape["col"] == 4
        body = per_device if sequence_each and square else per_device_general
        return jax.shard_map(
            body, mesh=mesh, in_specs=in_specs, out_specs=out_specs, check_vma=False
        )(*arrays)

    return step
```

```python
import jax
import jax.numpy as jnp
from jax import lax
from jax.experimental import pallas as pl
from jax.experimental.pallas import tpu as pltpu
from jax.sharding import PartitionSpec as P

D = 2048
HEAD_DIM = 64


EPSILON = 1e-05
THETA = 130000.0


def feature_total(values):
    return lax.psum(jnp.sum(values, axis=1), "col")


def normalize(values):
    squares = feature_total(values * values)
    inverse_rms = lax.rsqrt(squares / D + EPSILON)
    return (values * inverse_rms[:, None], inverse_rms)


def norm_backward(grad_normed, unit_rows, inverse_rms, gain_row):
    scaled = grad_normed * gain_row[None, :]
    center = feature_total(scaled * unit_rows) / D
    grad_values = inverse_rms[:, None] * (scaled - unit_rows * center[:, None])
    return (grad_values, jnp.sum(grad_normed * unit_rows, axis=0))


def product(left, weight, transposed):
    if transposed:
        return lax.dot_general(
            left, weight, (((1,), (1,)), ((), ())), preferred_element_type=jnp.float32
        )
    return jnp.dot(left, weight, preferred_element_type=jnp.float32)


def outer_product(left, right):
    return lax.dot_general(
        left, right, (((0,), (0,)), ((), ())), preferred_element_type=jnp.float32
    )


def gather_rows(values):
    return lax.all_gather(values, "row", axis=0, tiled=True)


def gather_cols(values):
    return lax.all_gather(values, "col", axis=0, tiled=True)


def sum_to_cols(gathered, weight, transposed):
    row_count = gathered.shape[0] // lax.axis_size("col")

    def partial_term(offset_rows, length_rows):
        return product(gathered, weight, transposed)

    return lax.psum_scatter(
        partial_term(jnp.int32(0), row_count * lax.axis_size("col")).astype(jnp.bfloat16),
        "col",
        scatter_dimension=0,
        tiled=True,
    ).astype(jnp.float32)


def sum_to_rows(gathered, weight, transposed):
    row_count = gathered.shape[0] // lax.axis_size("row")

    def partial_term(offset_rows, length_rows):
        return product(gathered, weight, transposed)

    return lax.psum_scatter(
        partial_term(jnp.int32(0), row_count * lax.axis_size("row")).astype(jnp.bfloat16),
        "row",
        scatter_dimension=0,
        tiled=True,
    ).astype(jnp.float32)


def rope_tables(row_count, seq_len):
    half_dim = HEAD_DIM // 2
    places = (jnp.arange(row_count, dtype=jnp.int32) % seq_len).astype(jnp.float32)
    rates = THETA ** (-2.0 * jnp.arange(half_dim, dtype=jnp.float32) / HEAD_DIM)
    angles = places[:, None] * rates[None, :]
    return (jnp.cos(angles), jnp.sin(angles))


def rotate(values, cosine, sine):
    row_count = values.shape[0]
    shaped = values.reshape(row_count, -1, HEAD_DIM)
    half_dim = HEAD_DIM // 2
    first_half = shaped[:, :, :half_dim]
    second_half = shaped[:, :, half_dim:]
    cosine_rows = cosine[:, None, :]
    sine_rows = sine[:, None, :]
    turned = jnp.concatenate(
        [
            first_half * cosine_rows - second_half * sine_rows,
            second_half * cosine_rows + first_half * sine_rows,
        ],
        axis=2,
    )
    return turned.reshape(row_count, -1)


def visible_keys(first_row, block_rows, seq_len, prefix_here):
    query_place = first_row + jnp.arange(block_rows, dtype=jnp.int32)
    key_place = jnp.arange(seq_len, dtype=jnp.int32)
    return (key_place[None, :] <= query_place[:, None]) | (key_place[None, :] < prefix_here)


def attention_forward(queries, keys, values, prefix_len, seq_len):
    row_count = queries.shape[0]
    heads_here = queries.shape[1] // HEAD_DIM
    block_rows = min(512, seq_len)
    per_sequence = seq_len // block_rows
    query_blocks = queries.reshape(row_count // block_rows, block_rows, heads_here, HEAD_DIM)
    key_seqs = keys.reshape(row_count // seq_len, seq_len, heads_here, HEAD_DIM)
    value_seqs = values.reshape(row_count // seq_len, seq_len, heads_here, HEAD_DIM)
    factor = HEAD_DIM ** (-0.5)
    numbers = jnp.arange(row_count // block_rows, dtype=jnp.int32)

    def one_block(inputs):
        query_block, number = inputs
        sequence = number // per_sequence
        first_row = number % per_sequence * block_rows
        key_seq = lax.dynamic_index_in_dim(key_seqs, sequence, 0, keepdims=False)
        value_seq = lax.dynamic_index_in_dim(value_seqs, sequence, 0, keepdims=False)
        prefix_here = lax.dynamic_index_in_dim(prefix_len, sequence, 0, keepdims=False)
        scores = (
            jnp.einsum("qhd,khd->hqk", query_block, key_seq, preferred_element_type=jnp.float32)
            * factor
        )
        visible = visible_keys(first_row, block_rows, seq_len, prefix_here)
        exponent = jnp.where(visible[None], jnp.exp(scores), 0.0)
        totals = jnp.sum(exponent, axis=2)
        probabilities = (exponent / totals[:, :, None]).astype(jnp.bfloat16)
        attended = jnp.einsum(
            "hqk,khd->qhd", probabilities, value_seq, preferred_element_type=jnp.float32
        )
        return (attended.reshape(block_rows, heads_here * HEAD_DIM), jnp.log(totals))

    attended, log_totals = lax.map(one_block, (query_blocks, numbers))
    return (attended.reshape(row_count, -1), log_totals)


def attention_backward(queries, keys, values, grad_attended, log_totals, prefix_len, seq_len):
    row_count = queries.shape[0]
    heads_here = queries.shape[1] // HEAD_DIM
    block_rows = min(512, seq_len)
    per_sequence = seq_len // block_rows
    query_blocks = queries.reshape(row_count // block_rows, block_rows, heads_here, HEAD_DIM)
    grad_blocks = grad_attended.reshape(row_count // block_rows, block_rows, heads_here, HEAD_DIM)
    key_seqs = keys.reshape(row_count // seq_len, seq_len, heads_here, HEAD_DIM)
    value_seqs = values.reshape(row_count // seq_len, seq_len, heads_here, HEAD_DIM)
    factor = HEAD_DIM ** (-0.5)
    numbers = jnp.arange(row_count // block_rows, dtype=jnp.int32)
    zero_seqs = jnp.zeros(key_seqs.shape, jnp.float32)

    def one_block(carry, inputs):
        grad_key_seqs, grad_value_seqs = carry
        query_block, grad_block, log_block, number = inputs
        sequence = number // per_sequence
        first_row = number % per_sequence * block_rows
        key_seq = lax.dynamic_index_in_dim(key_seqs, sequence, 0, keepdims=False)
        value_seq = lax.dynamic_index_in_dim(value_seqs, sequence, 0, keepdims=False)
        prefix_here = lax.dynamic_index_in_dim(prefix_len, sequence, 0, keepdims=False)
        scores = (
            jnp.einsum("qhd,khd->hqk", query_block, key_seq, preferred_element_type=jnp.float32)
            * factor
        )
        visible = visible_keys(first_row, block_rows, seq_len, prefix_here)
        probabilities = jnp.where(visible[None], jnp.exp(scores - log_block[:, :, None]), 0.0)
        grad_probs = jnp.einsum(
            "qhd,khd->hqk", grad_block, value_seq, preferred_element_type=jnp.float32
        )
        center = jnp.sum(probabilities * grad_probs, axis=2)
        grad_scores = (probabilities * (grad_probs - center[:, :, None]) * factor).astype(
            jnp.bfloat16
        )
        grad_query = jnp.einsum(
            "hqk,khd->qhd", grad_scores, key_seq, preferred_element_type=jnp.float32
        )
        grad_key = jnp.einsum(
            "hqk,qhd->khd", grad_scores, query_block, preferred_element_type=jnp.float32
        )
        grad_value = jnp.einsum(
            "hqk,qhd->khd",
            probabilities.astype(jnp.bfloat16),
            grad_block,
            preferred_element_type=jnp.float32,
        )
        grad_key_seqs = lax.dynamic_update_index_in_dim(
            grad_key_seqs,
            lax.dynamic_index_in_dim(grad_key_seqs, sequence, 0, keepdims=False) + grad_key,
            sequence,
            0,
        )
        grad_value_seqs = lax.dynamic_update_index_in_dim(
            grad_value_seqs,
            lax.dynamic_index_in_dim(grad_value_seqs, sequence, 0, keepdims=False) + grad_value,
            sequence,
            0,
        )
        return (
            (grad_key_seqs, grad_value_seqs),
            grad_query.reshape(block_rows, heads_here * HEAD_DIM),
        )

    carried, grad_queries = lax.scan(
        one_block, (zero_seqs, zero_seqs), (query_blocks, grad_blocks, log_totals, numbers)
    )
    grad_key_seqs, grad_value_seqs = carried
    return (
        grad_queries.reshape(row_count, -1),
        grad_key_seqs.reshape(row_count, -1),
        grad_value_seqs.reshape(row_count, -1),
    )


def per_device_general(
    tokens,
    w_query,
    w_key,
    w_value,
    w_output,
    w_gate,
    w_up,
    w_down,
    norm_attn,
    norm_ffn,
    prefix_len,
    cotangent,
):
    width_attn = w_query.shape[1]
    width_ffn = w_gate.shape[1]
    inputs = tokens.astype(jnp.float32)
    gain_attn = norm_attn.astype(jnp.float32)
    gain_ffn = norm_ffn.astype(jnp.float32)
    unit_one, inverse_one = normalize(inputs)
    normed_one = (unit_one * gain_attn[None, :]).astype(jnp.bfloat16)
    rows_one = gather_rows(normed_one)
    w_attn = jnp.concatenate([w_query, w_key, w_value], axis=1)
    projected = sum_to_cols(rows_one, w_attn, False)
    row_count = projected.shape[0]
    seq_len = row_count // prefix_len.shape[0]
    cosine, sine = rope_tables(row_count, seq_len)
    queries = rotate(projected[:, :width_attn], cosine, sine).astype(jnp.bfloat16)
    keys = rotate(projected[:, width_attn : 2 * width_attn], cosine, sine).astype(jnp.bfloat16)
    values = projected[:, 2 * width_attn :].astype(jnp.bfloat16)
    attended, log_totals = attention_forward(queries, keys, values, prefix_len, seq_len)
    attended_low = attended.astype(jnp.bfloat16)
    attended_rows = gather_cols(attended_low)
    hidden = inputs + sum_to_rows(attended_rows, w_output, False)
    unit_two, inverse_two = normalize(hidden)
    normed_two = (unit_two * gain_ffn[None, :]).astype(jnp.bfloat16)
    rows_two = gather_rows(normed_two)
    w_pair = jnp.concatenate([w_gate, w_up], axis=1)
    gate_up = sum_to_cols(rows_two, w_pair, False)
    gate = gate_up[:, :width_ffn]
    up_proj = gate_up[:, width_ffn:]
    gate_sigmoid = jax.nn.sigmoid(gate)
    silu_gate = gate * gate_sigmoid
    activ = (silu_gate * up_proj).astype(jnp.bfloat16)
    act_rows = gather_cols(activ)
    result = hidden + sum_to_rows(act_rows, w_down, False)
    output = result.astype(jnp.bfloat16)
    grad_rows = gather_rows(cotangent)
    grad_act = sum_to_cols(grad_rows, w_down, True)
    grad_gate = grad_act * up_proj * gate_sigmoid * (1.0 + gate * (1.0 - gate_sigmoid))
    grad_up = grad_act * silu_gate
    grad_pair = jnp.concatenate([grad_gate, grad_up], axis=1).astype(jnp.bfloat16)
    grad_pair_rows = gather_cols(grad_pair)
    grad_normed_two = sum_to_rows(grad_pair_rows, w_pair, True)
    weight_pair = outer_product(rows_two, grad_pair_rows)
    weight_down = outer_product(act_rows, grad_rows)
    grad_from_two, gain_part_two = norm_backward(grad_normed_two, unit_two, inverse_two, gain_ffn)
    grad_hidden = cotangent.astype(jnp.float32) + grad_from_two
    grad_hidden_low = grad_hidden.astype(jnp.bfloat16)
    grad_hidden_rows = gather_rows(grad_hidden_low)
    grad_attended = sum_to_cols(grad_hidden_rows, w_output, True).astype(jnp.bfloat16)
    weight_out = outer_product(attended_rows, grad_hidden_rows)
    grad_queries, grad_keys, grad_values = attention_backward(
        queries, keys, values, grad_attended, log_totals, prefix_len, seq_len
    )
    grad_proj = jnp.concatenate(
        [rotate(grad_queries, cosine, -sine), rotate(grad_keys, cosine, -sine), grad_values], axis=1
    ).astype(jnp.bfloat16)
    grad_proj_rows = gather_cols(grad_proj)
    grad_normed_one = sum_to_rows(grad_proj_rows, w_attn, True)
    weight_attn = outer_product(rows_one, grad_proj_rows)
    weight_attn, weight_out, weight_pair, weight_down = (
        lax.psum(weight_attn.astype(jnp.bfloat16), "dp").astype(jnp.float32),
        lax.psum(weight_out.astype(jnp.bfloat16), "dp").astype(jnp.float32),
        lax.psum(weight_pair.astype(jnp.bfloat16), "dp").astype(jnp.float32),
        lax.psum(weight_down.astype(jnp.bfloat16), "dp").astype(jnp.float32),
    )
    grad_from_one, gain_part_one = norm_backward(grad_normed_one, unit_one, inverse_one, gain_attn)
    grad_tokens = (grad_hidden + grad_from_one).astype(jnp.bfloat16)
    gain_one, gain_two = lax.psum((gain_part_one, gain_part_two), ("dp", "row"))
    return (
        output,
        grad_tokens,
        weight_attn[:, :width_attn],
        weight_attn[:, width_attn : 2 * width_attn],
        weight_attn[:, 2 * width_attn :],
        weight_out,
        weight_pair[:, :width_ffn],
        weight_pair[:, width_ffn:],
        weight_down,
        gain_one,
        gain_two,
    )


MESH = pl.DeviceIdType.MESH
F32 = jnp.float32
BF16 = jnp.bfloat16
COLS = 4
ROW_Y = 2
ROW_CORE = 1
VMEM_LIMIT = 64 * 1024 * 1024 - 64 * 1024


def dot_nn(left, right):
    return lax.dot_general(left, right, (((1,), (0,)), ((), ())), preferred_element_type=F32)


def dot_nt(left, right):
    return lax.dot_general(left, right, (((1,), (1,)), ((), ())), preferred_element_type=F32)


def dot_tn(left, right):
    return lax.dot_general(left, right, (((0,), (0,)), ((), ())), preferred_element_type=F32)


class Place:
    def __init__(self):
        self.x = lax.axis_index("dp")
        self.r = lax.axis_index("row")
        self.z = lax.axis_index("col")

    def peer_z(self, z):
        return {"col": z}

    def partner(self, name):
        if name == "x":
            return {"dp": 1 - self.x}
        bit = ROW_Y if name == "y" else ROW_CORE
        low = lax.rem(lax.div(self.r, bit), 2)
        return {"row": self.r + bit * (1 - 2 * low)}

    def barrier(self):
        sem = pltpu.get_barrier_semaphore()
        for s in (1, 2, 3):
            pl.semaphore_signal(
                sem, 1, device_id=self.peer_z(lax.rem(self.z + s, COLS)), device_id_type=MESH
            )
        for name in ("x", "y", "core"):
            pl.semaphore_signal(sem, 1, device_id=self.partner(name), device_id_type=MESH)
        pl.semaphore_wait(sem, 6)


def remote(src, dst, send, recv, device):
    return pltpu.make_async_remote_copy(
        src_ref=src,
        dst_ref=dst,
        send_sem=send,
        recv_sem=recv,
        device_id=device,
        device_id_type=MESH,
    )


class LineGather:
    def __init__(self, place, buf, send, recv):
        self.place, self.buf, self.send, self.recv = place, buf, send, recv

    def copy(self, step, side):
        z = self.place.z
        block = z - step if side == 0 else z + step
        to = z + 1 if side == 0 else z - 1
        block = jnp.clip(block, 0, COLS - 1)
        to = jnp.clip(to, 0, COLS - 1)
        return remote(
            self.buf.at[block],
            self.buf.at[block],
            self.send.at[side, step],
            self.recv.at[side, step],
            self.place.peer_z(to),
        )

    def sends(self, step, side):
        z = self.place.z
        if side == 0:
            return jnp.logical_and(z - step >= 0, z + 1 < COLS)
        return jnp.logical_and(z + step < COLS, z >= 1)

    def gets(self, step, side):
        z = self.place.z
        if side == 0:
            return z - 1 - step >= 0
        return z + 1 + step < COLS

    def start(self, step):
        for side in (0, 1):

            @pl.when(self.sends(step, side))
            def _():
                self.copy(step, side).start()

    def wait_recv(self, step):
        for side in (0, 1):

            @pl.when(self.gets(step, side))
            def _():
                self.copy(step, side).wait_recv()

    def finish(self):
        for step in range(COLS - 1):
            for side in (0, 1):

                @pl.when(self.sends(step, side))
                def _():
                    self.copy(step, side).wait_send()


class LineSum:
    def __init__(self, place, parts, right, left, send, recv):
        self.place, self.parts = place, parts
        self.inbox = (right, left)
        self.send, self.recv = send, recv

    def copy(self, step, side):
        z = self.place.z
        d = COLS - 1 - step if side == 0 else step
        to = jnp.clip(z + 1 if side == 0 else z - 1, 0, COLS - 1)
        return remote(
            self.parts.at[d],
            self.inbox[side].at[step],
            self.send.at[side, step],
            self.recv.at[side, step],
            self.place.peer_z(to),
        )

    def hops(self, side):
        z = self.place.z
        return z if side == 0 else COLS - 1 - z

    def sends(self, step, side):
        return self.hops(side) < COLS - 1 - step

    def gets(self, step, side):
        hops = self.hops(side)
        return jnp.logical_and(hops > 0, hops <= COLS - 1 - step)

    def run_slot(self, t):
        for side in (0, 1):
            step = t - self.hops(side)
            valid = jnp.logical_and(step >= 0, step < COLS - 1)
            step = jnp.clip(step, 0, COLS - 2)
            d = COLS - 1 - step if side == 0 else step

            @pl.when(jnp.logical_and(valid, self.gets(step, side)))
            def _():
                self.copy(step, side).wait_recv()
                rows = self.parts.shape[1]

                @pl.loop(0, rows // 32)
                def _(i):
                    part = pl.ds(pl.multiple_of(i * 32, 32), 32)
                    total = self.parts[d, part, :].astype(F32) + self.inbox[side][
                        step, part, :
                    ].astype(F32)
                    self.parts[d, part, :] = total.astype(BF16)

            @pl.when(jnp.logical_and(valid, self.sends(step, side)))
            def _():
                self.copy(step, side).start()

    def finish(self):
        for step in range(COLS - 1):
            for side in (0, 1):

                @pl.when(self.sends(step, side))
                def _():
                    self.copy(step, side).wait_send()


class Widen:
    def __init__(self, place, index, source, slot, sems):
        self.place, self.index, self.source, self.slot = place, index, source, slot
        self.sems = sems

    def pair(self, stage, j):
        return self.sems.at[0, stage, self.index, j], self.sems.at[1, stage, self.index, j]

    def local(self):
        z = self.place.z
        return pltpu.make_async_copy(
            self.source(z, None), self.slot(0, z, None), self.sems.at[0, 5, self.index, 0]
        )

    def to_col(self, s):
        place = self.place
        peer = lax.rem(place.z + s, COLS)
        send, recv = self.pair(0, s)
        return remote(
            self.source(peer, place.x), self.slot(0, place.z, place.x), send, recv, place.peer_z(peer)
        )

    def origin(self, s):
        return lax.rem(self.place.z + COLS - s, COLS)

    def to_dp(self, s):
        ref = self.slot(0, self.origin(s), self.place.x)
        send, recv = self.pair(1, s)
        return remote(ref, ref, send, recv, self.place.partner("x"))

    def near(self, stage, s):
        origin = self.origin(s)
        send, recv = self.pair(stage, s)
        if stage == 4:
            src, dst = self.slot(2, origin, None), self.slot(3, origin, None)
        else:
            src = self.source(self.place.z, None) if s == 0 else self.slot(0, origin, None)
            dst = self.slot(2 if stage == 2 else 1, origin, None)
        return remote(src, dst, send, recv, self.place.partner("y" if stage == 2 else "core"))

    def start_col(self):
        for s in (2, 1, 3):
            self.to_col(s).start()

    def start_near(self):
        self.near(2, 0).start()
        self.near(3, 0).start()
        self.local().start()

    def pass_dp(self, s):
        self.to_col(s).wait_recv()
        self.to_dp(s).start()

    def pass_near(self, s):
        self.to_dp(s).wait_recv()
        self.near(2, s).start()
        self.near(3, s).start()

    def pass_far(self, s):
        self.near(2, s).wait_recv()
        self.near(4, s).start()

    def arrived(self):
        self.local().wait()
        for s in range(COLS):
            self.near(3, s).wait_recv()
            self.near(4, s).wait_recv()

    def finish(self):
        for s in range(COLS):
            if s:
                self.to_col(s).wait_send()
                self.to_dp(s).wait_send()
            for stage in (2, 3, 4):
                self.near(stage, s).wait_send()


def swap_halves(values):
    lane = lax.broadcasted_iota(jnp.int32, values.shape, 1)
    up = pltpu.roll(values, 96, 1)
    down = pltpu.roll(values, 32, 1)
    return jnp.where(lax.rem(lane, 64) < 32, up, down)


def half_lanes(values, h):
    lane = lax.broadcasted_iota(jnp.int32, values.shape, 1)
    return jnp.where((lane >= 64) == bool(h), values, jnp.zeros_like(values))


def visible_block(first, rows, keys, prefix):
    query = first + lax.broadcasted_iota(jnp.int32, (rows, keys), 0)
    key = lax.broadcasted_iota(jnp.int32, (rows, keys), 1)
    return jnp.logical_or(key <= query, key < prefix)


def weight_paths(place, sems, w_refs, wide_refs):
    wqkv, wo, wg, wu, wd = w_refs
    vqkv, vo, vg, vu, vd = wide_refs

    def rows_of(first, size, half):
        if half is None:
            return pl.ds(pl.multiple_of(first, 64), size)
        return pl.ds(pl.multiple_of(first + half * (size // 2), 64), size // 2)

    def columns(p, width):
        return pl.ds(pl.multiple_of(p * width, 128), width)

    paths = [
        Widen(
            place,
            0,
            lambda p, h: wqkv.at[:, rows_of(0, 512, h), columns(p, 128)],
            lambda k, j, h: vqkv.at[k, j, :, rows_of(0, 512, h), :],
            sems,
        ),
        Widen(
            place,
            1,
            lambda p, h: wo.at[rows_of(p * 128, 128, h), :],
            lambda k, j, h: vo.at[k, j, rows_of(0, 128, h), :],
            sems,
        ),
    ]
    for i, (w, v) in enumerate(((wg, vg), (wu, vu))):
        paths.append(
            Widen(
                place,
                2 + i,
                lambda p, h, w=w: w.at[rows_of(0, 512, h), columns(p, 512)],
                lambda k, j, h, v=v: v.at[k, j, rows_of(0, 512, h), :],
                sems,
            )
        )
    paths.append(
        Widen(
            place,
            4,
            lambda p, h: wd.at[rows_of(p * 512, 512, h), :],
            lambda k, j, h: vd.at[k, j, rows_of(0, 512, h), :],
            sems,
        )
    )
    return paths


def forward_kernel(
    xin,
    wqkv,
    wo,
    wg,
    wu,
    wd,
    cosine,
    sine,
    prefix,
    xg,
    normed_one,
    q_out,
    k_out,
    v_out,
    att,
    hidden,
    normed_two,
    gains,
    inverse_one,
    vqkv,
    vo,
    vg,
    vu,
    vd,
    parts,
    inbox_r,
    inbox_l,
    acc,
    sems,
    line_sems,
    local_sem,
):
    place = Place()
    z = place.z
    place.barrier()
    own = pltpu.make_async_copy(xin, xg.at[z], local_sem.at[0])
    own.start()
    own.wait()
    gather_x = LineGather(place, xg, line_sems.at[0, 0], line_sems.at[0, 1])
    qkv, out, gate, up, down = weight_paths(
        place, sems, (wqkv, wo, wg, wu, wd), (vqkv, vo, vg, vu, vd)
    )
    qkv.start_col()
    qkv.start_near()
    out.start_col()
    out.start_near()
    gather_x.start(0)
    for s in (1, 3, 2):
        qkv.pass_dp(s)
    for s in (1, 3, 2):
        out.pass_dp(s)
        qkv.pass_near(s)
    for s in (1, 3, 2):
        out.pass_near(s)
    gate.start_near()
    up.start_near()
    down.start_near()
    qkv.pass_far(0)
    out.pass_far(0)
    gather_x.wait_recv(0)
    gather_x.start(1)
    gather_x.wait_recv(1)
    gather_x.start(2)
    for s in (1, 3, 2):
        qkv.pass_far(s)
    for s in (1, 3, 2):
        out.pass_far(s)
    gather_x.wait_recv(2)
    gate.start_col()
    up.start_col()
    down.start_col()

    @pl.loop(0, 16)
    def _(i):
        part = pl.ds(pl.multiple_of(i * 32, 32), 32)
        blocks = [xg[j, part, :].astype(F32) for j in range(COLS)]
        squares = sum(jnp.sum(b * b, axis=1, keepdims=True) for b in blocks)
        inverse = lax.rsqrt(squares / D + EPSILON)
        inverse_one[part, :] = jnp.broadcast_to(inverse, (32, 128))
        for j in range(COLS):
            gain = xg[j, 512:513, :].astype(F32)
            normed_one[part, j * 512 : (j + 1) * 512] = (blocks[j] * inverse * gain).astype(BF16)

    for j in range(COLS):
        gains[j] = xg[j, 512:528, :]
    qkv.arrived()

    for w in range(3):

        @pl.loop(0, 2)
        def _(pair):
            wide = jnp.concatenate(
                [vqkv[2 * pair + i, :, w].reshape(D, 128) for i in range(2)], axis=1
            )
            acc[:, 0:256] = dot_nn(normed_one[...], wide)
            for i in range(2):
                k = 2 * pair + i
                block = acc[:, i * 128 : (i + 1) * 128]
                if w < 2:
                    block = block * cosine[...] + swap_halves(block) * sine[...]
                (q_out, k_out, v_out)[w][k] = block.astype(BF16)


    reach = prefix[0]
    @pl.loop(0, COLS)
    def _(k):
        for first, keys in ((0, 256), (256, 512)):
            queries = q_out[k, first : first + 256, :]
            visible = visible_block(first, 256, keys, reach)
            kept = None
            for h in range(2):
                scores = dot_nt(half_lanes(queries, h), k_out[k, 0:keys, :]) * (HEAD_DIM**-0.5)
                weights = jnp.where(visible, jnp.exp(scores), 0.0)
                probs = (weights / jnp.sum(weights, axis=1, keepdims=True)).astype(BF16)
                got = half_lanes(dot_nn(probs, v_out[k, 0:keys, :]), h)
                kept = got if kept is None else kept + got
            att[k, first : first + 256, :] = kept.astype(BF16)

    out.arrived()
    attended = jnp.concatenate([att[k] for k in range(COLS)], axis=1)

    @pl.loop(0, COLS)
    def _(j):
        piece = dot_nn(attended, vo[:, j].reshape(512, 512))
        lanes = pl.ds(pl.multiple_of(j * 512, 512), 512)
        parts[:, :, lanes] = piece.astype(BF16).reshape(COLS, 128, 512)

    total = LineSum(place, parts, inbox_r, inbox_l, line_sems.at[1, 0], line_sems.at[1, 1])
    total.run_slot(0)
    for path in (gate, up, down):
        for s in (1, 3, 2):
            path.pass_dp(s)
        if path is not gate:
            (gate if path is up else up).pass_far(0)
        if path is down:
            total.run_slot(1)
        for s in (1, 3, 2):
            path.pass_near(s)
        if path is up:
            for s in (1, 3, 2):
                gate.pass_far(s)
    total.run_slot(2)
    up.pass_far(1)
    up.pass_far(3)
    total.run_slot(3)

    @pl.loop(0, 4)
    def _(i):
        part = pl.ds(pl.multiple_of(i * 32, 32), 32)
        rows = pl.ds(pl.multiple_of(z * 128 + i * 32, 32), 32)
        squares = jnp.zeros((32, 1), F32)
        for j in range(COLS):
            lanes = slice(j * 512, (j + 1) * 512)
            value = parts[z, part, lanes].astype(F32) + xg[j, rows, :].astype(F32)
            hidden[part, lanes] = value
            squares += jnp.sum(value * value, axis=1, keepdims=True)
        inverse = lax.rsqrt(squares / D + EPSILON)
        for j in range(COLS):
            lanes = slice(j * 512, (j + 1) * 512)
            gain = xg[j, 513:514, :].astype(F32)
            normed_two[z, part, lanes] = (hidden[part, lanes] * inverse * gain).astype(BF16)

    gather_n = LineGather(place, normed_two, line_sems.at[2, 0], line_sems.at[2, 1])
    gather_n.start(0)
    up.pass_far(2)
    down.pass_far(0)
    down.pass_far(1)
    gather_n.wait_recv(0)
    gather_n.start(1)
    down.pass_far(3)
    gather_n.wait_recv(1)
    gather_n.start(2)
    down.pass_far(2)
    gather_n.wait_recv(2)
    for path in (gate, up, down):
        path.arrived()
    for path in (qkv, out, gate, up, down):
        path.finish()
    gather_x.finish()
    total.finish()
    gather_n.finish()


def forward_half(xin, wqkv, wo, wg, wu, wd, cosine, sine, prefix):
    vmem = pl.BlockSpec(memory_space=pltpu.VMEM)
    hbm = pl.BlockSpec(memory_space=pl.ANY)
    shape = jax.ShapeDtypeStruct
    return pl.pallas_call(
        forward_kernel,
        name="forward_half",
        out_shape=[
            shape((4, 528, 512), BF16),
            shape((512, D), BF16),
            shape((4, 512, 128), BF16),
            shape((4, 512, 128), BF16),
            shape((4, 512, 128), BF16),
            shape((4, 512, 128), BF16),
            shape((128, D), F32),
            shape((4, 128, D), BF16),
            shape((4, 16, 512), BF16),
            shape((512, 128), F32),
            shape((4, 4, 3, 512, 128), BF16),
            shape((4, 4, 128, 512), BF16),
            shape((4, 4, 512, 512), BF16),
            shape((4, 4, 512, 512), BF16),
            shape((4, 4, 512, 512), BF16),
        ],
        in_specs=[vmem, hbm, hbm, hbm, hbm, hbm, vmem, vmem, pl.BlockSpec(memory_space=pltpu.SMEM)],
        out_specs=[vmem] * 12 + [hbm] * 3,
        scratch_shapes=[
            pltpu.VMEM((4, 128, D), BF16),
            pltpu.VMEM((3, 128, D), BF16),
            pltpu.VMEM((3, 128, D), BF16),
            pltpu.VMEM((512, 256), F32),
            pltpu.SemaphoreType.DMA((2, 6, 5, 4)),
            pltpu.SemaphoreType.DMA((3, 2, 2, 3)),
            pltpu.SemaphoreType.DMA((1,)),
        ],
        compiler_params=pltpu.CompilerParams(
            collective_id=1, has_side_effects=True, vmem_limit_bytes=VMEM_LIMIT
        ),
    )(xin, wqkv, wo, wg, wu, wd, cosine, sine, prefix)


def feed_forward_kernel(
    cot,
    n2,
    hidden,
    gains,
    vg_hbm,
    vu_hbm,
    vd_hbm,
    dh,
    orow,
    gain_part,
    mine,
    give,
    far,
    side,
    near,
    cg,
    vg,
    vu,
    vd,
    gate_s,
    up_s,
    act,
    dgate,
    dup,
    pout,
    box_or,
    box_ol,
    parts,
    box_r,
    box_l,
    tiles,
    adds,
    load_sems,
    line_sems,
    near_sems,
    tile_sems,
    add_sems,
    y_sems,
    side_sems,
    local_sem,
):
    place = Place()
    z = place.z
    own = pltpu.make_async_copy(cot, cg.at[z], local_sem.at[0])
    own.start()

    def load(i, k):
        src, dst = ((vg_hbm, vg), (vu_hbm, vu), (vd_hbm, vd))[i]
        return pltpu.make_async_copy(src.at[k], dst.at[k], load_sems.at[i, k])

    own.wait()
    for i, k in ((0, 0), (1, 0), (0, 1), (1, 1), (0, 2), (1, 2), (0, 3), (1, 3)):
        load(i, k).start()
    for k in range(COLS):
        load(2, k).start()
    place.barrier()
    gather_c = LineGather(place, cg, line_sems.at[0, 0], line_sems.at[0, 1])
    gather_c.start(0)

    def first_products(k):
        load(0, k).wait()
        load(1, k).wait()
        rows = n2[...].reshape(512, D)
        gate_s[k] = dot_nn(rows, vg[k].reshape(D, 512))
        up_s[k] = dot_nn(rows, vu[k].reshape(D, 512))

        @pl.loop(0, 16)
        def _(i):
            part = pl.ds(pl.multiple_of(i * 32, 32), 32)
            gate = gate_s[k, part, :]
            act[k, part, :] = (gate * jax.nn.sigmoid(gate) * up_s[k, part, :]).astype(BF16)

    pl.loop(0, 3)(first_products)
    gather_c.wait_recv(0)
    gather_c.start(1)
    pl.loop(3, COLS)(first_products)
    for k in range(COLS):
        load(2, k).wait()

    @pl.loop(0, COLS)
    def _(j):
        wide = jnp.concatenate([act[k] for k in range(COLS)], axis=1)
        piece = dot_nn(wide, vd[:, j].reshape(D, 512))
        lanes = pl.ds(pl.multiple_of(j * 512, 512), 512)
        pout[:, :, lanes] = piece.astype(BF16).reshape(COLS, 128, 512)

    gather_c.wait_recv(1)
    gather_c.start(2)
    out_sum = LineSum(place, pout, box_or, box_ol, line_sems.at[1, 0], line_sems.at[1, 1])
    out_sum.run_slot(0)
    gather_c.wait_recv(2)

    def left_of(w, k, j):
        return act[k] if w == 0 else n2[:, :, pl.ds(pl.multiple_of(j * 512, 512), 512)].reshape(512, 512)

    def right_of(w, k, j):
        return cg[j] if w == 0 else (dgate, dup)[w - 1][k]

    def near_copy(w, t):
        slot = lax.rem(t, 2)
        return remote(
            tiles.at[slot],
            near.at[w, t],
            tile_sems.at[slot],
            near_sems.at[w, t],
            place.partner("core"),
        )

    def send_near(w, first):
        @pl.loop(0, 8)
        def _(t):
            k = 1 + 2 * lax.div(t, 4)
            j = lax.rem(t, 4)
            slot = lax.rem(t, 2)
            if first:

                @pl.when(t >= 2)
                def _():
                    near_copy(w, t).wait_send()
            else:
                near_copy(w, t).wait_send()
            tiles[slot] = dot_tn(left_of(w, k, j), right_of(w, k, j)).astype(BF16)
            near_copy(w, t).start()

    def fetch(w, t):
        slot = lax.rem(t, 2)
        return pltpu.make_async_copy(near.at[w, t], adds.at[slot], add_sems.at[0, slot])

    def settle(w, t):
        slot = lax.rem(t, 2)
        j = lax.rem(t, 4)
        to = mine if t < 4 else give
        return pltpu.make_async_copy(adds.at[2 + slot], to.at[w, j], add_sems.at[1, slot])

    def add_near(w, half, keep=None):
        for j in range(2):
            near_copy(w, 4 * half + j).wait_recv()
            fetch(w, 4 * half + j).start()
        for j in range(COLS):
            t = 4 * half + j
            slot = t % 2
            k = 2 * half
            value = dot_tn(left_of(w, k, j), right_of(w, k, j))
            fetch(w, t).wait()
            value = (value + adds[slot].astype(F32)).astype(BF16)
            if j < 2:
                near_copy(w, t + 2).wait_recv()
                fetch(w, t + 2).start()
            if keep is not None:
                keep[0, j] = value
            else:
                if j >= 2:
                    settle(w, t - 2).wait()
                adds[2 + slot] = value
                settle(w, t).start()
        if keep is None:
            settle(w, 4 * half + 2).wait()
            settle(w, 4 * half + 3).wait()

    def side_copy(j):
        half = pl.ds(pl.multiple_of((1 - place.x) * 256, 256), 256)
        return remote(
            vd.at[0, j, half], side.at[j], side_sems.at[0, j], side_sems.at[1, j], place.partner("x")
        )

    def far_copy(j):
        return pltpu.make_async_copy(far.at[0, j], vd.at[1, j], side_sems.at[2, j])

    def keep_copy(j):
        return pltpu.make_async_copy(vd.at[0, j], mine.at[0, j], side_sems.at[3, j])

    def add_far(j):
        y_copy(0, j).wait_recv()
        far_copy(j).start()
        far_copy(j).wait()
        vd[0, j] = (vd[0, j].astype(F32) + vd[1, j].astype(F32)).astype(BF16)
        side_copy(j).start()
        keep_copy(j).start()

    def y_copy(w, j):
        return remote(
            give.at[w, j], far.at[w, j], y_sems.at[0, w, j], y_sems.at[1, w, j], place.partner("y")
        )

    def send_far(w):
        for j in range(COLS):
            y_copy(w, j).start()

    send_near(0, True)

    @pl.loop(0, COLS)
    def _(k):
        wide = jnp.concatenate([cg[j] for j in range(COLS)], axis=1)
        weight = jnp.concatenate([vd[k, j] for j in range(COLS)], axis=1)
        grad_act = dot_nt(wide, weight)
        for i in range(8):
            part = slice(i * 64, (i + 1) * 64)
            d_act = grad_act[part]
            gate = gate_s[k, part, :]
            sig = jax.nn.sigmoid(gate)
            dgate[k, part, :] = (
                d_act * up_s[k, part, :] * sig * (1.0 + gate * (1.0 - sig))
            ).astype(BF16)
            dup[k, part, :] = (d_act * gate * sig).astype(BF16)

        @pl.when(k == 0)
        def _():
            out_sum.run_slot(1)

    out_sum.run_slot(2)
    add_near(0, 1)
    send_far(0)

    @pl.loop(0, COLS)
    def _(j):
        piece = dot_nt(
            jnp.concatenate([dgate[k] for k in range(COLS)], axis=1),
            jnp.concatenate([vg[k, j] for k in range(COLS)], axis=1),
        ) + dot_nt(
            jnp.concatenate([dup[k] for k in range(COLS)], axis=1),
            jnp.concatenate([vu[k, j] for k in range(COLS)], axis=1),
        )
        lanes = pl.ds(pl.multiple_of(j * 512, 512), 512)
        parts[:, :, lanes] = piece.astype(BF16).reshape(COLS, 128, 512)

    total = LineSum(place, parts, box_r, box_l, line_sems.at[2, 0], line_sems.at[2, 1])
    out_sum.run_slot(3)
    total.run_slot(0)
    send_near(1, False)
    total.run_slot(1)
    add_near(1, 1)
    send_far(1)
    total.run_slot(2)
    send_near(2, False)
    total.run_slot(3)

    gain_part[...] = jnp.zeros((8, D), F32)

    @pl.loop(0, 4)
    def _(i):
        part = pl.ds(pl.multiple_of(i * 32, 32), 32)
        rows = pl.ds(pl.multiple_of(z * 128 + i * 32, 32), 32)
        squares = jnp.zeros((32, 1), F32)
        center = jnp.zeros((32, 1), F32)
        for j in range(COLS):
            lanes = slice(j * 512, (j + 1) * 512)
            value = hidden[part, lanes]
            squares += jnp.sum(value * value, axis=1, keepdims=True)
        inverse = lax.rsqrt(squares / D + EPSILON)
        for j in range(COLS):
            lanes = slice(j * 512, (j + 1) * 512)
            grad = parts[z, part, lanes].astype(F32)
            unit = hidden[part, lanes] * inverse
            center += jnp.sum(grad * gains[j, 1:2, :].astype(F32) * unit, axis=1, keepdims=True)
            gain_part[0:1, lanes] += jnp.sum(grad * unit, axis=0, keepdims=True)
        center = center / D
        for j in range(COLS):
            lanes = slice(j * 512, (j + 1) * 512)
            grad = parts[z, part, lanes].astype(F32)
            unit = hidden[part, lanes] * inverse
            scaled = grad * gains[j, 1:2, :].astype(F32)
            value = cg[j, rows, :].astype(F32) + inverse * (scaled - unit * center)
            dh[z, part, lanes] = value.astype(BF16)
            orow[j, part, :] = (hidden[part, lanes] + pout[z, part, lanes].astype(F32)).astype(BF16)

    gather_h = LineGather(place, dh, line_sems.at[3, 0], line_sems.at[3, 1])
    gather_h.start(0)
    add_near(0, 0, vd)
    add_near(2, 1)
    gather_h.wait_recv(0)
    gather_h.start(1)
    add_far(0)
    add_far(1)
    add_near(1, 0)
    gather_h.wait_recv(1)
    gather_h.start(2)
    add_far(2)
    add_far(3)
    add_near(2, 0)
    gather_h.wait_recv(2)
    for j in range(COLS):
        y_copy(1, j).wait_recv()
        side_copy(j).wait_recv()
    for j in range(COLS):
        side_copy(j).wait_send()
        keep_copy(j).wait()
    for w in range(2):
        for j in range(COLS):
            y_copy(w, j).wait_send()
    for t in range(6, 8):
        near_copy(2, t).wait_send()
    for line in (gather_c, out_sum, total, gather_h):
        line.finish()


def feed_forward(cot, n2, hidden, gains, vg, vu, vd):
    vmem = pl.BlockSpec(memory_space=pltpu.VMEM)
    hbm = pl.BlockSpec(memory_space=pl.ANY)
    shape = jax.ShapeDtypeStruct
    dma = pltpu.SemaphoreType.DMA
    return pl.pallas_call(
        feed_forward_kernel,
        name="feed_forward",
        out_shape=[
            shape((4, 128, D), BF16),
            shape((4, 128, 512), BF16),
            shape((8, D), F32),
            shape((3, 4, 512, 512), BF16),
            shape((3, 4, 512, 512), BF16),
            shape((2, 4, 512, 512), BF16),
            shape((4, 256, 512), BF16),
            shape((3, 8, 512, 512), BF16),
        ],
        in_specs=[hbm, vmem, vmem, vmem, hbm, hbm, hbm],
        out_specs=[vmem, vmem, vmem, hbm, hbm, hbm, hbm, hbm],
        scratch_shapes=[
            pltpu.VMEM((4, 512, 512), BF16),
            pltpu.VMEM((4, 4, 512, 512), BF16),
            pltpu.VMEM((4, 4, 512, 512), BF16),
            pltpu.VMEM((4, 4, 512, 512), BF16),
            pltpu.VMEM((4, 512, 512), F32),
            pltpu.VMEM((4, 512, 512), F32),
            pltpu.VMEM((4, 512, 512), BF16),
            pltpu.VMEM((4, 512, 512), BF16),
            pltpu.VMEM((4, 512, 512), BF16),
            pltpu.VMEM((4, 128, D), BF16),
            pltpu.VMEM((3, 128, D), BF16),
            pltpu.VMEM((3, 128, D), BF16),
            pltpu.VMEM((4, 128, D), BF16),
            pltpu.VMEM((3, 128, D), BF16),
            pltpu.VMEM((3, 128, D), BF16),
            pltpu.VMEM((2, 512, 512), BF16),
            pltpu.VMEM((4, 512, 512), BF16),
            dma((3, 4)),
            dma((4, 2, 2, 3)),
            dma((3, 8)),
            dma((2,)),
            dma((2, 2)),
            dma((2, 2, 4)),
            dma((4, 4)),
            dma((1,)),
        ],
        compiler_params=pltpu.CompilerParams(
            collective_id=2, has_side_effects=True, vmem_limit_bytes=VMEM_LIMIT
        ),
    )(cot, n2, hidden, gains, vg, vu, vd)


class Chain:
    def __init__(self, place, index, give, mine, far, side, final, sems, y_sems):
        self.place, self.index = place, index
        self.give, self.mine, self.far, self.side, self.final = give, mine, far, side, final
        self.sems, self.y_sems = sems, y_sems

    def remote(self, stage, j, src, dst, device):
        return remote(
            src, dst, self.sems.at[0, stage, self.index, j], self.sems.at[1, stage, self.index, j], device
        )

    def to_y(self, j):
        return remote(
            self.give.at[j],
            self.far.at[j],
            self.y_sems.at[0, self.index, j],
            self.y_sems.at[1, self.index, j],
            self.place.partner("y"),
        )

    def to_dp(self, j):
        return self.remote(
            0, j, self.mine.at[j, 1 - self.place.x], self.side.at[j], self.place.partner("x")
        )

    def to_col(self, s):
        place = self.place
        j = lax.rem(place.z + s, COLS)
        return self.remote(
            1, s, self.mine.at[j, place.x], self.final.at[place.z, place.x], place.peer_z(j)
        )

    def own(self):
        z, x = self.place.z, self.place.x
        return pltpu.make_async_copy(
            self.mine.at[z, x], self.final.at[z, x], self.sems.at[0, 1, self.index, 0]
        )

    def back(self, s):
        place = self.place
        origin = lax.rem(place.z + COLS - s, COLS)
        ref = self.final.at[origin, place.x]
        return self.remote(2, s, ref, ref, place.partner("x"))

    def start(self):
        for j in range(COLS):
            self.to_y(j).start()

    def level_dp(self, waits=True):
        x = self.place.x
        for j in range(COLS):
            if waits:
                self.to_y(j).wait_recv()
            for half in (1 - x, x):
                total = self.mine[j, half].astype(F32) + self.far[j, half].astype(F32)
                self.mine[j, half] = total.astype(BF16)
                if half is not x:
                    self.to_dp(j).start()

    def level_col(self, waits=True):
        x = self.place.x
        for s in (2, 1, 3, 0):
            j = lax.rem(self.place.z + s, COLS)
            if waits:
                self.to_dp(j).wait_recv()
            total = self.mine[j, x].astype(F32) + self.side[j].astype(F32)
            self.mine[j, x] = total.astype(BF16)
            if s:
                self.to_col(s).start()
            else:
                self.own().start()

    def level_back(self):
        self.own().wait()
        self.back(0).start()
        for s in (1, 3, 2):
            self.to_col(s).wait_recv()
            self.back(s).start()

    def finish(self, stages=2):
        for s in range(COLS):
            self.back(s).wait_recv()
        for s in range(COLS):
            if stages > 1:
                self.to_y(s).wait_send()
            if stages:
                self.to_dp(s).wait_send()
            if s:
                self.to_col(s).wait_send()
            self.back(s).wait_send()


def attention_grad_kernel(
    dh,
    att,
    q_in,
    k_in,
    v_in,
    vqkv_hbm,
    vo,
    normed_hbm,
    xg,
    inverse_one,
    gains,
    cosine,
    sine,
    prefix,
    orow,
    gain_two,
    mine_hbm,
    give_hbm,
    far_hbm,
    side_hbm,
    outg,
    gsum,
    small,
    final_f,
    final_a,
    final_o,
    vqkv,
    normed_one,
    datt,
    dqkv,
    acc,
    dk_acc,
    dv_acc,
    center,
    xb,
    parts,
    box_r,
    box_l,
    mine_f,
    far_f,
    side_f,
    away_a,
    near_a,
    give_a,
    mine_a,
    far_a,
    side_a,
    away_o,
    near_o,
    give_o,
    mine_o,
    far_o,
    side_o,
    msg,
    msg_in,
    swaps,
    load_sems,
    line_sems,
    chain_sems,
    y_sems,
    near_sems,
    msg_sems,
):
    place = Place()
    z = place.z
    loads = [pltpu.make_async_copy(mine_hbm.at[w], mine_f.at[w], load_sems.at[0, w]) for w in range(3)]
    loads += [
        pltpu.make_async_copy(side_hbm, side_f.at[0], load_sems.at[1, 0]),
        pltpu.make_async_copy(far_hbm.at[1], far_f.at[1], load_sems.at[1, 1]),
        pltpu.make_async_copy(normed_hbm, normed_one, load_sems.at[2, 1]),
        pltpu.make_async_copy(vqkv_hbm, vqkv, load_sems.at[2, 2]),
    ]
    for i in (1, 4, 0, 3, 2, 5, 6):
        loads[i].start()
    place.barrier()
    chains = [
        Chain(
            place,
            w,
            give_hbm.at[w],
            mine_f.at[w],
            far_f.at[w],
            side_f.at[w],
            final_f.at[w],
            chain_sems,
            y_sems,
        )
        for w in range(3)
    ]
    down, gate, up = chains
    heads = Chain(place, 3, give_a, mine_a, far_a, side_a, final_a, chain_sems, y_sems)
    outs = Chain(place, 4, give_o, mine_o, far_o, side_o, final_o, chain_sems, y_sems)
    up.start()

    def out_copy(s):
        j = lax.rem(z + s, COLS)
        return remote(
            orow.at[j], outg.at[z], line_sems.at[1, 0, 0, s - 1], line_sems.at[1, 1, 0, s - 1], place.peer_z(j)
        )

    out_own = pltpu.make_async_copy(orow.at[z], outg.at[z], load_sems.at[2, 0])
    out_own.start()

    loads[1].wait()
    loads[4].wait()
    gate.level_dp(False)
    loads[0].wait()
    loads[3].wait()
    down.level_col(False)
    rows = dh[...].reshape(512, D)
    wide = jnp.concatenate([vo[:, j].reshape(512, 512) for j in range(COLS)], axis=1)
    acc[...] = dot_nt(rows, wide)
    for k in range(COLS):
        datt[k] = acc[:, k * 128 : (k + 1) * 128].astype(BF16)

    def near_piece(w, t):
        k = 1 + 2 * (t // 4)
        j = t % 4
        src, dst = ((away_a, near_a), (away_o, near_o))[w]
        return remote(
            src.at[t],
            dst.at[t],
            near_sems.at[0, w, t],
            near_sems.at[1, w, t],
            place.partner("core"),
        )

    def grad_piece(w, k, j):
        if w == 0:
            return dot_tn(normed_one[:, j * 512 : (j + 1) * 512], dqkv[k])
        return dot_tn(att[k], dh[:, :, j * 512 : (j + 1) * 512].reshape(512, 512))

    def send_near(w):
        for t in range(8):
            (away_a, away_o)[w][t] = grad_piece(w, 1 + 2 * (t // 4), t % 4).astype(BF16)
            near_piece(w, t).start()

    def add_near(w, half):
        for j in range(COLS):
            t = 4 * half + j
            value = grad_piece(w, 2 * half, j)
            near_piece(w, t).wait_recv()
            value = (value + (near_a, near_o)[w][t].astype(F32)).astype(BF16)
            to = ((mine_a, give_a), (mine_o, give_o))[w][half]
            to[j] = value.reshape(to.shape[1:])
        if half:
            (heads, outs)[w].start()

    send_near(1)

    reach = prefix[0]
    scale = HEAD_DIM**-0.5
    @pl.loop(0, COLS)
    def _(k):
        dk_acc[...] = jnp.zeros((512, 128), F32)
        dv_acc[...] = jnp.zeros((512, 128), F32)
        for first, keys in ((0, 256), (256, 512)):
            part = slice(first, first + 256)
            visible = visible_block(first, 256, keys, reach)
            key_rows = k_in[k, 0:keys, :]
            value_rows = v_in[k, 0:keys, :]
            grad_q = None
            for h in range(2):
                query = half_lanes(q_in[k, part, :], h)
                grad = half_lanes(datt[k, part, :], h)
                scores = dot_nt(query, key_rows) * scale
                weights = jnp.where(visible, jnp.exp(scores), 0.0)
                probs = weights / jnp.sum(weights, axis=1, keepdims=True)
                grad_probs = dot_nt(grad, value_rows)
                middle = jnp.sum(probs * grad_probs, axis=1, keepdims=True)
                grad_scores = (probs * (grad_probs - middle) * scale).astype(BF16)
                got = half_lanes(dot_nn(grad_scores, key_rows), h)
                grad_q = got if grad_q is None else grad_q + got
                dk_acc[0:keys, :] += dot_tn(grad_scores, query)
                dv_acc[0:keys, :] += dot_tn(probs.astype(BF16), grad)
            turned = grad_q * cosine[part, :] - swap_halves(grad_q) * sine[part, :]
            dqkv[k, part, 0:128] = turned.astype(BF16)
        grad_k = dk_acc[...]
        dqkv[k, :, 128:256] = (grad_k * cosine[...] - swap_halves(grad_k) * sine[...]).astype(BF16)
        dqkv[k, :, 256:384] = dv_acc[...].astype(BF16)

    loads[5].wait()
    send_near(0)
    add_near(0, 1)
    add_near(1, 1)
    gate.level_col()
    for s in (1, 2, 3):
        out_copy(s).start()
    add_near(1, 0)
    loads[2].wait()
    loads[6].wait()

    center[...] = jnp.zeros((512, 128), F32)

    def block_copy(j):
        return pltpu.make_async_copy(xg.at[j], xb.at[j % 2], load_sems.at[3, j % 2])

    block_copy(0).start()
    wide_grad = jnp.concatenate([dqkv[k] for k in range(COLS)], axis=1)
    for j in range(COLS):
        if j < COLS - 1:
            block_copy(j + 1).start()
        weight = jnp.concatenate([vqkv[k, j, w] for k in range(COLS) for w in range(3)], axis=1)
        acc[...] = dot_nt(wide_grad, weight)
        block_copy(j).wait()
        msg[j] = jnp.zeros((8, 512), F32)
        gain = gains[j, 0:1, :].astype(F32)

        @pl.loop(0, 16)
        def _(i):
            part = pl.ds(pl.multiple_of(i * 32, 32), 32)
            grad = acc[part, :]
            unit = xb[j % 2, part, :].astype(F32) * inverse_one[part, 0:1]
            center[part, :] += jnp.broadcast_to(
                jnp.sum(grad * gain * unit, axis=1, keepdims=True), (32, 128)
            )
            msg[j, 1:2, :] += jnp.sum(grad * unit, axis=0, keepdims=True)
            parts[j, part, :] = grad.astype(BF16)

        if j == 1:
            down.level_back()
        msg[j, 2:3, :] = gain_two[0:1, j * 512 : (j + 1) * 512]
    total = LineSum(place, parts, box_r, box_l, line_sems.at[0, 0], line_sems.at[0, 1])
    total.run_slot(0)
    turned_center = jnp.transpose(center[...])
    for j in range(COLS):
        msg[j, 0:1, :] = turned_center[0:1, :]

    def msg_copy(s):
        j = lax.rem(z + s, COLS)
        return remote(
            msg.at[j], msg_in.at[s], msg_sems.at[0, s], msg_sems.at[1, s], place.peer_z(j)
        )

    for s in (1, 2, 3):
        msg_copy(s).start()
    up.level_dp()
    add_near(0, 0)
    total.run_slot(1)
    total.run_slot(2)
    heads.level_dp()
    up.level_col()
    outs.level_dp()
    gate.level_back()
    heads.level_col()
    outs.level_col()
    total.run_slot(3)
    gsum[...] = parts[z].astype(F32)
    for s in (1, 2, 3):
        msg_copy(s).wait_recv()
    small[0] = msg[z] + msg_in[1] + msg_in[2] + msg_in[3]
    swaps[0] = small[0]

    def swap_copy(i):
        name = ("core", "y", "x")[i]
        return remote(
            swaps.at[2 * i], swaps.at[2 * i + 1], msg_sems.at[0, 4 + i], msg_sems.at[1, 4 + i], place.partner(name)
        )

    swap_copy(0).start()
    up.level_back()
    swap_copy(0).wait_recv()
    swaps[2] = swaps[0] + swaps[1]
    swap_copy(1).start()
    heads.level_back()
    swap_copy(1).wait_recv()
    swaps[4] = swaps[2] + swaps[3]
    swap_copy(2).start()
    outs.level_back()
    swap_copy(2).wait_recv()
    small[1] = swaps[4] + swaps[5]
    for i in range(3):
        swap_copy(i).wait_send()
    for s in (1, 2, 3):
        msg_copy(s).wait_send()
        out_copy(s).wait_recv()
        out_copy(s).wait_send()
    out_own.wait()
    for w in range(2):
        for t in range(8):
            near_piece(w, t).wait_send()
    down.finish(0)
    gate.finish(1)
    for chain in (up, outs, heads):
        chain.finish()
    total.finish()


def attention_grad(
    dh, att, q, k, v, vqkv, vo, normed_one, xg, inverse_one, gains, cosine, sine, prefix, orow, gain_two, mine, give, far, side
):
    vmem = pl.BlockSpec(memory_space=pltpu.VMEM)
    hbm = pl.BlockSpec(memory_space=pl.ANY)
    smem = pl.BlockSpec(memory_space=pltpu.SMEM)
    shape = jax.ShapeDtypeStruct
    dma = pltpu.SemaphoreType.DMA

    def buffers(rows, width):
        flat = (2 * rows, width)
        halves = (4, 2, rows, width)
        return [
            pltpu.VMEM((8,) + flat, BF16),
            pltpu.VMEM((8,) + flat, BF16),
            pltpu.VMEM(halves, BF16),
            pltpu.VMEM(halves, BF16),
            pltpu.VMEM(halves, BF16),
            pltpu.VMEM((4, rows, width), BF16),
        ]

    return pl.pallas_call(
        attention_grad_kernel,
        name="attention_grad",
        out_shape=[
            shape((4, 128, 512), BF16),
            shape((512, 512), F32),
            shape((2, 8, 512), F32),
            shape((3, 4, 2, 256, 512), BF16),
            shape((4, 2, 256, 384), BF16),
            shape((4, 2, 64, 512), BF16),
        ],
        in_specs=[vmem] * 5 + [hbm, vmem, hbm, hbm] + [vmem] * 4 + [smem] + [vmem] * 2 + [hbm] * 4,
        out_specs=[vmem, vmem, vmem, hbm, hbm, hbm],
        scratch_shapes=[
            pltpu.VMEM((4, 4, 3, 512, 128), BF16),
            pltpu.VMEM((512, D), BF16),
            pltpu.VMEM((4, 512, 128), BF16),
            pltpu.VMEM((4, 512, 384), BF16),
            pltpu.VMEM((512, 512), F32),
            pltpu.VMEM((512, 128), F32),
            pltpu.VMEM((512, 128), F32),
            pltpu.VMEM((512, 128), F32),
            pltpu.VMEM((2, 528, 512), BF16),
            pltpu.VMEM((4, 512, 512), BF16),
            pltpu.VMEM((3, 512, 512), BF16),
            pltpu.VMEM((3, 512, 512), BF16),
            pltpu.VMEM((3, 4, 2, 256, 512), BF16),
            pltpu.VMEM((3, 4, 2, 256, 512), BF16),
            pltpu.VMEM((3, 4, 256, 512), BF16),
        ]
        + buffers(256, 384)
        + buffers(64, 512)
        + [
            pltpu.VMEM((4, 8, 512), F32),
            pltpu.VMEM((4, 8, 512), F32),
            pltpu.VMEM((6, 8, 512), F32),
            dma((4, 4)),
            dma((2, 2, 2, 3)),
            dma((2, 3, 5, 4)),
            dma((2, 5, 4)),
            dma((2, 2, 8)),
            dma((2, 7)),
        ],
        compiler_params=pltpu.CompilerParams(
            collective_id=3, has_side_effects=True, vmem_limit_bytes=VMEM_LIMIT
        ),
    )(
        dh, att, q, k, v, vqkv, vo, normed_one, xg, inverse_one, gains, cosine, sine, prefix, orow, gain_two,
        mine.reshape(3, 4, 2, 256, 512), give.reshape(3, 4, 2, 256, 512), far.reshape(2, 4, 2, 256, 512), side,
    )


def per_device(
    tokens,
    w_query,
    w_key,
    w_value,
    w_output,
    w_gate,
    w_up,
    w_down,
    norm_attn,
    norm_ffn,
    prefix_len,
    cotangent,
):
    rows = lax.axis_size("row")
    cols = lax.axis_size("col")
    seq_len = tokens.shape[0]
    width = tokens.shape[1]
    col_index = lax.axis_index("col")

    prefix_here = lax.ppermute(
        prefix_len,
        ("row", "col"),
        [(c * cols + r, r * cols + c) for r in range(rows) for c in range(cols)],
    )
    xin = jnp.concatenate(
        [tokens, norm_attn[None], norm_ffn[None], jnp.zeros((14, width), BF16)], axis=0
    )
    cosine, sine = rope_tables(seq_len, seq_len)
    cos_wide = jnp.concatenate([cosine] * 4, axis=1)
    sin_wide = jnp.concatenate([-sine, sine] * 2, axis=1)
    (xg, normed_one, q4, k4, v4, att4, hidden, n2, gains, inverse_one, vqkv, vo, vg, vu, vd) = forward_half(
        xin,
        jnp.stack([w_query, w_key, w_value]),
        w_output,
        w_gate,
        w_up,
        w_down,
        cos_wide,
        sin_wide,
        prefix_here,
    )
    dh, orow, gain_two, mine, give, far, side, _ = feed_forward(cotangent, n2, hidden, gains, vg, vu, vd)
    outg, gsum, small, final_f, final_a, final_o = attention_grad(
        dh, att4, q4, k4, v4, vqkv, vo, normed_one, xg, inverse_one, gains, cos_wide, sin_wide, prefix_here,
        orow, gain_two, mine, give, far, side,
    )
    inverse = inverse_one[:, :1]
    unit = tokens.astype(F32) * inverse
    low = lax.dynamic_slice_in_dim(dh.reshape(seq_len, cols * width), col_index * width, width, 1)
    scaled = gsum * norm_attn.astype(F32)[None, :]
    grad_tokens = low.astype(F32) + inverse * (scaled - unit * (small[0, 0] / (cols * width))[:, None])

    def wide_columns(blocks):
        count, _, half, size = blocks.shape
        return blocks.reshape(count, 2 * half, size).transpose(1, 0, 2).reshape(2 * half, count * size).astype(F32)

    return (
        outg.reshape(seq_len, width),
        grad_tokens.astype(BF16),
        wide_columns(final_a[..., :128]),
        wide_columns(final_a[..., 128:256]),
        wide_columns(final_a[..., 256:]),
        final_o.reshape(-1, width).astype(F32),
        wide_columns(final_f[1]),
        wide_columns(final_f[2]),
        final_f[0].reshape(-1, width).astype(F32),
        small[1, 1],
        small[1, 2],
    )


def solution(mesh):
    in_specs = (
        P(("dp", "row"), "col"),
        P("col", "row"),
        P("col", "row"),
        P("col", "row"),
        P("row", "col"),
        P("col", "row"),
        P("col", "row"),
        P("row", "col"),
        P("col"),
        P("col"),
        P(("dp", "col")),
        P(("dp", "row"), "col"),
    )
    out_specs = (
        P(("dp", "row"), "col"),
        P(("dp", "row"), "col"),
        P("col", "row"),
        P("col", "row"),
        P("col", "row"),
        P("row", "col"),
        P("col", "row"),
        P("col", "row"),
        P("row", "col"),
        P("col"),
        P("col"),
    )

    def step(*arrays):
        tokens, prefix_len = arrays[0], arrays[10]
        sequence_each = prefix_len.shape[0] == mesh.shape["dp"] * mesh.shape["row"]
        square = mesh.shape["dp"] == 2 and mesh.shape["row"] == 4 and mesh.shape["col"] == 4
        body = per_device if sequence_each and square else per_device_general
        return jax.shard_map(
            body, mesh=mesh, in_specs=in_specs, out_specs=out_specs, check_vma=False
        )(*arrays)

    return step
```

```python
import jax
import jax.numpy as jnp
from jax import lax
from jax.experimental import pallas as pl
from jax.experimental.pallas import tpu as pltpu
from jax.sharding import PartitionSpec as P

D = 2048
HEAD_DIM = 64


EPSILON = 1e-05
THETA = 130000.0


def feature_total(values):
    return lax.psum(jnp.sum(values, axis=1), "col")


def normalize(values):
    squares = feature_total(values * values)
    inverse_rms = lax.rsqrt(squares / D + EPSILON)
    return (values * inverse_rms[:, None], inverse_rms)


def norm_backward(grad_normed, unit_rows, inverse_rms, gain_row):
    scaled = grad_normed * gain_row[None, :]
    center = feature_total(scaled * unit_rows) / D
    grad_values = inverse_rms[:, None] * (scaled - unit_rows * center[:, None])
    return (grad_values, jnp.sum(grad_normed * unit_rows, axis=0))


def product(left, weight, transposed):
    if transposed:
        return lax.dot_general(
            left, weight, (((1,), (1,)), ((), ())), preferred_element_type=jnp.float32
        )
    return jnp.dot(left, weight, preferred_element_type=jnp.float32)


def outer_product(left, right):
    return lax.dot_general(
        left, right, (((0,), (0,)), ((), ())), preferred_element_type=jnp.float32
    )


def gather_rows(values):
    return lax.all_gather(values, "row", axis=0, tiled=True)


def gather_cols(values):
    return lax.all_gather(values, "col", axis=0, tiled=True)


def sum_to_cols(gathered, weight, transposed):
    row_count = gathered.shape[0] // lax.axis_size("col")

    def partial_term(offset_rows, length_rows):
        return product(gathered, weight, transposed)

    return lax.psum_scatter(
        partial_term(jnp.int32(0), row_count * lax.axis_size("col")).astype(jnp.bfloat16),
        "col",
        scatter_dimension=0,
        tiled=True,
    ).astype(jnp.float32)


def sum_to_rows(gathered, weight, transposed):
    row_count = gathered.shape[0] // lax.axis_size("row")

    def partial_term(offset_rows, length_rows):
        return product(gathered, weight, transposed)

    return lax.psum_scatter(
        partial_term(jnp.int32(0), row_count * lax.axis_size("row")).astype(jnp.bfloat16),
        "row",
        scatter_dimension=0,
        tiled=True,
    ).astype(jnp.float32)


def rope_tables(row_count, seq_len):
    half_dim = HEAD_DIM // 2
    places = (jnp.arange(row_count, dtype=jnp.int32) % seq_len).astype(jnp.float32)
    rates = THETA ** (-2.0 * jnp.arange(half_dim, dtype=jnp.float32) / HEAD_DIM)
    angles = places[:, None] * rates[None, :]
    return (jnp.cos(angles), jnp.sin(angles))


def rotate(values, cosine, sine):
    row_count = values.shape[0]
    shaped = values.reshape(row_count, -1, HEAD_DIM)
    half_dim = HEAD_DIM // 2
    first_half = shaped[:, :, :half_dim]
    second_half = shaped[:, :, half_dim:]
    cosine_rows = cosine[:, None, :]
    sine_rows = sine[:, None, :]
    turned = jnp.concatenate(
        [
            first_half * cosine_rows - second_half * sine_rows,
            second_half * cosine_rows + first_half * sine_rows,
        ],
        axis=2,
    )
    return turned.reshape(row_count, -1)


def visible_keys(first_row, block_rows, seq_len, prefix_here):
    query_place = first_row + jnp.arange(block_rows, dtype=jnp.int32)
    key_place = jnp.arange(seq_len, dtype=jnp.int32)
    return (key_place[None, :] <= query_place[:, None]) | (key_place[None, :] < prefix_here)


def attention_forward(queries, keys, values, prefix_len, seq_len):
    row_count = queries.shape[0]
    heads_here = queries.shape[1] // HEAD_DIM
    block_rows = min(512, seq_len)
    per_sequence = seq_len // block_rows
    query_blocks = queries.reshape(row_count // block_rows, block_rows, heads_here, HEAD_DIM)
    key_seqs = keys.reshape(row_count // seq_len, seq_len, heads_here, HEAD_DIM)
    value_seqs = values.reshape(row_count // seq_len, seq_len, heads_here, HEAD_DIM)
    factor = HEAD_DIM ** (-0.5)
    numbers = jnp.arange(row_count // block_rows, dtype=jnp.int32)

    def one_block(inputs):
        query_block, number = inputs
        sequence = number // per_sequence
        first_row = number % per_sequence * block_rows
        key_seq = lax.dynamic_index_in_dim(key_seqs, sequence, 0, keepdims=False)
        value_seq = lax.dynamic_index_in_dim(value_seqs, sequence, 0, keepdims=False)
        prefix_here = lax.dynamic_index_in_dim(prefix_len, sequence, 0, keepdims=False)
        scores = (
            jnp.einsum("qhd,khd->hqk", query_block, key_seq, preferred_element_type=jnp.float32)
            * factor
        )
        visible = visible_keys(first_row, block_rows, seq_len, prefix_here)
        exponent = jnp.where(visible[None], jnp.exp(scores), 0.0)
        totals = jnp.sum(exponent, axis=2)
        probabilities = (exponent / totals[:, :, None]).astype(jnp.bfloat16)
        attended = jnp.einsum(
            "hqk,khd->qhd", probabilities, value_seq, preferred_element_type=jnp.float32
        )
        return (attended.reshape(block_rows, heads_here * HEAD_DIM), jnp.log(totals))

    attended, log_totals = lax.map(one_block, (query_blocks, numbers))
    return (attended.reshape(row_count, -1), log_totals)


def attention_backward(queries, keys, values, grad_attended, log_totals, prefix_len, seq_len):
    row_count = queries.shape[0]
    heads_here = queries.shape[1] // HEAD_DIM
    block_rows = min(512, seq_len)
    per_sequence = seq_len // block_rows
    query_blocks = queries.reshape(row_count // block_rows, block_rows, heads_here, HEAD_DIM)
    grad_blocks = grad_attended.reshape(row_count // block_rows, block_rows, heads_here, HEAD_DIM)
    key_seqs = keys.reshape(row_count // seq_len, seq_len, heads_here, HEAD_DIM)
    value_seqs = values.reshape(row_count // seq_len, seq_len, heads_here, HEAD_DIM)
    factor = HEAD_DIM ** (-0.5)
    numbers = jnp.arange(row_count // block_rows, dtype=jnp.int32)
    zero_seqs = jnp.zeros(key_seqs.shape, jnp.float32)

    def one_block(carry, inputs):
        grad_key_seqs, grad_value_seqs = carry
        query_block, grad_block, log_block, number = inputs
        sequence = number // per_sequence
        first_row = number % per_sequence * block_rows
        key_seq = lax.dynamic_index_in_dim(key_seqs, sequence, 0, keepdims=False)
        value_seq = lax.dynamic_index_in_dim(value_seqs, sequence, 0, keepdims=False)
        prefix_here = lax.dynamic_index_in_dim(prefix_len, sequence, 0, keepdims=False)
        scores = (
            jnp.einsum("qhd,khd->hqk", query_block, key_seq, preferred_element_type=jnp.float32)
            * factor
        )
        visible = visible_keys(first_row, block_rows, seq_len, prefix_here)
        probabilities = jnp.where(visible[None], jnp.exp(scores - log_block[:, :, None]), 0.0)
        grad_probs = jnp.einsum(
            "qhd,khd->hqk", grad_block, value_seq, preferred_element_type=jnp.float32
        )
        center = jnp.sum(probabilities * grad_probs, axis=2)
        grad_scores = (probabilities * (grad_probs - center[:, :, None]) * factor).astype(
            jnp.bfloat16
        )
        grad_query = jnp.einsum(
            "hqk,khd->qhd", grad_scores, key_seq, preferred_element_type=jnp.float32
        )
        grad_key = jnp.einsum(
            "hqk,qhd->khd", grad_scores, query_block, preferred_element_type=jnp.float32
        )
        grad_value = jnp.einsum(
            "hqk,qhd->khd",
            probabilities.astype(jnp.bfloat16),
            grad_block,
            preferred_element_type=jnp.float32,
        )
        grad_key_seqs = lax.dynamic_update_index_in_dim(
            grad_key_seqs,
            lax.dynamic_index_in_dim(grad_key_seqs, sequence, 0, keepdims=False) + grad_key,
            sequence,
            0,
        )
        grad_value_seqs = lax.dynamic_update_index_in_dim(
            grad_value_seqs,
            lax.dynamic_index_in_dim(grad_value_seqs, sequence, 0, keepdims=False) + grad_value,
            sequence,
            0,
        )
        return (
            (grad_key_seqs, grad_value_seqs),
            grad_query.reshape(block_rows, heads_here * HEAD_DIM),
        )

    carried, grad_queries = lax.scan(
        one_block, (zero_seqs, zero_seqs), (query_blocks, grad_blocks, log_totals, numbers)
    )
    grad_key_seqs, grad_value_seqs = carried
    return (
        grad_queries.reshape(row_count, -1),
        grad_key_seqs.reshape(row_count, -1),
        grad_value_seqs.reshape(row_count, -1),
    )


def per_device_general(
    tokens,
    w_query,
    w_key,
    w_value,
    w_output,
    w_gate,
    w_up,
    w_down,
    norm_attn,
    norm_ffn,
    prefix_len,
    cotangent,
):
    width_attn = w_query.shape[1]
    width_ffn = w_gate.shape[1]
    inputs = tokens.astype(jnp.float32)
    gain_attn = norm_attn.astype(jnp.float32)
    gain_ffn = norm_ffn.astype(jnp.float32)
    unit_one, inverse_one = normalize(inputs)
    normed_one = (unit_one * gain_attn[None, :]).astype(jnp.bfloat16)
    rows_one = gather_rows(normed_one)
    w_attn = jnp.concatenate([w_query, w_key, w_value], axis=1)
    projected = sum_to_cols(rows_one, w_attn, False)
    row_count = projected.shape[0]
    seq_len = row_count // prefix_len.shape[0]
    cosine, sine = rope_tables(row_count, seq_len)
    queries = rotate(projected[:, :width_attn], cosine, sine).astype(jnp.bfloat16)
    keys = rotate(projected[:, width_attn : 2 * width_attn], cosine, sine).astype(jnp.bfloat16)
    values = projected[:, 2 * width_attn :].astype(jnp.bfloat16)
    attended, log_totals = attention_forward(queries, keys, values, prefix_len, seq_len)
    attended_low = attended.astype(jnp.bfloat16)
    attended_rows = gather_cols(attended_low)
    hidden = inputs + sum_to_rows(attended_rows, w_output, False)
    unit_two, inverse_two = normalize(hidden)
    normed_two = (unit_two * gain_ffn[None, :]).astype(jnp.bfloat16)
    rows_two = gather_rows(normed_two)
    w_pair = jnp.concatenate([w_gate, w_up], axis=1)
    gate_up = sum_to_cols(rows_two, w_pair, False)
    gate = gate_up[:, :width_ffn]
    up_proj = gate_up[:, width_ffn:]
    gate_sigmoid = jax.nn.sigmoid(gate)
    silu_gate = gate * gate_sigmoid
    activ = (silu_gate * up_proj).astype(jnp.bfloat16)
    act_rows = gather_cols(activ)
    result = hidden + sum_to_rows(act_rows, w_down, False)
    output = result.astype(jnp.bfloat16)
    grad_rows = gather_rows(cotangent)
    grad_act = sum_to_cols(grad_rows, w_down, True)
    grad_gate = grad_act * up_proj * gate_sigmoid * (1.0 + gate * (1.0 - gate_sigmoid))
    grad_up = grad_act * silu_gate
    grad_pair = jnp.concatenate([grad_gate, grad_up], axis=1).astype(jnp.bfloat16)
    grad_pair_rows = gather_cols(grad_pair)
    grad_normed_two = sum_to_rows(grad_pair_rows, w_pair, True)
    weight_pair = outer_product(rows_two, grad_pair_rows)
    weight_down = outer_product(act_rows, grad_rows)
    grad_from_two, gain_part_two = norm_backward(grad_normed_two, unit_two, inverse_two, gain_ffn)
    grad_hidden = cotangent.astype(jnp.float32) + grad_from_two
    grad_hidden_low = grad_hidden.astype(jnp.bfloat16)
    grad_hidden_rows = gather_rows(grad_hidden_low)
    grad_attended = sum_to_cols(grad_hidden_rows, w_output, True).astype(jnp.bfloat16)
    weight_out = outer_product(attended_rows, grad_hidden_rows)
    grad_queries, grad_keys, grad_values = attention_backward(
        queries, keys, values, grad_attended, log_totals, prefix_len, seq_len
    )
    grad_proj = jnp.concatenate(
        [rotate(grad_queries, cosine, -sine), rotate(grad_keys, cosine, -sine), grad_values], axis=1
    ).astype(jnp.bfloat16)
    grad_proj_rows = gather_cols(grad_proj)
    grad_normed_one = sum_to_rows(grad_proj_rows, w_attn, True)
    weight_attn = outer_product(rows_one, grad_proj_rows)
    weight_attn, weight_out, weight_pair, weight_down = (
        lax.psum(weight_attn.astype(jnp.bfloat16), "dp").astype(jnp.float32),
        lax.psum(weight_out.astype(jnp.bfloat16), "dp").astype(jnp.float32),
        lax.psum(weight_pair.astype(jnp.bfloat16), "dp").astype(jnp.float32),
        lax.psum(weight_down.astype(jnp.bfloat16), "dp").astype(jnp.float32),
    )
    grad_from_one, gain_part_one = norm_backward(grad_normed_one, unit_one, inverse_one, gain_attn)
    grad_tokens = (grad_hidden + grad_from_one).astype(jnp.bfloat16)
    gain_one, gain_two = lax.psum((gain_part_one, gain_part_two), ("dp", "row"))
    return (
        output,
        grad_tokens,
        weight_attn[:, :width_attn],
        weight_attn[:, width_attn : 2 * width_attn],
        weight_attn[:, 2 * width_attn :],
        weight_out,
        weight_pair[:, :width_ffn],
        weight_pair[:, width_ffn:],
        weight_down,
        gain_one,
        gain_two,
    )


MESH = pl.DeviceIdType.MESH
F32 = jnp.float32
BF16 = jnp.bfloat16
COLS = 4
ROW_Y = 2
ROW_CORE = 1
VMEM_LIMIT = 64 * 1024 * 1024 - 64 * 1024


def dot_nn(left, right):
    return lax.dot_general(left, right, (((1,), (0,)), ((), ())), preferred_element_type=F32)


def dot_nt(left, right):
    return lax.dot_general(left, right, (((1,), (1,)), ((), ())), preferred_element_type=F32)


def dot_tn(left, right):
    return lax.dot_general(left, right, (((0,), (0,)), ((), ())), preferred_element_type=F32)


class Place:
    def __init__(self):
        self.x = lax.axis_index("dp")
        self.r = lax.axis_index("row")
        self.z = lax.axis_index("col")

    def peer_z(self, z):
        return {"col": z}

    def partner(self, name):
        if name == "x":
            return {"dp": 1 - self.x}
        bit = ROW_Y if name == "y" else ROW_CORE
        low = lax.rem(lax.div(self.r, bit), 2)
        return {"row": self.r + bit * (1 - 2 * low)}

    def barrier(self):
        sem = pltpu.get_barrier_semaphore()
        for s in (1, 2, 3):
            pl.semaphore_signal(
                sem, 1, device_id=self.peer_z(lax.rem(self.z + s, COLS)), device_id_type=MESH
            )
        for name in ("x", "y", "core"):
            pl.semaphore_signal(sem, 1, device_id=self.partner(name), device_id_type=MESH)
        pl.semaphore_wait(sem, 6)


def remote(src, dst, send, recv, device):
    return pltpu.make_async_remote_copy(
        src_ref=src,
        dst_ref=dst,
        send_sem=send,
        recv_sem=recv,
        device_id=device,
        device_id_type=MESH,
    )


class LineGather:
    def __init__(self, place, buf, send, recv):
        self.place, self.buf, self.send, self.recv = place, buf, send, recv

    def copy(self, step, side):
        z = self.place.z
        block = z - step if side == 0 else z + step
        to = z + 1 if side == 0 else z - 1
        block = jnp.clip(block, 0, COLS - 1)
        to = jnp.clip(to, 0, COLS - 1)
        return remote(
            self.buf.at[block],
            self.buf.at[block],
            self.send.at[side, step],
            self.recv.at[side, step],
            self.place.peer_z(to),
        )

    def sends(self, step, side):
        z = self.place.z
        if side == 0:
            return jnp.logical_and(z - step >= 0, z + 1 < COLS)
        return jnp.logical_and(z + step < COLS, z >= 1)

    def gets(self, step, side):
        z = self.place.z
        if side == 0:
            return z - 1 - step >= 0
        return z + 1 + step < COLS

    def start(self, step):
        for side in (0, 1):

            @pl.when(self.sends(step, side))
            def _():
                self.copy(step, side).start()

    def wait_recv(self, step):
        for side in (0, 1):

            @pl.when(self.gets(step, side))
            def _():
                self.copy(step, side).wait_recv()

    def finish(self):
        for step in range(COLS - 1):
            for side in (0, 1):

                @pl.when(self.sends(step, side))
                def _():
                    self.copy(step, side).wait_send()


class LineSum:
    def __init__(self, place, parts, right, left, send, recv):
        self.place, self.parts = place, parts
        self.inbox = (right, left)
        self.send, self.recv = send, recv

    def copy(self, step, side):
        z = self.place.z
        d = COLS - 1 - step if side == 0 else step
        to = jnp.clip(z + 1 if side == 0 else z - 1, 0, COLS - 1)
        return remote(
            self.parts.at[d],
            self.inbox[side].at[step],
            self.send.at[side, step],
            self.recv.at[side, step],
            self.place.peer_z(to),
        )

    def hops(self, side):
        z = self.place.z
        return z if side == 0 else COLS - 1 - z

    def sends(self, step, side):
        return self.hops(side) < COLS - 1 - step

    def gets(self, step, side):
        hops = self.hops(side)
        return jnp.logical_and(hops > 0, hops <= COLS - 1 - step)

    def run_slot(self, t):
        for side in (0, 1):
            step = t - self.hops(side)
            valid = jnp.logical_and(step >= 0, step < COLS - 1)
            step = jnp.clip(step, 0, COLS - 2)
            d = COLS - 1 - step if side == 0 else step

            @pl.when(jnp.logical_and(valid, self.gets(step, side)))
            def _():
                self.copy(step, side).wait_recv()
                rows = self.parts.shape[1]

                @pl.loop(0, rows // 32)
                def _(i):
                    part = pl.ds(pl.multiple_of(i * 32, 32), 32)
                    total = self.parts[d, part, :].astype(F32) + self.inbox[side][
                        step, part, :
                    ].astype(F32)
                    self.parts[d, part, :] = total.astype(BF16)

            @pl.when(jnp.logical_and(valid, self.sends(step, side)))
            def _():
                self.copy(step, side).start()

    def finish(self):
        for step in range(COLS - 1):
            for side in (0, 1):

                @pl.when(self.sends(step, side))
                def _():
                    self.copy(step, side).wait_send()


class Widen:
    def __init__(self, place, index, source, slot, sems):
        self.place, self.index, self.source, self.slot = place, index, source, slot
        self.sems = sems

    def pair(self, stage, j):
        return self.sems.at[0, stage, self.index, j], self.sems.at[1, stage, self.index, j]

    def local(self):
        z = self.place.z
        return pltpu.make_async_copy(
            self.source(z, None), self.slot(0, z, None), self.sems.at[0, 5, self.index, 0]
        )

    def to_col(self, s):
        place = self.place
        peer = lax.rem(place.z + s, COLS)
        send, recv = self.pair(0, s)
        return remote(
            self.source(peer, place.x), self.slot(0, place.z, place.x), send, recv, place.peer_z(peer)
        )

    def origin(self, s):
        return lax.rem(self.place.z + COLS - s, COLS)

    def to_dp(self, s):
        ref = self.slot(0, self.origin(s), self.place.x)
        send, recv = self.pair(1, s)
        return remote(ref, ref, send, recv, self.place.partner("x"))

    def near(self, stage, s):
        origin = self.origin(s)
        send, recv = self.pair(stage, s)
        if stage == 4:
            src, dst = self.slot(2, origin, None), self.slot(3, origin, None)
        else:
            src = self.source(self.place.z, None) if s == 0 else self.slot(0, origin, None)
            dst = self.slot(2 if stage == 2 else 1, origin, None)
        return remote(src, dst, send, recv, self.place.partner("y" if stage == 2 else "core"))

    def start_col(self):
        for s in (2, 1, 3):
            self.to_col(s).start()

    def start_near(self):
        self.near(2, 0).start()
        self.near(3, 0).start()
        self.local().start()

    def pass_dp(self, s):
        self.to_col(s).wait_recv()
        self.to_dp(s).start()

    def pass_near(self, s):
        self.to_dp(s).wait_recv()
        self.near(2, s).start()
        self.near(3, s).start()

    def pass_far(self, s):
        self.near(2, s).wait_recv()
        self.near(4, s).start()

    def arrived(self):
        self.local().wait()
        for s in range(COLS):
            self.near(3, s).wait_recv()
            self.near(4, s).wait_recv()

    def finish(self):
        for s in range(COLS):
            if s:
                self.to_col(s).wait_send()
                self.to_dp(s).wait_send()
            for stage in (2, 3, 4):
                self.near(stage, s).wait_send()


def swap_halves(values):
    lane = lax.broadcasted_iota(jnp.int32, values.shape, 1)
    up = pltpu.roll(values, 96, 1)
    down = pltpu.roll(values, 32, 1)
    return jnp.where(lax.rem(lane, 64) < 32, up, down)


def half_lanes(values, h):
    lane = lax.broadcasted_iota(jnp.int32, values.shape, 1)
    return jnp.where((lane >= 64) == bool(h), values, jnp.zeros_like(values))


def visible_block(first, rows, keys, prefix):
    query = first + lax.broadcasted_iota(jnp.int32, (rows, keys), 0)
    key = lax.broadcasted_iota(jnp.int32, (rows, keys), 1)
    return jnp.logical_or(key <= query, key < prefix)


def weight_paths(place, sems, w_refs, wide_refs):
    wqkv, wo, wg, wu, wd = w_refs
    vqkv, vo, vg, vu, vd = wide_refs

    def rows_of(first, size, half):
        if half is None:
            return pl.ds(pl.multiple_of(first, 64), size)
        return pl.ds(pl.multiple_of(first + half * (size // 2), 64), size // 2)

    def columns(p, width):
        return pl.ds(pl.multiple_of(p * width, 128), width)

    paths = [
        Widen(
            place,
            0,
            lambda p, h: wqkv.at[:, rows_of(0, 512, h), columns(p, 128)],
            lambda k, j, h: vqkv.at[k, j, :, rows_of(0, 512, h), :],
            sems,
        ),
        Widen(
            place,
            1,
            lambda p, h: wo.at[rows_of(p * 128, 128, h), :],
            lambda k, j, h: vo.at[k, j, rows_of(0, 128, h), :],
            sems,
        ),
    ]
    for i, (w, v) in enumerate(((wg, vg), (wu, vu))):
        paths.append(
            Widen(
                place,
                2 + i,
                lambda p, h, w=w: w.at[rows_of(0, 512, h), columns(p, 512)],
                lambda k, j, h, v=v: v.at[k, j, rows_of(0, 512, h), :],
                sems,
            )
        )
    paths.append(
        Widen(
            place,
            4,
            lambda p, h: wd.at[rows_of(p * 512, 512, h), :],
            lambda k, j, h: vd.at[k, j, rows_of(0, 512, h), :],
            sems,
        )
    )
    return paths


def forward_kernel(
    xin,
    wqkv,
    wo,
    wg,
    wu,
    wd,
    cosine,
    sine,
    prefix,
    xg,
    normed_one,
    q_out,
    k_out,
    v_out,
    att,
    hidden,
    normed_two,
    gains,
    inverse_one,
    vqkv,
    vo,
    vg,
    vu,
    vd,
    parts,
    inbox_r,
    inbox_l,
    acc,
    sems,
    line_sems,
    local_sem,
):
    place = Place()
    z = place.z
    place.barrier()
    own = pltpu.make_async_copy(xin, xg.at[z], local_sem.at[0])
    own.start()
    own.wait()
    gather_x = LineGather(place, xg, line_sems.at[0, 0], line_sems.at[0, 1])
    qkv, out, gate, up, down = weight_paths(
        place, sems, (wqkv, wo, wg, wu, wd), (vqkv, vo, vg, vu, vd)
    )
    qkv.start_col()
    qkv.start_near()
    out.start_col()
    out.start_near()
    gather_x.start(0)
    for s in (1, 3, 2):
        qkv.pass_dp(s)
    for s in (1, 3, 2):
        out.pass_dp(s)
        qkv.pass_near(s)
    for s in (1, 3, 2):
        out.pass_near(s)
    gate.start_near()
    up.start_near()
    down.start_near()
    qkv.pass_far(0)
    out.pass_far(0)
    gather_x.wait_recv(0)
    gather_x.start(1)
    gather_x.wait_recv(1)
    gather_x.start(2)
    for s in (1, 3, 2):
        qkv.pass_far(s)
    for s in (1, 3, 2):
        out.pass_far(s)
    gather_x.wait_recv(2)
    gate.start_col()
    up.start_col()
    down.start_col()

    @pl.loop(0, 16)
    def _(i):
        part = pl.ds(pl.multiple_of(i * 32, 32), 32)
        blocks = [xg[j, part, :].astype(F32) for j in range(COLS)]
        squares = sum(jnp.sum(b * b, axis=1, keepdims=True) for b in blocks)
        inverse = lax.rsqrt(squares / D + EPSILON)
        inverse_one[part, :] = jnp.broadcast_to(inverse, (32, 128))
        for j in range(COLS):
            gain = xg[j, 512:513, :].astype(F32)
            normed_one[part, j * 512 : (j + 1) * 512] = (blocks[j] * inverse * gain).astype(BF16)

    for j in range(COLS):
        gains[j] = xg[j, 512:528, :]
    qkv.arrived()

    for w in range(3):

        @pl.loop(0, 2)
        def _(pair):
            wide = jnp.concatenate(
                [vqkv[2 * pair + i, :, w].reshape(D, 128) for i in range(2)], axis=1
            )
            acc[:, 0:256] = dot_nn(normed_one[...], wide)
            for i in range(2):
                k = 2 * pair + i
                block = acc[:, i * 128 : (i + 1) * 128]
                if w < 2:
                    block = block * cosine[...] + swap_halves(block) * sine[...]
                (q_out, k_out, v_out)[w][k] = block.astype(BF16)


    reach = prefix[0]
    @pl.loop(0, COLS)
    def _(k):
        for first, keys in ((0, 256), (256, 512)):
            queries = q_out[k, first : first + 256, :]
            visible = visible_block(first, 256, keys, reach)
            kept = None
            for h in range(2):
                scores = dot_nt(half_lanes(queries, h), k_out[k, 0:keys, :]) * (HEAD_DIM**-0.5)
                weights = jnp.where(visible, jnp.exp(scores), 0.0)
                probs = (weights / jnp.sum(weights, axis=1, keepdims=True)).astype(BF16)
                got = half_lanes(dot_nn(probs, v_out[k, 0:keys, :]), h)
                kept = got if kept is None else kept + got
            att[k, first : first + 256, :] = kept.astype(BF16)

    out.arrived()
    attended = jnp.concatenate([att[k] for k in range(COLS)], axis=1)

    @pl.loop(0, COLS)
    def _(j):
        piece = dot_nn(attended, vo[:, j].reshape(512, 512))
        lanes = pl.ds(pl.multiple_of(j * 512, 512), 512)
        parts[:, :, lanes] = piece.astype(BF16).reshape(COLS, 128, 512)

    total = LineSum(place, parts, inbox_r, inbox_l, line_sems.at[1, 0], line_sems.at[1, 1])
    total.run_slot(0)
    for path in (gate, up, down):
        for s in (1, 3, 2):
            path.pass_dp(s)
        if path is not gate:
            (gate if path is up else up).pass_far(0)
        if path is down:
            total.run_slot(1)
        for s in (1, 3, 2):
            path.pass_near(s)
        if path is up:
            for s in (1, 3, 2):
                gate.pass_far(s)
    total.run_slot(2)
    up.pass_far(1)
    up.pass_far(3)
    total.run_slot(3)

    @pl.loop(0, 4)
    def _(i):
        part = pl.ds(pl.multiple_of(i * 32, 32), 32)
        rows = pl.ds(pl.multiple_of(z * 128 + i * 32, 32), 32)
        squares = jnp.zeros((32, 1), F32)
        for j in range(COLS):
            lanes = slice(j * 512, (j + 1) * 512)
            value = parts[z, part, lanes].astype(F32) + xg[j, rows, :].astype(F32)
            hidden[part, lanes] = value
            squares += jnp.sum(value * value, axis=1, keepdims=True)
        inverse = lax.rsqrt(squares / D + EPSILON)
        for j in range(COLS):
            lanes = slice(j * 512, (j + 1) * 512)
            gain = xg[j, 513:514, :].astype(F32)
            normed_two[z, part, lanes] = (hidden[part, lanes] * inverse * gain).astype(BF16)

    gather_n = LineGather(place, normed_two, line_sems.at[2, 0], line_sems.at[2, 1])
    gather_n.start(0)
    up.pass_far(2)
    down.pass_far(0)
    down.pass_far(1)
    gather_n.wait_recv(0)
    gather_n.start(1)
    down.pass_far(3)
    gather_n.wait_recv(1)
    gather_n.start(2)
    down.pass_far(2)
    gather_n.wait_recv(2)
    for path in (gate, up, down):
        path.arrived()
    for path in (qkv, out, gate, up, down):
        path.finish()
    gather_x.finish()
    total.finish()
    gather_n.finish()


def forward_half(xin, wqkv, wo, wg, wu, wd, cosine, sine, prefix):
    vmem = pl.BlockSpec(memory_space=pltpu.VMEM)
    hbm = pl.BlockSpec(memory_space=pl.ANY)
    shape = jax.ShapeDtypeStruct
    return pl.pallas_call(
        forward_kernel,
        name="forward_half",
        out_shape=[
            shape((4, 528, 512), BF16),
            shape((512, D), BF16),
            shape((4, 512, 128), BF16),
            shape((4, 512, 128), BF16),
            shape((4, 512, 128), BF16),
            shape((4, 512, 128), BF16),
            shape((128, D), F32),
            shape((4, 128, D), BF16),
            shape((4, 16, 512), BF16),
            shape((512, 128), F32),
            shape((4, 4, 3, 512, 128), BF16),
            shape((4, 4, 128, 512), BF16),
            shape((4, 4, 512, 512), BF16),
            shape((4, 4, 512, 512), BF16),
            shape((4, 4, 512, 512), BF16),
        ],
        in_specs=[vmem, hbm, hbm, hbm, hbm, hbm, vmem, vmem, pl.BlockSpec(memory_space=pltpu.SMEM)],
        out_specs=[vmem] * 12 + [hbm] * 3,
        scratch_shapes=[
            pltpu.VMEM((4, 128, D), BF16),
            pltpu.VMEM((3, 128, D), BF16),
            pltpu.VMEM((3, 128, D), BF16),
            pltpu.VMEM((512, 256), F32),
            pltpu.SemaphoreType.DMA((2, 6, 5, 4)),
            pltpu.SemaphoreType.DMA((3, 2, 2, 3)),
            pltpu.SemaphoreType.DMA((1,)),
        ],
        compiler_params=pltpu.CompilerParams(
            collective_id=1, has_side_effects=True, vmem_limit_bytes=VMEM_LIMIT
        ),
    )(xin, wqkv, wo, wg, wu, wd, cosine, sine, prefix)


def feed_forward_kernel(
    cot,
    n2,
    hidden,
    gains,
    vg_hbm,
    vu_hbm,
    vd_hbm,
    dh,
    orow,
    gain_part,
    mine,
    give,
    far,
    side,
    near,
    cg,
    vg,
    vu,
    vd,
    gate_s,
    up_s,
    act,
    dgate,
    dup,
    pout,
    box_or,
    box_ol,
    parts,
    box_r,
    box_l,
    tiles,
    adds,
    load_sems,
    line_sems,
    near_sems,
    tile_sems,
    add_sems,
    y_sems,
    side_sems,
    local_sem,
):
    place = Place()
    z = place.z
    own = pltpu.make_async_copy(cot, cg.at[z], local_sem.at[0])
    own.start()

    def load(i, k):
        src, dst = ((vg_hbm, vg), (vu_hbm, vu), (vd_hbm, vd))[i]
        return pltpu.make_async_copy(src.at[k], dst.at[k], load_sems.at[i, k])

    own.wait()
    for i, k in ((0, 0), (1, 0), (0, 1), (1, 1), (0, 2), (1, 2), (0, 3), (1, 3)):
        load(i, k).start()
    for k in range(COLS):
        load(2, k).start()
    place.barrier()
    gather_c = LineGather(place, cg, line_sems.at[0, 0], line_sems.at[0, 1])
    gather_c.start(0)

    def first_products(k):
        load(0, k).wait()
        load(1, k).wait()
        rows = n2[...].reshape(512, D)
        gate_s[k] = dot_nn(rows, vg[k].reshape(D, 512))
        up_s[k] = dot_nn(rows, vu[k].reshape(D, 512))

        @pl.loop(0, 16)
        def _(i):
            part = pl.ds(pl.multiple_of(i * 32, 32), 32)
            gate = gate_s[k, part, :]
            act[k, part, :] = (gate * jax.nn.sigmoid(gate) * up_s[k, part, :]).astype(BF16)

    pl.loop(0, 3)(first_products)
    gather_c.wait_recv(0)
    gather_c.start(1)
    pl.loop(3, COLS)(first_products)
    for k in range(COLS):
        load(2, k).wait()

    @pl.loop(0, COLS)
    def _(j):
        wide = jnp.concatenate([act[k] for k in range(COLS)], axis=1)
        piece = dot_nn(wide, vd[:, j].reshape(D, 512))
        lanes = pl.ds(pl.multiple_of(j * 512, 512), 512)
        pout[:, :, lanes] = piece.astype(BF16).reshape(COLS, 128, 512)

    gather_c.wait_recv(1)
    gather_c.start(2)
    out_sum = LineSum(place, pout, box_or, box_ol, line_sems.at[1, 0], line_sems.at[1, 1])
    out_sum.run_slot(0)
    gather_c.wait_recv(2)

    def left_of(w, k, j):
        return act[k] if w == 0 else n2[:, :, pl.ds(pl.multiple_of(j * 512, 512), 512)].reshape(512, 512)

    def right_of(w, k, j):
        return cg[j] if w == 0 else (dgate, dup)[w - 1][k]

    def near_copy(w, t):
        slot = lax.rem(t, 2)
        return remote(
            tiles.at[slot],
            near.at[w, t],
            tile_sems.at[slot],
            near_sems.at[w, t],
            place.partner("core"),
        )

    def send_near(w, half, first=False):
        @pl.loop(4 * half, 4 * half + 4)
        def _(t):
            k = 1 + 2 * half
            j = t - 4 * half
            slot = lax.rem(t, 2)
            if first:

                @pl.when(j >= 2)
                def _():
                    near_copy(w, t).wait_send()
            else:
                near_copy(w, t).wait_send()
            tiles[slot] = dot_tn(left_of(w, k, j), right_of(w, k, j)).astype(BF16)
            near_copy(w, t).start()

    def fetch(w, t):
        slot = lax.rem(t, 2)
        return pltpu.make_async_copy(near.at[w, t], adds.at[slot], add_sems.at[0, slot])

    def settle(w, t):
        slot = lax.rem(t, 2)
        j = lax.rem(t, 4)
        to = mine if t < 4 else give
        return pltpu.make_async_copy(adds.at[2 + slot], to.at[w, j], add_sems.at[1, slot])

    def add_near(w, half, keep=None):
        for j in range(2):
            near_copy(w, 4 * half + j).wait_recv()
            fetch(w, 4 * half + j).start()
        for j in range(COLS):
            t = 4 * half + j
            slot = t % 2
            k = 2 * half
            value = dot_tn(left_of(w, k, j), right_of(w, k, j))
            fetch(w, t).wait()
            value = (value + adds[slot].astype(F32)).astype(BF16)
            if j < 2:
                near_copy(w, t + 2).wait_recv()
                fetch(w, t + 2).start()
            if keep is not None:
                keep[2 * w, j] = value
            else:
                if j >= 2:
                    settle(w, t - 2).wait()
                adds[2 + slot] = value
                settle(w, t).start()
        if keep is None:
            settle(w, 4 * half + 2).wait()
            settle(w, 4 * half + 3).wait()

    def side_copy(w, j):
        half = pl.ds(pl.multiple_of((1 - place.x) * 256, 256), 256)
        return remote(
            vd.at[2 * w, j, half],
            side.at[w, j],
            side_sems.at[0, w, j],
            side_sems.at[1, w, j],
            place.partner("x"),
        )

    def far_copy(w, j):
        return pltpu.make_async_copy(far.at[w, j], vd.at[2 * w + 1, j], side_sems.at[2, w, j])

    def keep_copy(w, j):
        return pltpu.make_async_copy(vd.at[2 * w, j], mine.at[w, j], side_sems.at[3, w, j])

    def add_far(w, j):
        y_copy(w, j).wait_recv()
        far_copy(w, j).start()
        far_copy(w, j).wait()
        vd[2 * w, j] = (vd[2 * w, j].astype(F32) + vd[2 * w + 1, j].astype(F32)).astype(BF16)
        side_copy(w, j).start()
        keep_copy(w, j).start()

    def y_copy(w, j):
        return remote(
            give.at[w, j], far.at[w, j], y_sems.at[0, w, j], y_sems.at[1, w, j], place.partner("y")
        )

    def send_far(w):
        for j in range(COLS):
            y_copy(w, j).start()

    send_near(0, 1, True)
    add_near(0, 1)
    send_far(0)

    @pl.loop(0, COLS)
    def _(k):
        wide = jnp.concatenate([cg[j] for j in range(COLS)], axis=1)
        weight = jnp.concatenate([vd[k, j] for j in range(COLS)], axis=1)
        grad_act = dot_nt(wide, weight)
        for i in range(8):
            part = slice(i * 64, (i + 1) * 64)
            d_act = grad_act[part]
            gate = gate_s[k, part, :]
            sig = jax.nn.sigmoid(gate)
            dgate[k, part, :] = (
                d_act * up_s[k, part, :] * sig * (1.0 + gate * (1.0 - sig))
            ).astype(BF16)
            dup[k, part, :] = (d_act * gate * sig).astype(BF16)

        @pl.when(k == 0)
        def _():
            out_sum.run_slot(1)

    out_sum.run_slot(2)

    @pl.loop(0, COLS)
    def _(j):
        piece = dot_nt(
            jnp.concatenate([dgate[k] for k in range(COLS)], axis=1),
            jnp.concatenate([vg[k, j] for k in range(COLS)], axis=1),
        ) + dot_nt(
            jnp.concatenate([dup[k] for k in range(COLS)], axis=1),
            jnp.concatenate([vu[k, j] for k in range(COLS)], axis=1),
        )
        lanes = pl.ds(pl.multiple_of(j * 512, 512), 512)
        parts[:, :, lanes] = piece.astype(BF16).reshape(COLS, 128, 512)

    total = LineSum(place, parts, box_r, box_l, line_sems.at[2, 0], line_sems.at[2, 1])
    out_sum.run_slot(3)
    total.run_slot(0)
    send_near(1, 1)
    send_near(0, 0)
    total.run_slot(1)
    add_near(1, 1)
    send_far(1)
    add_near(0, 0, vd)
    total.run_slot(2)
    add_far(0, 0)
    add_far(0, 1)
    send_near(1, 0)
    add_far(0, 2)
    total.run_slot(3)

    gain_part[...] = jnp.zeros((8, D), F32)

    @pl.loop(0, 4)
    def _(i):
        part = pl.ds(pl.multiple_of(i * 32, 32), 32)
        rows = pl.ds(pl.multiple_of(z * 128 + i * 32, 32), 32)
        squares = jnp.zeros((32, 1), F32)
        center = jnp.zeros((32, 1), F32)
        for j in range(COLS):
            lanes = slice(j * 512, (j + 1) * 512)
            value = hidden[part, lanes]
            squares += jnp.sum(value * value, axis=1, keepdims=True)
        inverse = lax.rsqrt(squares / D + EPSILON)
        for j in range(COLS):
            lanes = slice(j * 512, (j + 1) * 512)
            grad = parts[z, part, lanes].astype(F32)
            unit = hidden[part, lanes] * inverse
            center += jnp.sum(grad * gains[j, 1:2, :].astype(F32) * unit, axis=1, keepdims=True)
            gain_part[0:1, lanes] += jnp.sum(grad * unit, axis=0, keepdims=True)
        center = center / D
        for j in range(COLS):
            lanes = slice(j * 512, (j + 1) * 512)
            grad = parts[z, part, lanes].astype(F32)
            unit = hidden[part, lanes] * inverse
            scaled = grad * gains[j, 1:2, :].astype(F32)
            value = cg[j, rows, :].astype(F32) + inverse * (scaled - unit * center)
            dh[z, part, lanes] = value.astype(BF16)
            orow[j, part, :] = (hidden[part, lanes] + pout[z, part, lanes].astype(F32)).astype(BF16)

    gather_h = LineGather(place, dh, line_sems.at[3, 0], line_sems.at[3, 1])
    gather_h.start(0)
    add_near(1, 0, vd)
    send_near(2, 1)
    add_far(0, 3)
    gather_h.wait_recv(0)
    gather_h.start(1)
    add_far(1, 0)
    send_near(2, 0)
    add_near(2, 1)
    gather_h.wait_recv(1)
    gather_h.start(2)
    add_far(1, 1)
    add_near(2, 0)
    add_far(1, 2)
    gather_h.wait_recv(2)
    add_far(1, 3)
    for w in range(2):
        for j in range(COLS):
            side_copy(w, j).wait_recv()
            side_copy(w, j).wait_send()
            keep_copy(w, j).wait()
            y_copy(w, j).wait_send()
    for t in range(2, 4):
        near_copy(2, t).wait_send()
    for line in (gather_c, out_sum, total, gather_h):
        line.finish()


def feed_forward(cot, n2, hidden, gains, vg, vu, vd):
    vmem = pl.BlockSpec(memory_space=pltpu.VMEM)
    hbm = pl.BlockSpec(memory_space=pl.ANY)
    shape = jax.ShapeDtypeStruct
    dma = pltpu.SemaphoreType.DMA
    return pl.pallas_call(
        feed_forward_kernel,
        name="feed_forward",
        out_shape=[
            shape((4, 128, D), BF16),
            shape((4, 128, 512), BF16),
            shape((8, D), F32),
            shape((3, 4, 512, 512), BF16),
            shape((3, 4, 512, 512), BF16),
            shape((2, 4, 512, 512), BF16),
            shape((2, 4, 256, 512), BF16),
            shape((3, 8, 512, 512), BF16),
        ],
        in_specs=[hbm, vmem, vmem, vmem, hbm, hbm, hbm],
        out_specs=[vmem, vmem, vmem, hbm, hbm, hbm, hbm, hbm],
        scratch_shapes=[
            pltpu.VMEM((4, 512, 512), BF16),
            pltpu.VMEM((4, 4, 512, 512), BF16),
            pltpu.VMEM((4, 4, 512, 512), BF16),
            pltpu.VMEM((4, 4, 512, 512), BF16),
            pltpu.VMEM((4, 512, 512), F32),
            pltpu.VMEM((4, 512, 512), F32),
            pltpu.VMEM((4, 512, 512), BF16),
            pltpu.VMEM((4, 512, 512), BF16),
            pltpu.VMEM((4, 512, 512), BF16),
            pltpu.VMEM((4, 128, D), BF16),
            pltpu.VMEM((3, 128, D), BF16),
            pltpu.VMEM((3, 128, D), BF16),
            pltpu.VMEM((4, 128, D), BF16),
            pltpu.VMEM((3, 128, D), BF16),
            pltpu.VMEM((3, 128, D), BF16),
            pltpu.VMEM((2, 512, 512), BF16),
            pltpu.VMEM((4, 512, 512), BF16),
            dma((3, 4)),
            dma((4, 2, 2, 3)),
            dma((3, 8)),
            dma((2,)),
            dma((2, 2)),
            dma((2, 2, 4)),
            dma((4, 2, 4)),
            dma((1,)),
        ],
        compiler_params=pltpu.CompilerParams(
            collective_id=2, has_side_effects=True, vmem_limit_bytes=VMEM_LIMIT
        ),
    )(cot, n2, hidden, gains, vg, vu, vd)


class Chain:
    def __init__(self, place, index, give, mine, far, side, final, sems, y_sems):
        self.place, self.index = place, index
        self.give, self.mine, self.far, self.side, self.final = give, mine, far, side, final
        self.sems, self.y_sems = sems, y_sems

    def remote(self, stage, j, src, dst, device):
        return remote(
            src, dst, self.sems.at[0, stage, self.index, j], self.sems.at[1, stage, self.index, j], device
        )

    def to_y(self, j):
        return remote(
            self.give.at[j],
            self.far.at[j],
            self.y_sems.at[0, self.index, j],
            self.y_sems.at[1, self.index, j],
            self.place.partner("y"),
        )

    def to_dp(self, j):
        return self.remote(
            0, j, self.mine.at[j, 1 - self.place.x], self.side.at[j], self.place.partner("x")
        )

    def to_col(self, s):
        place = self.place
        j = lax.rem(place.z + s, COLS)
        return self.remote(
            1, s, self.mine.at[j, place.x], self.final.at[place.z, place.x], place.peer_z(j)
        )

    def own(self):
        z, x = self.place.z, self.place.x
        return pltpu.make_async_copy(
            self.mine.at[z, x], self.final.at[z, x], self.sems.at[0, 1, self.index, 0]
        )

    def back(self, s):
        place = self.place
        origin = lax.rem(place.z + COLS - s, COLS)
        ref = self.final.at[origin, place.x]
        return self.remote(2, s, ref, ref, place.partner("x"))

    def start(self):
        for j in range(COLS):
            self.to_y(j).start()

    def level_dp(self, waits=True):
        x = self.place.x
        for j in range(COLS):
            if waits:
                self.to_y(j).wait_recv()
            for half in (1 - x, x):
                total = self.mine[j, half].astype(F32) + self.far[j, half].astype(F32)
                self.mine[j, half] = total.astype(BF16)
                if half is not x:
                    self.to_dp(j).start()

    def level_col(self, waits=True):
        x = self.place.x
        for s in (2, 1, 3, 0):
            j = lax.rem(self.place.z + s, COLS)
            if waits:
                self.to_dp(j).wait_recv()
            total = self.mine[j, x].astype(F32) + self.side[j].astype(F32)
            self.mine[j, x] = total.astype(BF16)
            if s:
                self.to_col(s).start()
            else:
                self.own().start()

    def level_back(self):
        self.own().wait()
        self.back(0).start()
        for s in (1, 3, 2):
            self.to_col(s).wait_recv()
            self.back(s).start()

    def finish(self, stages=2):
        for s in range(COLS):
            self.back(s).wait_recv()
        for s in range(COLS):
            if stages > 1:
                self.to_y(s).wait_send()
            if stages:
                self.to_dp(s).wait_send()
            if s:
                self.to_col(s).wait_send()
            self.back(s).wait_send()


def attention_grad_kernel(
    dh,
    att,
    q_in,
    k_in,
    v_in,
    vqkv_hbm,
    vo,
    normed_hbm,
    xg,
    inverse_one,
    gains,
    cosine,
    sine,
    prefix,
    orow,
    gain_two,
    mine_hbm,
    give_hbm,
    side_hbm,
    outg,
    gsum,
    small,
    final_f,
    final_a,
    final_o,
    vqkv,
    normed_one,
    datt,
    dqkv,
    acc,
    dk_acc,
    dv_acc,
    center,
    xb,
    parts,
    box_r,
    box_l,
    mine_f,
    far_f,
    side_f,
    away_a,
    near_a,
    give_a,
    mine_a,
    far_a,
    side_a,
    away_o,
    near_o,
    give_o,
    mine_o,
    far_o,
    side_o,
    msg,
    msg_in,
    swaps,
    load_sems,
    line_sems,
    chain_sems,
    y_sems,
    near_sems,
    msg_sems,
):
    place = Place()
    z = place.z
    loads = [pltpu.make_async_copy(mine_hbm.at[w], mine_f.at[w], load_sems.at[0, w]) for w in range(3)]
    loads += [
        pltpu.make_async_copy(side_hbm.at[0], side_f.at[0], load_sems.at[1, 0]),
        pltpu.make_async_copy(side_hbm.at[1], side_f.at[1], load_sems.at[1, 1]),
        pltpu.make_async_copy(normed_hbm, normed_one, load_sems.at[2, 1]),
        pltpu.make_async_copy(vqkv_hbm, vqkv, load_sems.at[2, 2]),
    ]
    for i in (0, 3, 1, 4, 5, 6, 2):
        loads[i].start()
    place.barrier()
    chains = [
        Chain(
            place,
            w,
            give_hbm.at[w],
            mine_f.at[w],
            far_f,
            side_f.at[w],
            final_f.at[w],
            chain_sems,
            y_sems,
        )
        for w in range(3)
    ]
    down, gate, up = chains
    heads = Chain(place, 3, give_a, mine_a, far_a, side_a, final_a, chain_sems, y_sems)
    outs = Chain(place, 4, give_o, mine_o, far_o, side_o, final_o, chain_sems, y_sems)
    up.start()

    def out_copy(s):
        j = lax.rem(z + s, COLS)
        return remote(
            orow.at[j], outg.at[z], line_sems.at[1, 0, 0, s - 1], line_sems.at[1, 1, 0, s - 1], place.peer_z(j)
        )

    out_own = pltpu.make_async_copy(orow.at[z], outg.at[z], load_sems.at[2, 0])
    out_own.start()

    loads[0].wait()
    loads[3].wait()
    down.level_col(False)
    loads[1].wait()
    loads[4].wait()
    gate.level_col(False)
    rows = dh[...].reshape(512, D)
    wide = jnp.concatenate([vo[:, j].reshape(512, 512) for j in range(COLS)], axis=1)
    acc[...] = dot_nt(rows, wide)
    for k in range(COLS):
        datt[k] = acc[:, k * 128 : (k + 1) * 128].astype(BF16)

    def near_piece(w, t):
        k = 1 + 2 * (t // 4)
        j = t % 4
        src, dst = ((away_a, near_a), (away_o, near_o))[w]
        return remote(
            src.at[t],
            dst.at[t],
            near_sems.at[0, w, t],
            near_sems.at[1, w, t],
            place.partner("core"),
        )

    def grad_piece(w, k, j):
        if w == 0:
            return dot_tn(normed_one[:, j * 512 : (j + 1) * 512], dqkv[k])
        return dot_tn(att[k], dh[:, :, j * 512 : (j + 1) * 512].reshape(512, 512))

    def send_near(w):
        for t in range(8):
            (away_a, away_o)[w][t] = grad_piece(w, 1 + 2 * (t // 4), t % 4).astype(BF16)
            near_piece(w, t).start()

    def add_near(w, half):
        for j in range(COLS):
            t = 4 * half + j
            value = grad_piece(w, 2 * half, j)
            near_piece(w, t).wait_recv()
            value = (value + (near_a, near_o)[w][t].astype(F32)).astype(BF16)
            to = ((mine_a, give_a), (mine_o, give_o))[w][half]
            to[j] = value.reshape(to.shape[1:])
        if half:
            (heads, outs)[w].start()

    send_near(1)

    reach = prefix[0]
    scale = HEAD_DIM**-0.5
    @pl.loop(0, COLS)
    def _(k):
        dk_acc[...] = jnp.zeros((512, 128), F32)
        dv_acc[...] = jnp.zeros((512, 128), F32)
        for first, keys in ((0, 256), (256, 512)):
            part = slice(first, first + 256)
            visible = visible_block(first, 256, keys, reach)
            key_rows = k_in[k, 0:keys, :]
            value_rows = v_in[k, 0:keys, :]
            grad_q = None
            for h in range(2):
                query = half_lanes(q_in[k, part, :], h)
                grad = half_lanes(datt[k, part, :], h)
                scores = dot_nt(query, key_rows) * scale
                weights = jnp.where(visible, jnp.exp(scores), 0.0)
                probs = weights / jnp.sum(weights, axis=1, keepdims=True)
                grad_probs = dot_nt(grad, value_rows)
                middle = jnp.sum(probs * grad_probs, axis=1, keepdims=True)
                grad_scores = (probs * (grad_probs - middle) * scale).astype(BF16)
                got = half_lanes(dot_nn(grad_scores, key_rows), h)
                grad_q = got if grad_q is None else grad_q + got
                dk_acc[0:keys, :] += dot_tn(grad_scores, query)
                dv_acc[0:keys, :] += dot_tn(probs.astype(BF16), grad)
            turned = grad_q * cosine[part, :] - swap_halves(grad_q) * sine[part, :]
            dqkv[k, part, 0:128] = turned.astype(BF16)
        grad_k = dk_acc[...]
        dqkv[k, :, 128:256] = (grad_k * cosine[...] - swap_halves(grad_k) * sine[...]).astype(BF16)
        dqkv[k, :, 256:384] = dv_acc[...].astype(BF16)

    loads[5].wait()
    send_near(0)
    add_near(0, 1)
    down.level_back()
    add_near(1, 1)
    add_near(1, 0)
    loads[2].wait()
    loads[6].wait()

    center[...] = jnp.zeros((512, 128), F32)

    def block_copy(j):
        return pltpu.make_async_copy(xg.at[j], xb.at[j % 2], load_sems.at[3, j % 2])

    block_copy(0).start()
    wide_grad = jnp.concatenate([dqkv[k] for k in range(COLS)], axis=1)
    for j in range(COLS):
        if j < COLS - 1:
            block_copy(j + 1).start()
        weight = jnp.concatenate([vqkv[k, j, w] for k in range(COLS) for w in range(3)], axis=1)
        acc[...] = dot_nt(wide_grad, weight)
        block_copy(j).wait()
        msg[j] = jnp.zeros((8, 512), F32)
        gain = gains[j, 0:1, :].astype(F32)

        @pl.loop(0, 16)
        def _(i):
            part = pl.ds(pl.multiple_of(i * 32, 32), 32)
            grad = acc[part, :]
            unit = xb[j % 2, part, :].astype(F32) * inverse_one[part, 0:1]
            center[part, :] += jnp.broadcast_to(
                jnp.sum(grad * gain * unit, axis=1, keepdims=True), (32, 128)
            )
            msg[j, 1:2, :] += jnp.sum(grad * unit, axis=0, keepdims=True)
            parts[j, part, :] = grad.astype(BF16)

        msg[j, 2:3, :] = gain_two[0:1, j * 512 : (j + 1) * 512]
    total = LineSum(place, parts, box_r, box_l, line_sems.at[0, 0], line_sems.at[0, 1])
    total.run_slot(0)
    turned_center = jnp.transpose(center[...])
    for j in range(COLS):
        msg[j, 0:1, :] = turned_center[0:1, :]

    def msg_copy(s):
        j = lax.rem(z + s, COLS)
        return remote(
            msg.at[j], msg_in.at[s], msg_sems.at[0, s], msg_sems.at[1, s], place.peer_z(j)
        )

    for s in (1, 2, 3):
        msg_copy(s).start()
    for s in (1, 2, 3):
        out_copy(s).start()
    up.level_dp()
    gate.level_back()
    add_near(0, 0)
    total.run_slot(1)
    total.run_slot(2)
    up.level_col()
    heads.level_dp()
    outs.level_dp()
    total.run_slot(3)
    heads.level_col()
    outs.level_col()
    gsum[...] = parts[z].astype(F32)
    for s in (1, 2, 3):
        msg_copy(s).wait_recv()
    small[0] = msg[z] + msg_in[1] + msg_in[2] + msg_in[3]
    swaps[0] = small[0]

    def swap_copy(i):
        name = ("core", "y", "x")[i]
        return remote(
            swaps.at[2 * i], swaps.at[2 * i + 1], msg_sems.at[0, 4 + i], msg_sems.at[1, 4 + i], place.partner(name)
        )

    swap_copy(0).start()
    up.level_back()
    swap_copy(0).wait_recv()
    swaps[2] = swaps[0] + swaps[1]
    swap_copy(1).start()
    heads.level_back()
    swap_copy(1).wait_recv()
    swaps[4] = swaps[2] + swaps[3]
    swap_copy(2).start()
    outs.level_back()
    swap_copy(2).wait_recv()
    small[1] = swaps[4] + swaps[5]
    for i in range(3):
        swap_copy(i).wait_send()
    for s in (1, 2, 3):
        msg_copy(s).wait_send()
        out_copy(s).wait_recv()
        out_copy(s).wait_send()
    out_own.wait()
    for w in range(2):
        for t in range(8):
            near_piece(w, t).wait_send()
    down.finish(0)
    gate.finish(0)
    for chain in (up, outs, heads):
        chain.finish()
    total.finish()


def attention_grad(
    dh, att, q, k, v, vqkv, vo, normed_one, xg, inverse_one, gains, cosine, sine, prefix, orow, gain_two, mine, give, side
):
    vmem = pl.BlockSpec(memory_space=pltpu.VMEM)
    hbm = pl.BlockSpec(memory_space=pl.ANY)
    smem = pl.BlockSpec(memory_space=pltpu.SMEM)
    shape = jax.ShapeDtypeStruct
    dma = pltpu.SemaphoreType.DMA

    def buffers(rows, width):
        flat = (2 * rows, width)
        halves = (4, 2, rows, width)
        return [
            pltpu.VMEM((8,) + flat, BF16),
            pltpu.VMEM((8,) + flat, BF16),
            pltpu.VMEM(halves, BF16),
            pltpu.VMEM(halves, BF16),
            pltpu.VMEM(halves, BF16),
            pltpu.VMEM((4, rows, width), BF16),
        ]

    return pl.pallas_call(
        attention_grad_kernel,
        name="attention_grad",
        out_shape=[
            shape((4, 128, 512), BF16),
            shape((512, 512), F32),
            shape((2, 8, 512), F32),
            shape((3, 4, 2, 256, 512), BF16),
            shape((4, 2, 256, 384), BF16),
            shape((4, 2, 64, 512), BF16),
        ],
        in_specs=[vmem] * 5 + [hbm, vmem, hbm, hbm] + [vmem] * 4 + [smem] + [vmem] * 2 + [hbm] * 3,
        out_specs=[vmem, vmem, vmem, hbm, hbm, hbm],
        scratch_shapes=[
            pltpu.VMEM((4, 4, 3, 512, 128), BF16),
            pltpu.VMEM((512, D), BF16),
            pltpu.VMEM((4, 512, 128), BF16),
            pltpu.VMEM((4, 512, 384), BF16),
            pltpu.VMEM((512, 512), F32),
            pltpu.VMEM((512, 128), F32),
            pltpu.VMEM((512, 128), F32),
            pltpu.VMEM((512, 128), F32),
            pltpu.VMEM((2, 528, 512), BF16),
            pltpu.VMEM((4, 512, 512), BF16),
            pltpu.VMEM((3, 512, 512), BF16),
            pltpu.VMEM((3, 512, 512), BF16),
            pltpu.VMEM((3, 4, 2, 256, 512), BF16),
            pltpu.VMEM((4, 2, 256, 512), BF16),
            pltpu.VMEM((3, 4, 256, 512), BF16),
        ]
        + buffers(256, 384)
        + buffers(64, 512)
        + [
            pltpu.VMEM((4, 8, 512), F32),
            pltpu.VMEM((4, 8, 512), F32),
            pltpu.VMEM((6, 8, 512), F32),
            dma((4, 4)),
            dma((2, 2, 2, 3)),
            dma((2, 3, 5, 4)),
            dma((2, 5, 4)),
            dma((2, 2, 8)),
            dma((2, 7)),
        ],
        compiler_params=pltpu.CompilerParams(
            collective_id=3, has_side_effects=True, vmem_limit_bytes=VMEM_LIMIT
        ),
    )(
        dh, att, q, k, v, vqkv, vo, normed_one, xg, inverse_one, gains, cosine, sine, prefix, orow, gain_two,
        mine.reshape(3, 4, 2, 256, 512), give.reshape(3, 4, 2, 256, 512), side,
    )


def per_device(
    tokens,
    w_query,
    w_key,
    w_value,
    w_output,
    w_gate,
    w_up,
    w_down,
    norm_attn,
    norm_ffn,
    prefix_len,
    cotangent,
):
    rows = lax.axis_size("row")
    cols = lax.axis_size("col")
    seq_len = tokens.shape[0]
    width = tokens.shape[1]
    col_index = lax.axis_index("col")

    prefix_here = lax.ppermute(
        prefix_len,
        ("row", "col"),
        [(c * cols + r, r * cols + c) for r in range(rows) for c in range(cols)],
    )
    xin = jnp.concatenate(
        [tokens, norm_attn[None], norm_ffn[None], jnp.zeros((14, width), BF16)], axis=0
    )
    cosine, sine = rope_tables(seq_len, seq_len)
    cos_wide = jnp.concatenate([cosine] * 4, axis=1)
    sin_wide = jnp.concatenate([-sine, sine] * 2, axis=1)
    (xg, normed_one, q4, k4, v4, att4, hidden, n2, gains, inverse_one, vqkv, vo, vg, vu, vd) = forward_half(
        xin,
        jnp.stack([w_query, w_key, w_value]),
        w_output,
        w_gate,
        w_up,
        w_down,
        cos_wide,
        sin_wide,
        prefix_here,
    )
    dh, orow, gain_two, mine, give, _, side, _ = feed_forward(cotangent, n2, hidden, gains, vg, vu, vd)
    outg, gsum, small, final_f, final_a, final_o = attention_grad(
        dh, att4, q4, k4, v4, vqkv, vo, normed_one, xg, inverse_one, gains, cos_wide, sin_wide, prefix_here,
        orow, gain_two, mine, give, side,
    )
    inverse = inverse_one[:, :1]
    unit = tokens.astype(F32) * inverse
    low = lax.dynamic_slice_in_dim(dh.reshape(seq_len, cols * width), col_index * width, width, 1)
    scaled = gsum * norm_attn.astype(F32)[None, :]
    grad_tokens = low.astype(F32) + inverse * (scaled - unit * (small[0, 0] / (cols * width))[:, None])

    def wide_columns(blocks):
        count, _, half, size = blocks.shape
        return blocks.reshape(count, 2 * half, size).transpose(1, 0, 2).reshape(2 * half, count * size).astype(F32)

    return (
        outg.reshape(seq_len, width),
        grad_tokens.astype(BF16),
        wide_columns(final_a[..., :128]),
        wide_columns(final_a[..., 128:256]),
        wide_columns(final_a[..., 256:]),
        final_o.reshape(-1, width).astype(F32),
        wide_columns(final_f[1]),
        wide_columns(final_f[2]),
        final_f[0].reshape(-1, width).astype(F32),
        small[1, 1],
        small[1, 2],
    )


def solution(mesh):
    in_specs = (
        P(("dp", "row"), "col"),
        P("col", "row"),
        P("col", "row"),
        P("col", "row"),
        P("row", "col"),
        P("col", "row"),
        P("col", "row"),
        P("row", "col"),
        P("col"),
        P("col"),
        P(("dp", "col")),
        P(("dp", "row"), "col"),
    )
    out_specs = (
        P(("dp", "row"), "col"),
        P(("dp", "row"), "col"),
        P("col", "row"),
        P("col", "row"),
        P("col", "row"),
        P("row", "col"),
        P("col", "row"),
        P("col", "row"),
        P("row", "col"),
        P("col"),
        P("col"),
    )

    def step(*arrays):
        tokens, prefix_len = arrays[0], arrays[10]
        sequence_each = prefix_len.shape[0] == mesh.shape["dp"] * mesh.shape["row"]
        square = mesh.shape["dp"] == 2 and mesh.shape["row"] == 4 and mesh.shape["col"] == 4
        body = per_device if sequence_each and square else per_device_general
        return jax.shard_map(
            body, mesh=mesh, in_specs=in_specs, out_specs=out_specs, check_vma=False
        )(*arrays)

    return step
```
